16 devices in a mesh: dp: 2 (over y, z), ep: 8 (over x, core).
Axes of the slice: x: 4, y: 2, z: 1, core: 2. Of those that a mesh axis runs over, the one named last changes fastest.
The devices are a block of a 4x4x8 slice.
Arguments:
- grad_y: bfloat16 [2048, 1024], P(('dp', 'ep')), parts along dimension 0
- gate_vals: float32 [2048, 8], P(('dp', 'ep')), parts along dimension 0
- topk_idx: int32 [2048, 8], P(('dp', 'ep')), parts along dimension 0
- slot_ids: int32 [2048, 8], P(('dp', 'ep')), parts along dimension 0
- pair_counts: int32 [16, 32], P(('dp', 'ep')), parts along dimension 0
- y_routed: bfloat16 [2048, 8, 1024], P(('dp', 'ep')), parts along dimension 0
- x_disp: bfloat16 [64, 512, 1024], P(('dp', 'ep')), parts along dimension 0
- h_gate: bfloat16 [64, 512, 512], P(('dp', 'ep')), parts along dimension 0
- h_up: bfloat16 [64, 512, 512], P(('dp', 'ep')), parts along dimension 0
- w_gate: bfloat16 [32, 1024, 512], P('ep')
- w_up: bfloat16 [32, 1024, 512], P('ep')
- w_down: bfloat16 [32, 512, 1024], P('ep')
Outputs:
- output 1: bfloat16 [2048, 1024], P(('dp', 'ep')), parts along dimension 0
- output 2: float32 [2048, 8], P(('dp', 'ep')), parts along dimension 0
- output 3: float32 [64, 1024, 512], P(('dp', 'ep')), parts along dimension 0
- output 4: float32 [64, 1024, 512], P(('dp', 'ep')), parts along dimension 0
- output 5: float32 [64, 512, 1024], P(('dp', 'ep')), parts along dimension 0
There are 2 independent parts. The reference program is written for one: setup_inputs(seed, part) draws one part's arguments, and reference() takes and returns one part's arrays. A program takes and returns all parts, laid end to end along the dimension named above; an argument that names none is the same for every part.
All inputs are finite; a program needn't handle non-finite values.
Results may differ from the reference program's by a relative error of at most 0.0149547.
Values are sent between devices in bfloat16 or wider.
A program may use at most 768 MiB of HBM per device.

```python
import jax
import jax.numpy as jnp
from jax import lax

GROUP_DEV = 8
TOKENS_DEV = 128
EXPERTS = 32
TOP_K = 8
MODEL_DIM = 1024
FFN_DIM = 512
CAPACITY = 64
N_TOKENS = GROUP_DEV * TOKENS_DEV
EXPERT_ROWS = GROUP_DEV * CAPACITY


def setup_inputs(seed: int = 0, part: int = 0) -> dict:
    base_key = jax.random.fold_in(jax.random.key(seed), part)
    key_list = jax.random.split(base_key, 8)
    weight_keys = jax.random.split(jax.random.key(seed + 1), 3)
    key_noise, key_bias, key_hot = jax.random.split(key_list[0], 3)
    expert_iota = jnp.arange(EXPERTS, dtype=jnp.int32)
    token_iota = jnp.arange(TOKENS_DEV, dtype=jnp.int32)
    noise_int = jax.random.randint(key_noise, (GROUP_DEV, TOKENS_DEV, EXPERTS), 0, 4 * EXPERTS)
    bias_base = jax.random.randint(key_bias, (EXPERTS,), 0, 2 * EXPERTS)
    bias_int = (bias_base * bias_base) // (4 * EXPERTS)
    hot_expert = jax.random.randint(key_hot, (GROUP_DEV,), 0, EXPERTS)
    hot_bonus = jnp.where((token_iota[None, :, None] < CAPACITY) & (expert_iota[None, None, :] == hot_expert[:, None, None]), 8 * EXPERTS, 0)
    scores = (noise_int + bias_int[None, None, :] + hot_bonus) * EXPERTS + expert_iota[None, None, :]
    expert_ids = lax.top_k(scores, TOP_K)[1].astype(jnp.int32)

    def rank_one(ids_dev):
        flat_ids = ids_dev.reshape(-1)
        onehot = (flat_ids[:, None] == expert_iota[None, :]).astype(jnp.int32)
        before = jnp.cumsum(onehot, axis=0) - onehot
        rank_pos = jnp.sum(before * onehot, axis=1)
        return rank_pos.reshape(TOKENS_DEV, TOP_K), jnp.sum(onehot, axis=0)

    rank_pos, n_total = lax.map(rank_one, expert_ids)
    slot_dev = jnp.where(rank_pos < CAPACITY, rank_pos, -1).astype(jnp.int32)
    pair_counts = jnp.minimum(n_total, CAPACITY).astype(jnp.int32)
    is_kept = slot_dev >= 0
    slot_safe = jnp.where(is_kept, slot_dev, CAPACITY)
    slot_clip = jnp.where(is_kept, slot_dev, 0)
    src_dev = jnp.broadcast_to(jnp.arange(GROUP_DEV, dtype=jnp.int32)[:, None, None], expert_ids.shape)

    w_gate = (jax.random.normal(weight_keys[0], (EXPERTS, MODEL_DIM, FFN_DIM), jnp.float32) * MODEL_DIM ** -0.5).astype(jnp.bfloat16)
    w_up = (jax.random.normal(weight_keys[1], (EXPERTS, MODEL_DIM, FFN_DIM), jnp.float32) * MODEL_DIM ** -0.5).astype(jnp.bfloat16)
    w_down = (jax.random.normal(weight_keys[2], (EXPERTS, FFN_DIM, MODEL_DIM), jnp.float32) * FFN_DIM ** -0.5).astype(jnp.bfloat16)
    x_tok = jax.random.normal(key_list[1], (GROUP_DEV, TOKENS_DEV, MODEL_DIM), jnp.float32).astype(jnp.bfloat16)
    stale_rows = jax.random.normal(key_list[2], (EXPERTS, GROUP_DEV, CAPACITY, MODEL_DIM), jnp.float32).astype(jnp.bfloat16)
    x_vals = jnp.broadcast_to(x_tok[:, :, None, :], (GROUP_DEV, TOKENS_DEV, TOP_K, MODEL_DIM))
    x_disp = stale_rows.at[expert_ids, src_dev, slot_safe].set(x_vals, mode="drop").reshape(EXPERTS, EXPERT_ROWS, MODEL_DIM)

    def forward_one(operands):
        x_rows, w_gate_e, w_up_e, w_down_e = operands
        h_g = jnp.dot(x_rows, w_gate_e, preferred_element_type=jnp.float32).astype(jnp.bfloat16)
        h_u = jnp.dot(x_rows, w_up_e, preferred_element_type=jnp.float32).astype(jnp.bfloat16)
        gate_f = h_g.astype(jnp.float32)
        hidden_act = (gate_f * jax.nn.sigmoid(gate_f) * h_u.astype(jnp.float32)).astype(jnp.bfloat16)
        y_rows = jnp.dot(hidden_act, w_down_e, preferred_element_type=jnp.float32).astype(jnp.bfloat16)
        return h_g, h_u, y_rows

    h_gate, h_up, y_exp = lax.map(forward_one, (x_disp, w_gate, w_up, w_down))
    y_pick = y_exp.reshape(EXPERTS, GROUP_DEV, CAPACITY, MODEL_DIM)[expert_ids, src_dev, slot_clip]
    y_routed = jnp.where(is_kept[..., None], y_pick, jnp.zeros((), jnp.bfloat16)).reshape(N_TOKENS, TOP_K, MODEL_DIM)
    grad_y = jax.random.normal(key_list[3], (N_TOKENS, MODEL_DIM), jnp.float32).astype(jnp.bfloat16)
    gate_vals = jax.random.uniform(key_list[4], (N_TOKENS, TOP_K), jnp.float32, 0.25, 1.0)
    return {"grad_y": grad_y, "gate_vals": gate_vals, "topk_idx": expert_ids.reshape(N_TOKENS, TOP_K), "slot_ids": slot_dev.reshape(N_TOKENS, TOP_K), "pair_counts": pair_counts, "y_routed": y_routed, "x_disp": x_disp, "h_gate": h_gate, "h_up": h_up, "w_gate": w_gate, "w_up": w_up, "w_down": w_down}


def reference(grad_y, gate_vals, topk_idx, slot_ids, pair_counts, y_routed, x_disp, h_gate, h_up, w_gate, w_up, w_down):
    grad_gate = jnp.einsum("td,tkd->tk", grad_y.astype(jnp.float32), y_routed.astype(jnp.float32))
    is_kept = slot_ids >= 0
    src_dev = jnp.broadcast_to((jnp.arange(N_TOKENS, dtype=jnp.int32) // TOKENS_DEV)[:, None], topk_idx.shape)
    slot_safe = jnp.where(is_kept, slot_ids, CAPACITY)
    slot_clip = jnp.where(is_kept, slot_ids, 0)
    gated_rows = (gate_vals[:, :, None] * grad_y.astype(jnp.float32)[:, None, :]).astype(jnp.bfloat16)
    disp_rows = jnp.zeros((EXPERTS, GROUP_DEV, CAPACITY, MODEL_DIM), jnp.bfloat16).at[topk_idx, src_dev, slot_safe].set(gated_rows, mode="drop")
    keep_row = jnp.arange(CAPACITY)[None, None, :] < jnp.transpose(pair_counts)[:, :, None]
    disp_rows = jnp.where(keep_row[..., None], disp_rows, jnp.zeros((), jnp.bfloat16)).reshape(EXPERTS, EXPERT_ROWS, MODEL_DIM)

    def expert_one(operands):
        grad_rows, x_rows, hg_rows, hu_rows, w_gate_e, w_up_e, w_down_e = operands
        grad_hidden = jnp.dot(grad_rows, w_down_e.T, preferred_element_type=jnp.float32).astype(jnp.bfloat16)
        gate_f = hg_rows.astype(jnp.float32)
        up_f = hu_rows.astype(jnp.float32)
        gate_sig = jax.nn.sigmoid(gate_f)
        gate_act = gate_f * gate_sig
        hidden_act = (gate_act * up_f).astype(jnp.bfloat16)
        grad_h = grad_hidden.astype(jnp.float32)
        grad_hgate = (grad_h * up_f * gate_sig * (1.0 + gate_f * (1.0 - gate_sig))).astype(jnp.bfloat16)
        grad_hup = (grad_h * gate_act).astype(jnp.bfloat16)
        grad_wdown = jnp.dot(hidden_act.T, grad_rows, preferred_element_type=jnp.float32)
        grad_wgate = jnp.dot(x_rows.T, grad_hgate, preferred_element_type=jnp.float32)
        grad_wup = jnp.dot(x_rows.T, grad_hup, preferred_element_type=jnp.float32)
        grad_disp = (jnp.dot(grad_hgate, w_gate_e.T, preferred_element_type=jnp.float32) + jnp.dot(grad_hup, w_up_e.T, preferred_element_type=jnp.float32)).astype(jnp.bfloat16)
        return grad_disp, grad_wgate, grad_wup, grad_wdown

    grad_disp, grad_w_gate, grad_w_up, grad_w_down = lax.map(expert_one, (disp_rows, x_disp, h_gate, h_up, w_gate, w_up, w_down))
    back_rows = grad_disp.reshape(EXPERTS, GROUP_DEV, CAPACITY, MODEL_DIM)[topk_idx, src_dev, slot_clip]
    grad_x = jnp.sum(jnp.where(is_kept[..., None], back_rows.astype(jnp.float32), 0.0), axis=1).astype(jnp.bfloat16)
    return grad_x, grad_gate, grad_w_gate, grad_w_up, grad_w_down
```

```python
import jax
import jax.numpy as jnp
from jax import lax
from jax.sharding import PartitionSpec as P


def solution(mesh):
    n_dev = mesh.shape["ep"]
    rows_spec = P(("dp", "ep"), None)
    cube_spec = P(("dp", "ep"), None, None)
    weight_spec = P("ep", None, None)

    def local_step(grad_y, gate_vals, topk_idx, slot_ids, pair_counts, y_routed, x_disp, h_gate, h_up, w_gate, w_up, w_down):
        n_loc = w_gate.shape[0]
        cap = x_disp.shape[1] // n_dev
        tok, model = grad_y.shape
        me = lax.axis_index("ep")
        gy_all = lax.all_gather(grad_y, "ep", axis=0)
        meta = jnp.stack([gate_vals.T, jnp.where(slot_ids >= 0, topk_idx * cap + slot_ids, -1).astype(jnp.float32).T], 0)
        meta_all = lax.all_gather(meta, "ep", axis=0)
        gates = meta_all[:, 0]
        dest = meta_all[:, 1].astype(jnp.int32) - me * (n_loc * cap)
        slot_iota = jnp.arange(n_loc * cap, dtype=jnp.int32)
        hit = dest[:, None, :, :] == slot_iota[None, :, None, None]
        sel = jnp.any(hit, axis=2)
        onehot = sel.astype(jnp.bfloat16)
        gate_row = jnp.sum(jnp.where(hit, gates[:, None], 0.0), axis=(2, 3))
        picked = jnp.einsum("srt,std->srd", onehot, gy_all, preferred_element_type=jnp.float32)
        d_rows = (gate_row[..., None] * picked).astype(jnp.bfloat16)
        d_rows = d_rows.reshape(n_dev, n_loc, cap, model).transpose(1, 0, 2, 3).reshape(n_loc, n_dev * cap, model)
        grad_gate = jnp.einsum("td,tkd->tk", grad_y, y_routed, preferred_element_type=jnp.float32)

        grad_hidden = jnp.einsum("erd,efd->erf", d_rows, w_down, preferred_element_type=jnp.float32).astype(jnp.bfloat16)
        gate_f = h_gate.astype(jnp.float32)
        up_f = h_up.astype(jnp.float32)
        gate_sig = jax.nn.sigmoid(gate_f)
        gate_act = gate_f * gate_sig
        hidden_act = (gate_act * up_f).astype(jnp.bfloat16)
        grad_h = grad_hidden.astype(jnp.float32)
        dh1 = (grad_h * up_f * gate_sig * (1.0 + gate_f * (1.0 - gate_sig))).astype(jnp.bfloat16)
        dh3 = (grad_h * gate_act).astype(jnp.bfloat16)
        r = (jnp.einsum("erf,edf->erd", dh1, w_gate, preferred_element_type=jnp.float32) + jnp.einsum("erf,edf->erd", dh3, w_up, preferred_element_type=jnp.float32)).astype(jnp.bfloat16)
        r = r.reshape(n_loc, n_dev, cap, model).transpose(1, 0, 2, 3).reshape(n_dev, n_loc * cap, model)
        part = jnp.einsum("srt,srd->std", onehot, r, preferred_element_type=jnp.float32)
        gx = lax.psum_scatter(part, "ep", scatter_dimension=0, tiled=False)
        grad_x = gx.astype(jnp.bfloat16)
        grad_wdown = jnp.einsum("erf,erd->efd", hidden_act, d_rows, preferred_element_type=jnp.float32)
        grad_wgate = jnp.einsum("erd,erf->edf", x_disp, dh1, preferred_element_type=jnp.float32)
        grad_wup = jnp.einsum("erd,erf->edf", x_disp, dh3, preferred_element_type=jnp.float32)
        return grad_x, grad_gate, grad_wgate, grad_wup, grad_wdown

    return jax.shard_map(local_step, mesh=mesh, in_specs=(rows_spec, rows_spec, rows_spec, rows_spec, rows_spec, cube_spec, cube_spec, cube_spec, cube_spec, weight_spec, weight_spec, weight_spec), out_specs=(rows_spec, rows_spec, cube_spec, cube_spec, cube_spec), check_vma=False)
```

```python
import functools

import jax
import jax.numpy as jnp
from jax import lax
from jax.experimental import pallas as pl
from jax.experimental.pallas import tpu as pltpu
from jax.sharding import PartitionSpec as P

MESH = pl.DeviceIdType.MESH
F32 = jnp.float32
BF16 = jnp.bfloat16
NT = (((1,), (1,)), ((), ()))
TN = (((0,), (0,)), ((), ()))
SUBS = 2


def exchange_kernel(n_dev, cap, counts, gates, idx, slot, gy_hbm, yr_hbm, h1_hbm, h3_hbm, wg_hbm, wu_hbm, wd_hbm,
                    gx_out, gg_out, d_hbm, dh_hbm, a_hbm,
                    gy_all, yr, h1, h3, wcat, wd, fs, d_buf, dh_buf, a_buf, meta, pt, rbuf, own, psend, pairin, rsend, rrecv,
                    loc_sem, out_sem, meta_ssem, meta_rsem, ag_ssem, ag_rsem, pair_ssem, pair_rsem, ring_ssem, ring_rsem):
    n_loc, ffn, model = wd.shape
    top_k, tok = idx.shape
    n_chip = n_dev // 2
    half = model // 2
    hrow = tok // 2
    me = lax.axis_index("ep")
    x = me // 2
    c = me % 2
    partner = x * 2 + (1 - c)

    def chip(d):
        return (x + d + n_chip) % n_chip

    def dev(i):
        return {"ep": i}

    def load(src, dst, s):
        cp = pltpu.make_async_copy(src, dst, loc_sem.at[s])
        cp.start()
        return cp

    ld_gy = load(gy_hbm, gy_all.at[me], 0)
    ld_yr = load(yr_hbm, yr, 1)
    ld_h1 = load(h1_hbm, h1, 2)
    ld_h3 = load(h3_hbm, h3, 3)
    ld_wd = load(wd_hbm, wd, 4)
    ld_wg = load(wg_hbm, wcat.at[:, :, pl.ds(0, ffn)], 5)
    ld_wu = load(wu_hbm, wcat.at[:, :, pl.ds(ffn, ffn)], 6)

    cnt = jnp.zeros(idx.shape, jnp.int32)
    for e in range(n_loc * n_dev):
        cnt = jnp.where(idx[...] == e, counts[0, e], cnt)
    keep = (slot[...] >= 0) & (slot[...] < cnt)
    meta[me, 0] = gates[...]
    meta[me, 1] = jnp.where(keep, idx[...] * cap + slot[...], -1).astype(F32)

    barrier = pltpu.get_barrier_semaphore()
    for r in range(1, n_dev):
        pl.semaphore_signal(barrier, inc=1, device_id=dev((me + r) % n_dev), device_id_type=MESH)
    pl.semaphore_wait(barrier, n_dev - 1)

    meta_cp = []
    for r in range(1, n_dev):
        cp = pltpu.make_async_remote_copy(src_ref=meta.at[me], dst_ref=meta.at[me], send_sem=meta_ssem.at[r - 1], recv_sem=meta_rsem.at[r - 1],
                                          device_id=dev((me + r) % n_dev), device_id_type=MESH)
        cp.start()
        meta_cp.append(cp)

    def gy_copy(block, lo, n, s, to):
        ref = gy_all.at[block, pl.ds(lo, n), :]
        return pltpu.make_async_remote_copy(src_ref=ref, dst_ref=ref, send_sem=ag_ssem.at[s], recv_sem=ag_rsem.at[s], device_id=dev(to), device_id_type=MESH)

    right = chip(1) * 2 + c
    left = chip(-1) * 2 + c
    far = chip(2) * 2 + c
    ld_gy.wait()
    to_r0 = gy_copy(me, 0, hrow, 0, right)
    to_l1 = gy_copy(me, hrow, hrow, 1, left)
    to_r1 = gy_copy(me, hrow, hrow, 2, right)
    to_l0 = gy_copy(me, 0, hrow, 3, left)
    to_p = gy_copy(me, 0, tok, 4, partner)
    for cp in (to_r0, to_l1, to_p, to_r1, to_l0):
        cp.start()
    fw_r = gy_copy(left, 0, hrow, 5, right)
    fw_l = gy_copy(right, hrow, hrow, 6, left)
    p_l0 = gy_copy(left, 0, hrow, 7, partner)
    p_r1 = gy_copy(right, hrow, hrow, 8, partner)
    p_l1 = gy_copy(left, hrow, hrow, 9, partner)
    p_r0 = gy_copy(right, 0, hrow, 10, partner)
    p_f0 = gy_copy(far, 0, hrow, 11, partner)
    p_f1 = gy_copy(far, hrow, hrow, 12, partner)

    ld_yr.wait()
    step = 16

    @pl.loop(0, tok // step)
    def _(i):
        t = pl.multiple_of(i * step, step)
        g = gy_all[me, pl.ds(t, step), :].astype(F32)
        y = yr[pl.ds(t, step), :, :].astype(F32)
        gg_out[pl.ds(t, step), :] = jnp.sum(y * g[:, None, :], axis=2)

    ld_h1.wait()
    ld_h3.wait()
    rstep = 32

    @pl.loop(0, n_loc * (h1.shape[1] // rstep))
    def _(i):
        e = i // (h1.shape[1] // rstep)
        r = pl.multiple_of((i % (h1.shape[1] // rstep)) * rstep, rstep)
        a = h1[e, pl.ds(r, rstep), :].astype(F32)
        b = h3[e, pl.ds(r, rstep), :].astype(F32)
        g = jax.nn.sigmoid(a)
        s = a * g
        a_buf[e, pl.ds(r, rstep), :] = (s * b).astype(BF16)
        fs[e, pl.ds(r, rstep), pl.ds(0, ffn)] = b * g * (1.0 + a * (1.0 - g))
        fs[e, pl.ds(r, rstep), pl.ds(ffn, ffn)] = s

    out_a = pltpu.make_async_copy(a_buf, a_hbm, out_sem.at[0])
    out_a.start()

    to_r0.wait_recv()
    fw_r.start()
    p_l0.start()
    to_l1.wait_recv()
    fw_l.start()
    p_r1.start()
    for cp in meta_cp:
        cp.wait_recv()
    to_p.wait_recv()
    ld_wd.wait()
    ld_wg.wait()
    ld_wu.wait()

    def build(h):
        rel = meta[h, 1] - (me * (n_loc * cap)).astype(F32)
        gate = meta[h, 0]
        rows = lax.broadcasted_iota(jnp.int32, (n_loc * cap, tok), 0).astype(F32)
        sel = jnp.zeros((n_loc * cap, tok), F32)
        gsel = jnp.zeros((n_loc * cap, tok), F32)
        for k in range(top_k):
            hit = rows == rel[k:k + 1, :]
            sel = jnp.where(hit, 1.0, sel)
            gsel = jnp.where(hit, gate[k:k + 1, :], gsel)
        grow = jnp.sum(gsel, axis=1, keepdims=True)
        pt[h] = sel.T.astype(BF16)
        picked = jnp.dot(sel.astype(BF16), gy_all[h], preferred_element_type=F32)
        rows_d = (grow * picked).astype(BF16)
        for e in range(n_loc):
            d_buf[e, pl.ds(pl.multiple_of(h * cap, cap), cap), :] = rows_d[e * cap:(e + 1) * cap]

    def pair_copy(q, s, lo):
        return pltpu.make_async_remote_copy(src_ref=psend.at[q, :, pl.ds(lo, half)], dst_ref=pairin.at[q, :, pl.ds(lo, half)],
                                            send_sem=pair_ssem.at[s], recv_sem=pair_rsem.at[s], device_id=dev(partner), device_id_type=MESH)

    def unit(dists):
        qs = [chip(d) for d in dists]
        ns = len(qs)

        for q in qs:
            @pl.loop(0, 2)
            def _(i):
                build(q * 2 + i)

        def rows_of(ref, e, q, cols=None):
            rows = pl.ds(pl.multiple_of(q * (2 * cap), 2 * cap), 2 * cap)
            return ref[e, rows, :]

        @pl.loop(0, n_loc)
        def _(e):
            d = jnp.concatenate([rows_of(d_buf, e, q) for q in qs], axis=0)
            da = lax.dot_general(d, wd[e], NT, preferred_element_type=F32).astype(BF16).astype(F32)
            da2 = jnp.concatenate([da, da], axis=1)
            for i, q in enumerate(qs):
                dh = (da2[i * 2 * cap:(i + 1) * 2 * cap] * rows_of(fs, e, q)).astype(BF16)
                dh_buf[e, pl.ds(pl.multiple_of(q * (2 * cap), 2 * cap), 2 * cap), :] = dh

        copies = []
        for hf in range(2):
            @pl.loop(0, n_loc)
            def _(e):
                dh = jnp.concatenate([rows_of(dh_buf, e, q) for q in qs], axis=0)
                r = lax.dot_general(dh, wcat[e, pl.ds(hf * half, half), :], NT, preferred_element_type=F32).astype(BF16)
                for i in range(ns):
                    for j in range(2):
                        rbuf[i, j, pl.ds(pl.multiple_of(e * cap, cap), cap), pl.ds(hf * half, half)] = r[(i * 2 + j) * cap:(i * 2 + j + 1) * cap]

            for i, q in enumerate(qs):
                psend[q, :, pl.ds(hf * half, half)] = jnp.dot(pt[q * 2 + 1 - c], rbuf[i, 1 - c, :, pl.ds(hf * half, half)], preferred_element_type=F32)
            for i, q in enumerate(qs):
                own[q, :, pl.ds(hf * half, half)] = jnp.dot(pt[q * 2 + c], rbuf[i, c, :, pl.ds(hf * half, half)], preferred_element_type=F32)
            for i, d in enumerate(dists):
                cp = pair_copy(qs[i], ((d + n_chip) % n_chip) * 2 + hf, hf * half)
                cp.start()
                copies.append(cp)
        return copies

    pair_cps = {}
    pair_cps[0] = unit((0,))

    to_r1.wait_recv()
    p_l1.start()
    to_l0.wait_recv()
    p_r0.start()
    for cp in (p_l0, p_r1, p_l1, p_r0):
        cp.wait_recv()
    near = unit((-1, 1))
    pair_cps[-1] = [near[0], near[2]]
    pair_cps[1] = [near[1], near[3]]

    fw_r.wait_recv()
    p_f0.start()
    fw_l.wait_recv()
    p_f1.start()

    sub = tok // SUBS

    def ring_copy(dr, st, s):
        k = (dr * 3 + st) * SUBS + s
        return pltpu.make_async_remote_copy(src_ref=rsend.at[k], dst_ref=rrecv.at[k], send_sem=ring_ssem.at[k], recv_sem=ring_rsem.at[k],
                                            device_id=dev(right if dr == 0 else left), device_id_type=MESH)

    ring = {(dr, st, s): ring_copy(dr, st, s) for dr in range(2) for st in range(3) for s in range(SUBS)}
    dest = {0: (-1, 2, 1, 0), 1: (1, 2, -1, 0)}

    def ring_step(st):
        for dr in range(2):
            pair_cps[dest[dr][st]][dr].wait_recv()
        for s in range(SUBS):
            for dr in range(2):
                q = chip(dest[dr][st])
                rows, cols = pl.ds(s * sub, sub), pl.ds(dr * half, half)
                v = own[q, rows, cols] + pairin[q, rows, cols]
                if st > 0:
                    ring[dr, st - 1, s].wait_recv()
                    v = v + rrecv[(dr * 3 + st - 1) * SUBS + s]
                if st < 3:
                    rsend[(dr * 3 + st) * SUBS + s] = v
                    ring[dr, st, s].start()
                else:
                    gx_out[rows, cols] = v.astype(BF16)

    ring_step(0)
    p_f0.wait_recv()
    p_f1.wait_recv()
    pair_cps[2] = unit((2,))
    out_d = pltpu.make_async_copy(d_buf, d_hbm, out_sem.at[1])
    out_dh = pltpu.make_async_copy(dh_buf, dh_hbm, out_sem.at[2])
    out_d.start()
    out_dh.start()
    ring_step(1)
    ring_step(2)
    ring_step(3)

    for cp in meta_cp + [to_r0, to_l1, to_r1, to_l0, to_p, fw_r, fw_l, p_l0, p_r1, p_l1, p_r0, p_f0, p_f1]:
        cp.wait_send()
    for cps in pair_cps.values():
        for cp in cps:
            cp.wait_send()
    for cp in ring.values():
        cp.wait_send()
    out_a.wait()
    out_d.wait()
    out_dh.wait()


def weight_kernel(x_ref, dh_ref, a_ref, d_ref, gwg, gwu, gwd):
    ffn = gwg.shape[2]
    r = lax.dot_general(x_ref[0], dh_ref[0], TN, preferred_element_type=F32)
    gwg[0] = r[:, :ffn]
    gwu[0] = r[:, ffn:]
    gwd[0] = lax.dot_general(a_ref[0], d_ref[0], TN, preferred_element_type=F32)


def solution(mesh):
    n_dev = mesh.shape["ep"]
    rows_spec = P(("dp", "ep"), None)
    cube_spec = P(("dp", "ep"), None, None)
    weight_spec = P("ep", None, None)

    def local_step(grad_y, gate_vals, topk_idx, slot_ids, pair_counts, y_routed, x_disp, h_gate, h_up, w_gate, w_up, w_down):
        n_loc, ffn, model = w_down.shape
        tok, top_k = topk_idx.shape
        rows = x_disp.shape[1]
        cap = rows // n_dev
        n_chip = n_dev // 2
        vm = pl.BlockSpec(memory_space=pltpu.VMEM)
        hbm = pl.BlockSpec(memory_space=pl.ANY)
        dma = pltpu.SemaphoreType.DMA
        gx, gg, d_rows, dh, act = pl.pallas_call(
            functools.partial(exchange_kernel, n_dev, cap),
            out_shape=(jax.ShapeDtypeStruct((tok, model), BF16), jax.ShapeDtypeStruct((tok, top_k), F32),
                       jax.ShapeDtypeStruct((n_loc, rows, model), BF16), jax.ShapeDtypeStruct((n_loc, rows, 2 * ffn), BF16),
                       jax.ShapeDtypeStruct((n_loc, rows, ffn), BF16)),
            in_specs=[pl.BlockSpec(memory_space=pltpu.SMEM), vm, vm, vm] + [hbm] * 7,
            out_specs=(vm, vm, hbm, hbm, hbm),
            scratch_shapes=[
                pltpu.VMEM((n_dev, tok, model), BF16),
                pltpu.VMEM((tok, top_k, model), BF16),
                pltpu.VMEM((n_loc, rows, ffn), BF16),
                pltpu.VMEM((n_loc, rows, ffn), BF16),
                pltpu.VMEM((n_loc, model, 2 * ffn), BF16),
                pltpu.VMEM((n_loc, ffn, model), BF16),
                pltpu.VMEM((n_loc, rows, 2 * ffn), F32),
                pltpu.VMEM((n_loc, rows, model), BF16),
                pltpu.VMEM((n_loc, rows, 2 * ffn), BF16),
                pltpu.VMEM((n_loc, rows, ffn), BF16),
                pltpu.VMEM((n_dev, 2, top_k, tok), F32),
                pltpu.VMEM((n_dev, tok, n_loc * cap), BF16),
                pltpu.VMEM((2, 2, n_loc * cap, model), BF16),
                pltpu.VMEM((n_chip, tok, model), F32),
                pltpu.VMEM((n_chip, tok, model), F32),
                pltpu.VMEM((n_chip, tok, model), F32),
                pltpu.VMEM((6 * SUBS, tok // SUBS, model // 2), F32),
                pltpu.VMEM((6 * SUBS, tok // SUBS, model // 2), F32),
                dma((7,)), dma((3,)), dma((n_dev - 1,)), dma((n_dev - 1,)), dma((13,)), dma((13,)),
                dma((2 * n_chip,)), dma((2 * n_chip,)), dma((6 * SUBS,)), dma((6 * SUBS,)),
            ],
            compiler_params=pltpu.CompilerParams(collective_id=0, has_side_effects=True, vmem_limit_bytes=62 * 1024 * 1024),
            name="exchange",
        )(pair_counts, gate_vals.T, topk_idx.T, slot_ids.T, grad_y, y_routed, h_gate, h_up, w_gate, w_up, w_down)
        js = 2
        gwg, gwu, gwd = pl.pallas_call(
            weight_kernel,
            grid=(n_loc, js),
            out_shape=(jax.ShapeDtypeStruct((n_loc, model, ffn), F32), jax.ShapeDtypeStruct((n_loc, model, ffn), F32),
                       jax.ShapeDtypeStruct((n_loc, ffn, model), F32)),
            in_specs=[pl.BlockSpec((1, rows, model // js), lambda e, j: (e, 0, j)), pl.BlockSpec((1, rows, 2 * ffn), lambda e, j: (e, 0, 0)),
                      pl.BlockSpec((1, rows, ffn // js), lambda e, j: (e, 0, j)), pl.BlockSpec((1, rows, model), lambda e, j: (e, 0, 0))],
            out_specs=(pl.BlockSpec((1, model // js, ffn), lambda e, j: (e, j, 0)), pl.BlockSpec((1, model // js, ffn), lambda e, j: (e, j, 0)),
                       pl.BlockSpec((1, ffn // js, model), lambda e, j: (e, j, 0))),
            compiler_params=pltpu.CompilerParams(dimension_semantics=("arbitrary", "arbitrary")),
            name="weights",
        )(x_disp, dh, act, d_rows)
        return gx, gg, gwg, gwu, gwd

    return jax.shard_map(local_step, mesh=mesh, in_specs=(rows_spec, rows_spec, rows_spec, rows_spec, rows_spec, cube_spec, cube_spec, cube_spec, cube_spec, weight_spec, weight_spec, weight_spec), out_specs=(rows_spec, rows_spec, cube_spec, cube_spec, cube_spec), check_vma=False)
```

```python
import functools

import jax
import jax.numpy as jnp
from jax import lax
from jax.experimental import pallas as pl
from jax.experimental.pallas import tpu as pltpu
from jax.sharding import PartitionSpec as P

MESH = pl.DeviceIdType.MESH
F32 = jnp.float32
BF16 = jnp.bfloat16
NT = (((1,), (1,)), ((), ()))
TN = (((0,), (0,)), ((), ()))
SUBS = 2


def exchange_kernel(n_dev, cap, counts, gates, idx, slot, gy_hbm, yr_hbm, h1_hbm, h3_hbm, wg_hbm, wu_hbm, wd_hbm, x_hbm,
                    gx_out, gg_out, d_buf, dh_buf, a_buf, x_buf,
                    gy_all, yr, h1, h3, wcat, wd, fs, gg_rows, meta, pt, rbuf, own, psend, pairin, rsend, rrecv,
                    loc_sem, meta_ssem, meta_rsem, ag_ssem, ag_rsem, pair_ssem, pair_rsem, ring_ssem, ring_rsem):
    n_loc, ffn, model = wd.shape
    top_k, tok = idx.shape
    n_chip = n_dev // 2
    half = model // 2
    hrow = tok // 2
    me = lax.axis_index("ep")
    x = me // 2
    c = me % 2
    partner = x * 2 + (1 - c)

    def chip(d):
        return (x + d + n_chip) % n_chip

    def dev(i):
        return {"ep": i}

    def load(src, dst, s):
        cp = pltpu.make_async_copy(src, dst, loc_sem.at[s])
        cp.start()
        return cp

    ld_gy = load(gy_hbm, gy_all.at[me], 0)
    ld_yr = load(yr_hbm, yr, 1)
    ld_h1 = load(h1_hbm, h1, 2)
    ld_h3 = load(h3_hbm, h3, 3)
    ld_wd = load(wd_hbm, wd, 4)
    ld_wg = load(wg_hbm, wcat.at[:, :, pl.ds(0, ffn)], 5)
    ld_wu = load(wu_hbm, wcat.at[:, :, pl.ds(ffn, ffn)], 6)

    cnt = jnp.zeros(idx.shape, jnp.int32)
    for e in range(n_loc * n_dev):
        cnt = jnp.where(idx[...] == e, counts[0, e], cnt)
    keep = (slot[...] >= 0) & (slot[...] < cnt)
    meta[me, 0] = gates[...]
    meta[me, 1] = jnp.where(keep, idx[...] * cap + slot[...], -1).astype(F32)

    barrier = pltpu.get_barrier_semaphore()
    for r in range(1, n_dev):
        pl.semaphore_signal(barrier, inc=1, device_id=dev((me + r) % n_dev), device_id_type=MESH)
    pl.semaphore_wait(barrier, n_dev - 1)

    meta_cp = []
    for r in range(1, n_dev):
        cp = pltpu.make_async_remote_copy(src_ref=meta.at[me], dst_ref=meta.at[me], send_sem=meta_ssem.at[r - 1], recv_sem=meta_rsem.at[r - 1],
                                          device_id=dev((me + r) % n_dev), device_id_type=MESH)
        cp.start()
        meta_cp.append(cp)

    def gy_copy(block, lo, n, s, to):
        ref = gy_all.at[block, pl.ds(lo, n), :]
        return pltpu.make_async_remote_copy(src_ref=ref, dst_ref=ref, send_sem=ag_ssem.at[s], recv_sem=ag_rsem.at[s], device_id=dev(to), device_id_type=MESH)

    right = chip(1) * 2 + c
    left = chip(-1) * 2 + c
    far = chip(2) * 2 + c
    ld_gy.wait()
    to_r0 = gy_copy(me, 0, hrow, 0, right)
    to_l1 = gy_copy(me, hrow, hrow, 1, left)
    to_r1 = gy_copy(me, hrow, hrow, 2, right)
    to_l0 = gy_copy(me, 0, hrow, 3, left)
    to_p = gy_copy(me, 0, tok, 4, partner)
    for cp in (to_r0, to_l1, to_p, to_r1, to_l0):
        cp.start()
    fw_r = gy_copy(left, 0, hrow, 5, right)
    fw_l = gy_copy(right, hrow, hrow, 6, left)
    p_l0 = gy_copy(left, 0, hrow, 7, partner)
    p_r1 = gy_copy(right, hrow, hrow, 8, partner)
    p_l1 = gy_copy(left, hrow, hrow, 9, partner)
    p_r0 = gy_copy(right, 0, hrow, 10, partner)
    p_f0 = gy_copy(far, 0, hrow, 11, partner)
    p_f1 = gy_copy(far, hrow, hrow, 12, partner)

    ld_yr.wait()
    step = 16

    @pl.loop(0, tok // step)
    def _(i):
        t = pl.multiple_of(i * step, step)
        g = gy_all[me, pl.ds(t, step), :].astype(F32)
        y = yr[pl.ds(t, step), :, :].astype(F32)
        gg_rows[pl.ds(t, step), :] = jnp.sum(y * g[:, None, :], axis=2)

    gg_out[...] = gg_rows[...].T

    ld_h1.wait()
    ld_h3.wait()
    rstep = 32

    @pl.loop(0, n_loc * (h1.shape[1] // rstep))
    def _(i):
        e = i // (h1.shape[1] // rstep)
        r = pl.multiple_of((i % (h1.shape[1] // rstep)) * rstep, rstep)
        a = h1[e, pl.ds(r, rstep), :].astype(F32)
        b = h3[e, pl.ds(r, rstep), :].astype(F32)
        g = jax.nn.sigmoid(a)
        s = a * g
        a_buf[e, pl.ds(r, rstep), :] = (s * b).astype(BF16)
        fs[e, pl.ds(r, rstep), pl.ds(0, ffn)] = b * g * (1.0 + a * (1.0 - g))
        fs[e, pl.ds(r, rstep), pl.ds(ffn, ffn)] = s


    to_r0.wait_recv()
    fw_r.start()
    p_l0.start()
    to_l1.wait_recv()
    fw_l.start()
    p_r1.start()
    for cp in meta_cp:
        cp.wait_recv()
    to_p.wait_recv()
    ld_wd.wait()
    ld_wg.wait()
    ld_wu.wait()

    def build(h):
        rel = meta[h, 1] - (me * (n_loc * cap)).astype(F32)
        gate = meta[h, 0]
        rows = lax.broadcasted_iota(jnp.int32, (n_loc * cap, tok), 0).astype(F32)
        sel = jnp.zeros((n_loc * cap, tok), F32)
        gsel = jnp.zeros((n_loc * cap, tok), F32)
        for k in range(top_k):
            hit = rows == rel[k:k + 1, :]
            sel = jnp.where(hit, 1.0, sel)
            gsel = jnp.where(hit, gate[k:k + 1, :], gsel)
        grow = jnp.sum(gsel, axis=1, keepdims=True)
        pt[h] = sel.T.astype(BF16)
        picked = jnp.dot(sel.astype(BF16), gy_all[h], preferred_element_type=F32)
        rows_d = (grow * picked).astype(BF16)
        for e in range(n_loc):
            d_buf[e, pl.ds(pl.multiple_of(h * cap, cap), cap), :] = rows_d[e * cap:(e + 1) * cap]

    def pair_copy(q, s, lo):
        return pltpu.make_async_remote_copy(src_ref=psend.at[q, :, pl.ds(lo, half)], dst_ref=pairin.at[q, :, pl.ds(lo, half)],
                                            send_sem=pair_ssem.at[s], recv_sem=pair_rsem.at[s], device_id=dev(partner), device_id_type=MESH)

    def unit(dists):
        qs = [chip(d) for d in dists]
        ns = len(qs)

        for q in qs:
            @pl.loop(0, 2)
            def _(i):
                build(q * 2 + i)

        def rows_of(ref, e, q, cols=None):
            rows = pl.ds(pl.multiple_of(q * (2 * cap), 2 * cap), 2 * cap)
            return ref[e, rows, :]

        @pl.loop(0, n_loc)
        def _(e):
            d = jnp.concatenate([rows_of(d_buf, e, q) for q in qs], axis=0)
            da = lax.dot_general(d, wd[e], NT, preferred_element_type=F32).astype(BF16).astype(F32)
            da2 = jnp.concatenate([da, da], axis=1)
            for i, q in enumerate(qs):
                dh = (da2[i * 2 * cap:(i + 1) * 2 * cap] * rows_of(fs, e, q)).astype(BF16)
                dh_buf[e, pl.ds(pl.multiple_of(q * (2 * cap), 2 * cap), 2 * cap), :] = dh

        copies = []
        for hf in range(2):
            @pl.loop(0, n_loc)
            def _(e):
                dh = jnp.concatenate([rows_of(dh_buf, e, q) for q in qs], axis=0)
                r = lax.dot_general(dh, wcat[e, pl.ds(hf * half, half), :], NT, preferred_element_type=F32).astype(BF16)
                for i in range(ns):
                    for j in range(2):
                        rbuf[i, j, pl.ds(pl.multiple_of(e * cap, cap), cap), pl.ds(hf * half, half)] = r[(i * 2 + j) * cap:(i * 2 + j + 1) * cap]

            for i, q in enumerate(qs):
                psend[q, :, pl.ds(hf * half, half)] = jnp.dot(pt[q * 2 + 1 - c], rbuf[i, 1 - c, :, pl.ds(hf * half, half)], preferred_element_type=F32)
            for i, q in enumerate(qs):
                own[q, :, pl.ds(hf * half, half)] = jnp.dot(pt[q * 2 + c], rbuf[i, c, :, pl.ds(hf * half, half)], preferred_element_type=F32)
            for i, d in enumerate(dists):
                cp = pair_copy(qs[i], ((d + n_chip) % n_chip) * 2 + hf, hf * half)
                cp.start()
                copies.append(cp)
        return copies

    ld_x = load(x_hbm, x_buf, 7)
    pair_cps = {}
    pair_cps[0] = unit((0,))

    to_r1.wait_recv()
    p_l1.start()
    to_l0.wait_recv()
    p_r0.start()
    for cp in (p_l0, p_r1, p_l1, p_r0):
        cp.wait_recv()
    near = unit((-1, 1))
    pair_cps[-1] = [near[0], near[2]]
    pair_cps[1] = [near[1], near[3]]

    fw_r.wait_recv()
    p_f0.start()
    fw_l.wait_recv()
    p_f1.start()

    sub = tok // SUBS

    def ring_copy(dr, st, s):
        k = (dr * 3 + st) * SUBS + s
        return pltpu.make_async_remote_copy(src_ref=rsend.at[k], dst_ref=rrecv.at[k], send_sem=ring_ssem.at[k], recv_sem=ring_rsem.at[k],
                                            device_id=dev(right if dr == 0 else left), device_id_type=MESH)

    ring = {(dr, st, s): ring_copy(dr, st, s) for dr in range(2) for st in range(3) for s in range(SUBS)}
    dest = {0: (-1, 2, 1, 0), 1: (1, 2, -1, 0)}

    def ring_step(st):
        for dr in range(2):
            pair_cps[dest[dr][st]][dr].wait_recv()
        for s in range(SUBS):
            for dr in range(2):
                q = chip(dest[dr][st])
                rows, cols = pl.ds(s * sub, sub), pl.ds(dr * half, half)
                v = own[q, rows, cols] + pairin[q, rows, cols]
                if st > 0:
                    ring[dr, st - 1, s].wait_recv()
                    v = v + rrecv[(dr * 3 + st - 1) * SUBS + s]
                if st < 3:
                    rsend[(dr * 3 + st) * SUBS + s] = v
                    ring[dr, st, s].start()
                else:
                    gx_out[rows, cols] = v.astype(BF16)

    ring_step(0)
    p_f0.wait_recv()
    p_f1.wait_recv()
    pair_cps[2] = unit((2,))
    ring_step(1)
    ring_step(2)
    ring_step(3)

    for cp in meta_cp + [to_r0, to_l1, to_r1, to_l0, to_p, fw_r, fw_l, p_l0, p_r1, p_l1, p_r0, p_f0, p_f1]:
        cp.wait_send()
    for cps in pair_cps.values():
        for cp in cps:
            cp.wait_send()
    for cp in ring.values():
        cp.wait_send()
    ld_x.wait()


def weight_kernel(js, x_ref, dh_ref, a_ref, d_ref, gx_ref, gg_ref, gx_out, gg_out, gwg, gwu, gwd, gbuf, dbuf, sem):
    n_loc, model, ffn = gwg.shape
    xc, ac = model // js, ffn // js
    gx_out[...] = gx_ref[...]
    gg_out[...] = gg_ref[...]

    def copies(i):
        e, j, b = i // js, i % js, i % 2
        rows, arows = pl.ds(pl.multiple_of(j * xc, xc), xc), pl.ds(pl.multiple_of(j * ac, ac), ac)
        return (pltpu.make_async_copy(gbuf.at[b, :, pl.ds(0, ffn)], gwg.at[e, rows, :], sem.at[b, 0]),
                pltpu.make_async_copy(gbuf.at[b, :, pl.ds(ffn, ffn)], gwu.at[e, rows, :], sem.at[b, 1]),
                pltpu.make_async_copy(dbuf.at[b], gwd.at[e, arows, :], sem.at[b, 2]))

    @pl.loop(0, n_loc * js)
    def _(i):
        e, j, b = i // js, i % js, i % 2

        @pl.when(i >= 2)
        def _():
            for cp in copies(i - 2):
                cp.wait()

        gbuf[b] = lax.dot_general(x_ref[e, :, pl.ds(pl.multiple_of(j * xc, xc), xc)], dh_ref[e], TN, preferred_element_type=F32)
        dbuf[b] = lax.dot_general(a_ref[e, :, pl.ds(pl.multiple_of(j * ac, ac), ac)], d_ref[e], TN, preferred_element_type=F32)
        for cp in copies(i):
            cp.start()

    for i in range(n_loc * js - 2, n_loc * js):
        for cp in copies(i):
            cp.wait()


def solution(mesh):
    n_dev = mesh.shape["ep"]
    rows_spec = P(("dp", "ep"), None)
    cube_spec = P(("dp", "ep"), None, None)
    weight_spec = P("ep", None, None)

    def local_step(grad_y, gate_vals, topk_idx, slot_ids, pair_counts, y_routed, x_disp, h_gate, h_up, w_gate, w_up, w_down):
        n_loc, ffn, model = w_down.shape
        tok, top_k = topk_idx.shape
        rows = x_disp.shape[1]
        cap = rows // n_dev
        n_chip = n_dev // 2
        vm = pl.BlockSpec(memory_space=pltpu.VMEM)
        hbm = pl.BlockSpec(memory_space=pl.ANY)
        dma = pltpu.SemaphoreType.DMA
        gx, gg, d_rows, dh, act, x_rows = pl.pallas_call(
            functools.partial(exchange_kernel, n_dev, cap),
            out_shape=(pltpu.VMEM((tok, model), BF16), pltpu.VMEM((top_k, tok), F32), pltpu.VMEM((n_loc, rows, model), BF16),
                       pltpu.VMEM((n_loc, rows, 2 * ffn), BF16), pltpu.VMEM((n_loc, rows, ffn), BF16), pltpu.VMEM((n_loc, rows, model), BF16)),
            in_specs=[pl.BlockSpec(memory_space=pltpu.SMEM), vm, vm, vm] + [hbm] * 8,
            out_specs=(vm,) * 6,
            scratch_shapes=[
                pltpu.VMEM((n_dev, tok, model), BF16),
                pltpu.VMEM((tok, top_k, model), BF16),
                pltpu.VMEM((n_loc, rows, ffn), BF16),
                pltpu.VMEM((n_loc, rows, ffn), BF16),
                pltpu.VMEM((n_loc, model, 2 * ffn), BF16),
                pltpu.VMEM((n_loc, ffn, model), BF16),
                pltpu.VMEM((n_loc, rows, 2 * ffn), F32),
                pltpu.VMEM((tok, top_k), F32),
                pltpu.VMEM((n_dev, 2, top_k, tok), F32),
                pltpu.VMEM((n_dev, tok, n_loc * cap), BF16),
                pltpu.VMEM((2, 2, n_loc * cap, model), BF16),
                pltpu.VMEM((n_chip, tok, model), F32),
                pltpu.VMEM((n_chip, tok, model), F32),
                pltpu.VMEM((n_chip, tok, model), F32),
                pltpu.VMEM((6 * SUBS, tok // SUBS, model // 2), F32),
                pltpu.VMEM((6 * SUBS, tok // SUBS, model // 2), F32),
                dma((8,)), dma((n_dev - 1,)), dma((n_dev - 1,)), dma((13,)), dma((13,)),
                dma((2 * n_chip,)), dma((2 * n_chip,)), dma((6 * SUBS,)), dma((6 * SUBS,)),
            ],
            compiler_params=pltpu.CompilerParams(collective_id=0, has_side_effects=True, vmem_limit_bytes=44 * 1024 * 1024),
            name="exchange",
        )(pair_counts, gate_vals.T, topk_idx.T, slot_ids.T, grad_y, y_routed, h_gate, h_up, w_gate, w_up, w_down, x_disp)
        js = 2
        gx, gg, gwg, gwu, gwd = pl.pallas_call(
            functools.partial(weight_kernel, js),
            out_shape=(jax.ShapeDtypeStruct((tok, model), BF16), jax.ShapeDtypeStruct((top_k, tok), F32), jax.ShapeDtypeStruct((n_loc, model, ffn), F32),
                       jax.ShapeDtypeStruct((n_loc, model, ffn), F32), jax.ShapeDtypeStruct((n_loc, ffn, model), F32)),
            in_specs=[vm] * 6,
            out_specs=(vm, vm, hbm, hbm, hbm),
            scratch_shapes=[pltpu.VMEM((2, model // js, 2 * ffn), F32), pltpu.VMEM((2, ffn // js, model), F32), dma((2, 3))],
            compiler_params=pltpu.CompilerParams(vmem_limit_bytes=20 * 1024 * 1024),
            name="weights",
        )(x_rows, dh, act, d_rows, gx, gg)
        return gx, gg.T, gwg, gwu, gwd

    return jax.shard_map(local_step, mesh=mesh, in_specs=(rows_spec, rows_spec, rows_spec, rows_spec, rows_spec, cube_spec, cube_spec, cube_spec, cube_spec, weight_spec, weight_spec, weight_spec), out_specs=(rows_spec, rows_spec, cube_spec, cube_spec, cube_spec), check_vma=False)
```

```python
import functools

import jax
import jax.numpy as jnp
from jax import lax
from jax.experimental import pallas as pl
from jax.experimental.pallas import tpu as pltpu
from jax.sharding import PartitionSpec as P

MESH = pl.DeviceIdType.MESH
F32 = jnp.float32
BF16 = jnp.bfloat16
NT = (((1,), (1,)), ((), ()))
TN = (((0,), (0,)), ((), ()))
SUBS = 2


def exchange_kernel(n_dev, cap, counts, gates, idx, slot, gy_hbm, yr_hbm, h1_hbm, h3_hbm, wg_hbm, wu_hbm, wd_hbm, x_hbm,
                    gx_out, gg_out, d_buf, dh_buf, a_buf, x_buf,
                    gy_all, yr, h1, h3, wcat, wd, fs, gg_rows, meta, pt, rbuf, own, psend, pairin, rsend, rrecv,
                    loc_sem, meta_ssem, meta_rsem, ag_ssem, ag_rsem, pair_ssem, pair_rsem, ring_ssem, ring_rsem):
    n_loc, ffn, model = wd.shape
    top_k, tok = idx.shape
    n_chip = n_dev // 2
    half = model // 2
    hrow = tok // 2
    me = lax.axis_index("ep")
    x = me // 2
    c = me % 2
    partner = x * 2 + (1 - c)

    def chip(d):
        return (x + d + n_chip) % n_chip

    def dev(i):
        return {"ep": i}

    def load(src, dst, s):
        cp = pltpu.make_async_copy(src, dst, loc_sem.at[s])
        cp.start()
        return cp

    ld_gy = load(gy_hbm, gy_all.at[me], 0)
    ld_h1 = load(h1_hbm, h1, 2)
    ld_h3 = load(h3_hbm, h3, 3)
    ld_wd = load(wd_hbm, wd, 4)
    ld_wg = load(wg_hbm, wcat.at[:, :, pl.ds(0, ffn)], 5)
    ld_wu = load(wu_hbm, wcat.at[:, :, pl.ds(ffn, ffn)], 6)

    cnt = jnp.zeros(idx.shape, jnp.int32)
    for e in range(n_loc * n_dev):
        cnt = jnp.where(idx[...] == e, counts[0, e], cnt)
    keep = (slot[...] >= 0) & (slot[...] < cnt)
    meta[me, 0] = gates[...]
    meta[me, 1] = jnp.where(keep, idx[...] * cap + slot[...], -1).astype(F32)

    barrier = pltpu.get_barrier_semaphore()
    for r in range(1, n_dev):
        pl.semaphore_signal(barrier, inc=1, device_id=dev((me + r) % n_dev), device_id_type=MESH)
    pl.semaphore_wait(barrier, n_dev - 1)

    meta_cp = []
    for r in range(1, n_dev):
        cp = pltpu.make_async_remote_copy(src_ref=meta.at[me], dst_ref=meta.at[me], send_sem=meta_ssem.at[r - 1], recv_sem=meta_rsem.at[r - 1],
                                          device_id=dev((me + r) % n_dev), device_id_type=MESH)
        cp.start()
        meta_cp.append(cp)

    def gy_copy(block, lo, n, s, to):
        ref = gy_all.at[block, pl.ds(lo, n), :]
        return pltpu.make_async_remote_copy(src_ref=ref, dst_ref=ref, send_sem=ag_ssem.at[s], recv_sem=ag_rsem.at[s], device_id=dev(to), device_id_type=MESH)

    right = chip(1) * 2 + c
    left = chip(-1) * 2 + c
    far = chip(2) * 2 + c
    ld_gy.wait()
    to_r0 = gy_copy(me, 0, hrow, 0, right)
    to_l1 = gy_copy(me, hrow, hrow, 1, left)
    to_r1 = gy_copy(me, hrow, hrow, 2, right)
    to_l0 = gy_copy(me, 0, hrow, 3, left)
    to_p = gy_copy(me, 0, tok, 4, partner)
    for cp in (to_r0, to_l1, to_p, to_r1, to_l0):
        cp.start()
    fw_r = gy_copy(left, 0, hrow, 5, right)
    fw_l = gy_copy(right, hrow, hrow, 6, left)
    p_l0 = gy_copy(left, 0, hrow, 7, partner)
    p_r1 = gy_copy(right, hrow, hrow, 8, partner)
    p_l1 = gy_copy(left, hrow, hrow, 9, partner)
    p_r0 = gy_copy(right, 0, hrow, 10, partner)
    p_f0 = gy_copy(far, 0, hrow, 11, partner)
    p_f1 = gy_copy(far, hrow, hrow, 12, partner)

    ld_h1.wait()
    ld_h3.wait()
    rstep = 32

    @pl.loop(0, n_loc * (h1.shape[1] // rstep))
    def _(i):
        e = i // (h1.shape[1] // rstep)
        r = pl.multiple_of((i % (h1.shape[1] // rstep)) * rstep, rstep)
        a = h1[e, pl.ds(r, rstep), :].astype(F32)
        b = h3[e, pl.ds(r, rstep), :].astype(F32)
        g = jax.nn.sigmoid(a)
        s = a * g
        a_buf[e, pl.ds(r, rstep), :] = (s * b).astype(BF16)
        fs[e, pl.ds(r, rstep), pl.ds(0, ffn)] = b * g * (1.0 + a * (1.0 - g))
        fs[e, pl.ds(r, rstep), pl.ds(ffn, ffn)] = s


    def build(h):
        rel = meta[h, 1] - (me * (n_loc * cap)).astype(F32)
        gate = meta[h, 0]
        rows = lax.broadcasted_iota(jnp.int32, (n_loc * cap, tok), 0).astype(F32)
        sel = jnp.zeros((n_loc * cap, tok), F32)
        gsel = jnp.zeros((n_loc * cap, tok), F32)
        for k in range(top_k):
            hit = rows == rel[k:k + 1, :]
            sel = jnp.where(hit, 1.0, sel)
            gsel = jnp.where(hit, gate[k:k + 1, :], gsel)
        grow = jnp.sum(gsel, axis=1, keepdims=True)
        pt[h] = sel.T.astype(BF16)
        picked = jnp.dot(sel.astype(BF16), gy_all[h], preferred_element_type=F32)
        rows_d = (grow * picked).astype(BF16)
        for e in range(n_loc):
            d_buf[e, pl.ds(pl.multiple_of(h * cap, cap), cap), :] = rows_d[e * cap:(e + 1) * cap]

    def pair_copy(q, s, lo):
        return pltpu.make_async_remote_copy(src_ref=psend.at[q, :, pl.ds(lo, half)], dst_ref=pairin.at[q, :, pl.ds(lo, half)],
                                            send_sem=pair_ssem.at[s], recv_sem=pair_rsem.at[s], device_id=dev(partner), device_id_type=MESH)

    def rows_of(ref, e, q):
        return ref[e, pl.ds(pl.multiple_of(q * (2 * cap), 2 * cap), 2 * cap), :]

    def hidden(qs):
        @pl.loop(0, n_loc)
        def _(e):
            d = jnp.concatenate([rows_of(d_buf, e, q) for q in qs], axis=0)
            da = lax.dot_general(d, wd[e], NT, preferred_element_type=F32).astype(BF16).astype(F32)
            da2 = jnp.concatenate([da, da], axis=1)
            for i, q in enumerate(qs):
                dh = (da2[i * 2 * cap:(i + 1) * 2 * cap] * rows_of(fs, e, q)).astype(BF16)
                dh_buf[e, pl.ds(pl.multiple_of(q * (2 * cap), 2 * cap), 2 * cap), :] = dh

    pair_cps = {}

    def back(dists, qs, hf):
        cols = pl.ds(hf * half, half)

        @pl.loop(0, n_loc)
        def _(e):
            dh = jnp.concatenate([rows_of(dh_buf, e, q) for q in qs], axis=0)
            r = lax.dot_general(dh, wcat[e, cols, :], NT, preferred_element_type=F32).astype(BF16)
            for i in range(len(qs)):
                for j in range(2):
                    rbuf[i, j, pl.ds(pl.multiple_of(e * cap, cap), cap), cols] = r[(i * 2 + j) * cap:(i * 2 + j + 1) * cap]

        for i, q in enumerate(qs):
            psend[q, :, cols] = jnp.dot(pt[q * 2 + 1 - c], rbuf[i, 1 - c, :, cols], preferred_element_type=F32)
        for i, d in enumerate(dists):
            cp = pair_copy(qs[i], ((d + n_chip) % n_chip) * 2 + hf, hf * half)
            cp.start()
            pair_cps[d, hf] = cp
        for i, q in enumerate(qs):
            own[q, :, cols] = jnp.dot(pt[q * 2 + c], rbuf[i, c, :, cols], preferred_element_type=F32)

    width = half // SUBS

    def ring_copy(dr, st, s):
        k = (dr * 3 + st) * SUBS + s
        return pltpu.make_async_remote_copy(src_ref=rsend.at[k], dst_ref=rrecv.at[k], send_sem=ring_ssem.at[k], recv_sem=ring_rsem.at[k],
                                            device_id=dev(right if dr == 0 else left), device_id_type=MESH)

    ring = {(dr, st, s): ring_copy(dr, st, s) for dr in range(2) for st in range(3) for s in range(SUBS)}
    dest = {0: (-1, 2, 1, 0), 1: (1, 2, -1, 0)}
    waited = set()

    def ring_step(st, subs=range(SUBS)):
        for s in subs:
            for dr in range(2):
                d = dest[dr][st]
                cols = pl.ds((2 * s + dr) * width, width)
                hf = ((2 * s + dr) * width) // half
                if (d, hf) not in waited:
                    waited.add((d, hf))
                    pair_cps[d, hf].wait_recv()
                q = chip(d)
                v = own[q, :, cols] + pairin[q, :, cols]
                if st > 0:
                    ring[dr, st - 1, s].wait_recv()
                    v = v + rrecv[(dr * 3 + st - 1) * SUBS + s]
                if st < 3:
                    rsend[(dr * 3 + st) * SUBS + s] = v
                    ring[dr, st, s].start()
                else:
                    gx_out[:, cols] = v.astype(BF16)

    for cp in meta_cp:
        cp.wait_recv()
    to_p.wait_recv()
    build(x * 2)
    build(x * 2 + 1)
    to_r0.wait_recv()
    fw_r.start()
    p_l0.start()
    to_l1.wait_recv()
    fw_l.start()
    p_r1.start()
    to_r1.wait_recv()
    p_l1.start()
    to_l0.wait_recv()
    p_r0.start()
    build(left)
    build(right)
    p_l0.wait_recv()
    p_l1.wait_recv()
    build(chip(-1) * 2 + 1 - c)
    p_r0.wait_recv()
    p_r1.wait_recv()
    build(chip(1) * 2 + 1 - c)
    ld_wd.wait()
    near = [chip(-1), chip(1)]
    hidden(near)
    fw_r.wait_recv()
    p_f0.start()
    fw_l.wait_recv()
    p_f1.start()
    ld_wg.wait()
    ld_wu.wait()
    ld_x = load(x_hbm, x_buf, 7)
    ld_yr = load(yr_hbm, yr, 1)
    back((-1, 1), near, 0)
    back((-1, 1), near, 1)
    ring_step(0)
    build(far)
    p_f0.wait_recv()
    p_f1.wait_recv()
    build(chip(2) * 2 + 1 - c)
    rest = [chip(2), x]
    hidden(rest)
    back((2, 0), rest, 0)
    back((2, 0), rest, 1)
    ring_step(1)

    ld_yr.wait()
    step = 16

    @pl.loop(0, tok // step)
    def _(i):
        t = pl.multiple_of(i * step, step)
        g = gy_all[me, pl.ds(t, step), :].astype(F32)
        y = yr[pl.ds(t, step), :, :].astype(F32)
        gg_rows[pl.ds(t, step), :] = jnp.sum(y * g[:, None, :], axis=2)

    gg_out[...] = gg_rows[...].T

    ring_step(2)
    ring_step(3)

    for cp in meta_cp + [to_r0, to_l1, to_r1, to_l0, to_p, fw_r, fw_l, p_l0, p_r1, p_l1, p_r0, p_f0, p_f1]:
        cp.wait_send()
    for cp in pair_cps.values():
        cp.wait_send()
    for cp in ring.values():
        cp.wait_send()
    ld_x.wait()


def weight_kernel(js, x_ref, dh_ref, a_ref, d_ref, gx_ref, gg_ref, gx_out, gg_out, gwg, gwu, gwd, gbuf, dbuf, sem):
    n_loc, model, ffn = gwg.shape
    xc, ac = model // js, ffn // js
    gx_out[...] = gx_ref[...]
    gg_out[...] = gg_ref[...]

    def copies(i):
        e, j, b = i // js, i % js, i % 2
        rows, arows = pl.ds(pl.multiple_of(j * xc, xc), xc), pl.ds(pl.multiple_of(j * ac, ac), ac)
        return (pltpu.make_async_copy(gbuf.at[b, :, pl.ds(0, ffn)], gwg.at[e, rows, :], sem.at[b, 0]),
                pltpu.make_async_copy(gbuf.at[b, :, pl.ds(ffn, ffn)], gwu.at[e, rows, :], sem.at[b, 1]),
                pltpu.make_async_copy(dbuf.at[b], gwd.at[e, arows, :], sem.at[b, 2]))

    @pl.loop(0, n_loc * js)
    def _(i):
        e, j, b = i // js, i % js, i % 2

        @pl.when(i >= 2)
        def _():
            for cp in copies(i - 2):
                cp.wait()

        gbuf[b] = lax.dot_general(x_ref[e, :, pl.ds(pl.multiple_of(j * xc, xc), xc)], dh_ref[e], TN, preferred_element_type=F32)
        dbuf[b] = lax.dot_general(a_ref[e, :, pl.ds(pl.multiple_of(j * ac, ac), ac)], d_ref[e], TN, preferred_element_type=F32)
        for cp in copies(i):
            cp.start()

    for i in range(n_loc * js - 2, n_loc * js):
        for cp in copies(i):
            cp.wait()


def solution(mesh):
    n_dev = mesh.shape["ep"]
    rows_spec = P(("dp", "ep"), None)
    cube_spec = P(("dp", "ep"), None, None)
    weight_spec = P("ep", None, None)

    def local_step(grad_y, gate_vals, topk_idx, slot_ids, pair_counts, y_routed, x_disp, h_gate, h_up, w_gate, w_up, w_down):
        n_loc, ffn, model = w_down.shape
        tok, top_k = topk_idx.shape
        rows = x_disp.shape[1]
        cap = rows // n_dev
        n_chip = n_dev // 2
        vm = pl.BlockSpec(memory_space=pltpu.VMEM)
        hbm = pl.BlockSpec(memory_space=pl.ANY)
        dma = pltpu.SemaphoreType.DMA
        gx, gg, d_rows, dh, act, x_rows = pl.pallas_call(
            functools.partial(exchange_kernel, n_dev, cap),
            out_shape=(pltpu.VMEM((tok, model), BF16), pltpu.VMEM((top_k, tok), F32), pltpu.VMEM((n_loc, rows, model), BF16),
                       pltpu.VMEM((n_loc, rows, 2 * ffn), BF16), pltpu.VMEM((n_loc, rows, ffn), BF16), pltpu.VMEM((n_loc, rows, model), BF16)),
            in_specs=[pl.BlockSpec(memory_space=pltpu.SMEM), vm, vm, vm] + [hbm] * 8,
            out_specs=(vm,) * 6,
            scratch_shapes=[
                pltpu.VMEM((n_dev, tok, model), BF16),
                pltpu.VMEM((tok, top_k, model), BF16),
                pltpu.VMEM((n_loc, rows, ffn), BF16),
                pltpu.VMEM((n_loc, rows, ffn), BF16),
                pltpu.VMEM((n_loc, model, 2 * ffn), BF16),
                pltpu.VMEM((n_loc, ffn, model), BF16),
                pltpu.VMEM((n_loc, rows, 2 * ffn), F32),
                pltpu.VMEM((tok, top_k), F32),
                pltpu.VMEM((n_dev, 2, top_k, tok), F32),
                pltpu.VMEM((n_dev, tok, n_loc * cap), BF16),
                pltpu.VMEM((2, 2, n_loc * cap, model), BF16),
                pltpu.VMEM((n_chip, tok, model), F32),
                pltpu.VMEM((n_chip, tok, model), F32),
                pltpu.VMEM((n_chip, tok, model), F32),
                pltpu.VMEM((6 * SUBS, tok, model // 2 // SUBS), F32),
                pltpu.VMEM((6 * SUBS, tok, model // 2 // SUBS), F32),
                dma((8,)), dma((n_dev - 1,)), dma((n_dev - 1,)), dma((13,)), dma((13,)),
                dma((2 * n_chip,)), dma((2 * n_chip,)), dma((6 * SUBS,)), dma((6 * SUBS,)),
            ],
            compiler_params=pltpu.CompilerParams(collective_id=0, has_side_effects=True, vmem_limit_bytes=44 * 1024 * 1024),
            name="exchange",
        )(pair_counts, gate_vals.T, topk_idx.T, slot_ids.T, grad_y, y_routed, h_gate, h_up, w_gate, w_up, w_down, x_disp)
        js = 2
        gx, gg, gwg, gwu, gwd = pl.pallas_call(
            functools.partial(weight_kernel, js),
            out_shape=(jax.ShapeDtypeStruct((tok, model), BF16), jax.ShapeDtypeStruct((top_k, tok), F32), jax.ShapeDtypeStruct((n_loc, model, ffn), F32),
                       jax.ShapeDtypeStruct((n_loc, model, ffn), F32), jax.ShapeDtypeStruct((n_loc, ffn, model), F32)),
            in_specs=[vm] * 6,
            out_specs=(vm, vm, hbm, hbm, hbm),
            scratch_shapes=[pltpu.VMEM((2, model // js, 2 * ffn), F32), pltpu.VMEM((2, ffn // js, model), F32), dma((2, 3))],
            compiler_params=pltpu.CompilerParams(vmem_limit_bytes=20 * 1024 * 1024),
            name="weights",
        )(x_rows, dh, act, d_rows, gx, gg)
        return gx, gg.T, gwg, gwu, gwd

    return jax.shard_map(local_step, mesh=mesh, in_specs=(rows_spec, rows_spec, rows_spec, rows_spec, rows_spec, cube_spec, cube_spec, cube_spec, cube_spec, weight_spec, weight_spec, weight_spec), out_specs=(rows_spec, rows_spec, cube_spec, cube_spec, cube_spec), check_vma=False)
```

```python
import functools

import jax
import jax.numpy as jnp
from jax import lax
from jax.experimental import pallas as pl
from jax.experimental.pallas import tpu as pltpu
from jax.sharding import PartitionSpec as P

MESH = pl.DeviceIdType.MESH
F32 = jnp.float32
BF16 = jnp.bfloat16
NT = (((1,), (1,)), ((), ()))
TN = (((0,), (0,)), ((), ()))
SUBS = 4


def exchange_kernel(n_dev, cap, counts_hbm, gates_hbm, idx_hbm, slot_hbm, gy_hbm, yr_hbm, h1_hbm, h3_hbm, wg_hbm, wu_hbm, wd_hbm, x_hbm,
                    base_out, tail_r, tail_l, gg_out, d_buf, dh_buf, a_buf, x_buf,
                    counts, idx, slot, gy_all, yr, h1, h3, wcat, wd, fs, gg_rows, meta, pt, rbuf, own, psend, pairin, rsend, rrecv,
                    loc_sem, meta_ssem, meta_rsem, ag_ssem, ag_rsem, pair_ssem, pair_rsem, ring_ssem, ring_rsem):
    n_loc, ffn, model = wd.shape
    top_k, tok = idx.shape
    n_chip = n_dev // 2
    half = model // 2
    hrow = tok // 2
    me = lax.axis_index("ep")
    x = me // 2
    c = me % 2
    partner = x * 2 + (1 - c)

    def chip(d):
        return (x + d + n_chip) % n_chip

    def dev(i):
        return {"ep": i}

    def load(src, dst, s):
        cp = pltpu.make_async_copy(src, dst, loc_sem.at[s])
        cp.start()
        return cp

    ld_small = (load(counts_hbm, counts, 8), load(idx_hbm, idx, 9), load(slot_hbm, slot, 10), load(gates_hbm, meta.at[me, 0], 11))
    ld_gy = load(gy_hbm, gy_all.at[me], 0)
    ld_h1 = load(h1_hbm, h1, 2)
    ld_h3 = load(h3_hbm, h3, 3)
    ld_wd = load(wd_hbm, wd, 4)
    ld_wg = load(wg_hbm, wcat.at[:, :, pl.ds(0, ffn)], 5)
    ld_wu = load(wu_hbm, wcat.at[:, :, pl.ds(ffn, ffn)], 6)

    barrier = pltpu.get_barrier_semaphore()
    for r in range(1, n_dev):
        pl.semaphore_signal(barrier, inc=1, device_id=dev((me + r) % n_dev), device_id_type=MESH)

    for cp in ld_small:
        cp.wait()
    cnt = jnp.zeros(idx.shape, jnp.int32)
    for e in range(n_loc * n_dev):
        cnt = jnp.where(idx[...] == e, counts[0, e], cnt)
    keep = (slot[...] >= 0) & (slot[...] < cnt)
    meta[me, 1] = jnp.where(keep, idx[...] * cap + slot[...], -1).astype(F32)
    pl.semaphore_wait(barrier, n_dev - 1)

    meta_cp = []
    for r in range(1, n_dev):
        cp = pltpu.make_async_remote_copy(src_ref=meta.at[me], dst_ref=meta.at[me], send_sem=meta_ssem.at[r - 1], recv_sem=meta_rsem.at[r - 1],
                                          device_id=dev((me + r) % n_dev), device_id_type=MESH)
        cp.start()
        meta_cp.append(cp)

    def gy_copy(block, lo, n, s, to):
        ref = gy_all.at[block, pl.ds(lo, n), :]
        return pltpu.make_async_remote_copy(src_ref=ref, dst_ref=ref, send_sem=ag_ssem.at[s], recv_sem=ag_rsem.at[s], device_id=dev(to), device_id_type=MESH)

    right = chip(1) * 2 + c
    left = chip(-1) * 2 + c
    far = chip(2) * 2 + c
    ld_gy.wait()
    to_r0 = gy_copy(me, 0, hrow, 0, right)
    to_l1 = gy_copy(me, hrow, hrow, 1, left)
    to_r1 = gy_copy(me, hrow, hrow, 2, right)
    to_l0 = gy_copy(me, 0, hrow, 3, left)
    to_p = gy_copy(me, 0, tok, 4, partner)
    for cp in (to_r0, to_l1, to_p, to_r1, to_l0):
        cp.start()
    fw_r = gy_copy(left, 0, hrow, 5, right)
    fw_l = gy_copy(right, hrow, hrow, 6, left)
    p_l0 = gy_copy(left, 0, hrow, 7, partner)
    p_r1 = gy_copy(right, hrow, hrow, 8, partner)
    p_l1 = gy_copy(left, hrow, hrow, 9, partner)
    p_r0 = gy_copy(right, 0, hrow, 10, partner)
    p_f0 = gy_copy(far, 0, hrow, 11, partner)
    p_f1 = gy_copy(far, hrow, hrow, 12, partner)

    ld_h1.wait()
    ld_h3.wait()
    rstep = 32

    @pl.loop(0, n_loc * (h1.shape[1] // rstep))
    def _(i):
        e = i // (h1.shape[1] // rstep)
        r = pl.multiple_of((i % (h1.shape[1] // rstep)) * rstep, rstep)
        a = h1[e, pl.ds(r, rstep), :].astype(F32)
        b = h3[e, pl.ds(r, rstep), :].astype(F32)
        g = jax.nn.sigmoid(a)
        s = a * g
        a_buf[e, pl.ds(r, rstep), :] = (s * b).astype(BF16)
        fs[e, pl.ds(r, rstep), pl.ds(0, ffn)] = b * g * (1.0 + a * (1.0 - g))
        fs[e, pl.ds(r, rstep), pl.ds(ffn, ffn)] = s


    def build(h):
        rel = meta[h, 1] - (me * (n_loc * cap)).astype(F32)
        gate = meta[h, 0]
        rows = lax.broadcasted_iota(jnp.int32, (n_loc * cap, tok), 0).astype(F32)
        sel = jnp.zeros((n_loc * cap, tok), F32)
        gsel = jnp.zeros((n_loc * cap, tok), F32)
        for k in range(top_k):
            hit = rows == rel[k:k + 1, :]
            sel = jnp.where(hit, 1.0, sel)
            gsel = jnp.where(hit, gate[k:k + 1, :], gsel)
        grow = jnp.sum(gsel, axis=1, keepdims=True)
        pt[h] = sel.T.astype(BF16)
        picked = jnp.dot(sel.astype(BF16), gy_all[h], preferred_element_type=F32)
        rows_d = (grow * picked).astype(BF16)
        for e in range(n_loc):
            d_buf[e, pl.ds(pl.multiple_of(h * cap, cap), cap), :] = rows_d[e * cap:(e + 1) * cap]

    def pair_copy(q, s, lo):
        return pltpu.make_async_remote_copy(src_ref=psend.at[q, lo], dst_ref=pairin.at[q, lo],
                                            send_sem=pair_ssem.at[s], recv_sem=pair_rsem.at[s], device_id=dev(partner), device_id_type=MESH)

    def rows_of(ref, e, q):
        return ref[e, pl.ds(pl.multiple_of(q * (2 * cap), 2 * cap), 2 * cap), :]

    def hidden(qs):
        @pl.loop(0, n_loc)
        def _(e):
            d = jnp.concatenate([rows_of(d_buf, e, q) for q in qs], axis=0)
            da = lax.dot_general(d, wd[e], NT, preferred_element_type=F32).astype(BF16).astype(F32)
            da2 = jnp.concatenate([da, da], axis=1)
            for i, q in enumerate(qs):
                dh = (da2[i * 2 * cap:(i + 1) * 2 * cap] * rows_of(fs, e, q)).astype(BF16)
                dh_buf[e, pl.ds(pl.multiple_of(q * (2 * cap), 2 * cap), 2 * cap), :] = dh

    pair_cps = {}

    chunk = model // SUBS

    def back(dists, qs, hf):
        cols = pl.ds(hf * chunk, chunk)

        @pl.loop(0, n_loc)
        def _(e):
            dh = jnp.concatenate([rows_of(dh_buf, e, q) for q in qs], axis=0)
            r = lax.dot_general(dh, wcat[e, cols, :], NT, preferred_element_type=F32).astype(BF16)
            for i in range(len(qs)):
                for j in range(2):
                    rbuf[i, j, pl.ds(pl.multiple_of(e * cap, cap), cap), :] = r[(i * 2 + j) * cap:(i * 2 + j + 1) * cap]

        for i, q in enumerate(qs):
            psend[q, hf] = jnp.dot(pt[q * 2 + 1 - c], rbuf[i, 1 - c], preferred_element_type=F32)
        for i, d in enumerate(dists):
            cp = pair_copy(qs[i], ((d + n_chip) % n_chip) * SUBS + hf, hf)
            cp.start()
            pair_cps[d, hf] = cp
        for i, q in enumerate(qs):
            own[q, hf] = jnp.dot(pt[q * 2 + c], rbuf[i, c], preferred_element_type=F32)

    width = half // SUBS

    def ring_copy(dr, st, s):
        k = (dr * 2 + st) * SUBS + s
        return pltpu.make_async_remote_copy(src_ref=rsend.at[k], dst_ref=rrecv.at[k], send_sem=ring_ssem.at[k], recv_sem=ring_rsem.at[k],
                                            device_id=dev(right if dr == 0 else left), device_id_type=MESH)

    ring = {(dr, st, s): ring_copy(dr, st, s) for dr in range(2) for st in range(2) for s in range(SUBS)}
    dest = {0: (-1, 2, 1), 1: (1, 2, -1)}
    tails = (tail_r, tail_l)
    waited = set()

    def pair_sum(d, s, dr):
        if (d, s) not in waited:
            waited.add((d, s))
            pair_cps[d, s].wait_recv()
        q = chip(d)
        cols = pl.ds(dr * width, width)
        return own[q, s, :, cols] + pairin[q, s, :, cols]

    def ring_step(st, s):
        for dr in range(2):
            v = pair_sum(dest[dr][st], s, dr)
            if st > 0:
                ring[dr, st - 1, s].wait_recv()
                v = v + rrecv[(dr * 2 + st - 1) * SUBS + s]
            if st < 2:
                rsend[(dr * 2 + st) * SUBS + s] = v
                ring[dr, st, s].start()
            else:
                tails[dr][s] = v

    for cp in meta_cp:
        cp.wait_recv()
    to_p.wait_recv()
    build(x * 2)
    build(x * 2 + 1)
    to_r0.wait_recv()
    fw_r.start()
    p_l0.start()
    to_l1.wait_recv()
    fw_l.start()
    p_r1.start()
    to_r1.wait_recv()
    p_l1.start()
    to_l0.wait_recv()
    p_r0.start()
    build(left)
    build(right)
    p_l0.wait_recv()
    p_l1.wait_recv()
    build(chip(-1) * 2 + 1 - c)
    p_r0.wait_recv()
    p_r1.wait_recv()
    build(chip(1) * 2 + 1 - c)
    ld_wd.wait()
    near = [chip(-1), chip(1)]
    hidden(near)
    fw_r.wait_recv()
    p_f0.start()
    fw_l.wait_recv()
    p_f1.start()
    ld_wg.wait()
    ld_wu.wait()
    ld_x = load(x_hbm, x_buf, 7)
    ld_yr = load(yr_hbm, yr, 1)
    back((-1, 1), near, 0)
    for s in range(1, SUBS):
        back((-1, 1), near, s)
        ring_step(0, s - 1)
    ring_step(0, SUBS - 1)
    build(far)
    p_f0.wait_recv()
    p_f1.wait_recv()
    build(chip(2) * 2 + 1 - c)
    rest = [chip(2), x]
    hidden(rest)
    back((2, 0), rest, 0)
    for s in range(1, SUBS):
        back((2, 0), rest, s)
        ring_step(1, s - 1)
    ring_step(1, SUBS - 1)

    ld_yr.wait()
    step = 16

    @pl.loop(0, tok // step)
    def _(i):
        t = pl.multiple_of(i * step, step)
        g = gy_all[me, pl.ds(t, step), :].astype(F32)
        y = yr[pl.ds(t, step), :, :].astype(F32)
        gg_rows[pl.ds(t, step), :] = jnp.sum(y * g[:, None, :], axis=2)

    gg_out[...] = gg_rows[...].T

    for s in range(SUBS):
        for dr in range(2):
            base_out[s, :, pl.ds(dr * width, width)] = pair_sum(0, s, dr)
    for s in range(SUBS):
        ring_step(2, s)

    for cp in meta_cp + [to_r0, to_l1, to_r1, to_l0, to_p, fw_r, fw_l, p_l0, p_r1, p_l1, p_r0, p_f0, p_f1]:
        cp.wait_send()
    for cp in pair_cps.values():
        cp.wait_send()
    for cp in ring.values():
        cp.wait_send()
    ld_x.wait()


def weight_kernel(js, x_ref, dh_ref, a_ref, d_ref, gg_ref, gg_out, gwg, gwu, gwd, gbuf, dbuf, sem):
    n_loc, model, ffn = gwg.shape
    xc, ac = model // js, ffn // js
    gg_out[...] = gg_ref[...]

    def copies(i):
        e, j, b = i // js, i % js, i % 2
        rows, arows = pl.ds(pl.multiple_of(j * xc, xc), xc), pl.ds(pl.multiple_of(j * ac, ac), ac)
        return (pltpu.make_async_copy(gbuf.at[b, :, pl.ds(0, ffn)], gwg.at[e, rows, :], sem.at[b, 0]),
                pltpu.make_async_copy(gbuf.at[b, :, pl.ds(ffn, ffn)], gwu.at[e, rows, :], sem.at[b, 1]),
                pltpu.make_async_copy(dbuf.at[b], gwd.at[e, arows, :], sem.at[b, 2]))

    @pl.loop(0, n_loc * js)
    def _(i):
        e, j, b = i // js, i % js, i % 2

        @pl.when(i >= 2)
        def _():
            for cp in copies(i - 2):
                cp.wait()

        gbuf[b] = lax.dot_general(x_ref[e, :, pl.ds(pl.multiple_of(j * xc, xc), xc)], dh_ref[e], TN, preferred_element_type=F32)
        dbuf[b] = lax.dot_general(a_ref[e, :, pl.ds(pl.multiple_of(j * ac, ac), ac)], d_ref[e], TN, preferred_element_type=F32)
        for cp in copies(i):
            cp.start()

    for i in range(n_loc * js - 2, n_loc * js):
        for cp in copies(i):
            cp.wait()


def finish_kernel(base, from_l, from_r, gx_out):
    width = from_l.shape[2]
    for s in range(SUBS):
        for dr, ref in enumerate((from_l, from_r)):
            gx_out[:, pl.ds((2 * s + dr) * width, width)] = (base[s, :, pl.ds(dr * width, width)] + ref[s]).astype(BF16)


def solution(mesh):
    n_dev = mesh.shape["ep"]
    rows_spec = P(("dp", "ep"), None)
    cube_spec = P(("dp", "ep"), None, None)
    weight_spec = P("ep", None, None)

    def local_step(grad_y, gate_vals, topk_idx, slot_ids, pair_counts, y_routed, x_disp, h_gate, h_up, w_gate, w_up, w_down):
        n_loc, ffn, model = w_down.shape
        tok, top_k = topk_idx.shape
        rows = x_disp.shape[1]
        cap = rows // n_dev
        n_chip = n_dev // 2
        vm = pl.BlockSpec(memory_space=pltpu.VMEM)
        hbm = pl.BlockSpec(memory_space=pl.ANY)
        dma = pltpu.SemaphoreType.DMA
        vs = pltpu.VMEM
        tail = vs((SUBS, tok, model // 2 // SUBS), F32)
        base, tail_r, tail_l, gg, d_rows, dh, act, x_rows = pl.pallas_call(
            functools.partial(exchange_kernel, n_dev, cap),
            out_shape=(vs((SUBS, tok, model // SUBS), F32), tail, tail, pltpu.VMEM((top_k, tok), F32), pltpu.VMEM((n_loc, rows, model), BF16),
                       pltpu.VMEM((n_loc, rows, 2 * ffn), BF16), pltpu.VMEM((n_loc, rows, ffn), BF16), pltpu.VMEM((n_loc, rows, model), BF16)),
            in_specs=[hbm] * 12,
            out_specs=(vm,) * 8,
            scratch_shapes=[
                pltpu.SMEM(pair_counts.shape, jnp.int32),
                pltpu.VMEM((top_k, tok), jnp.int32),
                pltpu.VMEM((top_k, tok), jnp.int32),
                pltpu.VMEM((n_dev, tok, model), BF16),
                pltpu.VMEM((tok, top_k, model), BF16),
                pltpu.VMEM((n_loc, rows, ffn), BF16),
                pltpu.VMEM((n_loc, rows, ffn), BF16),
                pltpu.VMEM((n_loc, model, 2 * ffn), BF16),
                pltpu.VMEM((n_loc, ffn, model), BF16),
                pltpu.VMEM((n_loc, rows, 2 * ffn), F32),
                pltpu.VMEM((tok, top_k), F32),
                pltpu.VMEM((n_dev, 2, top_k, tok), F32),
                pltpu.VMEM((n_dev, tok, n_loc * cap), BF16),
                pltpu.VMEM((2, 2, n_loc * cap, model // SUBS), BF16),
                pltpu.VMEM((n_chip, SUBS, tok, model // SUBS), F32),
                pltpu.VMEM((n_chip, SUBS, tok, model // SUBS), F32),
                pltpu.VMEM((n_chip, SUBS, tok, model // SUBS), F32),
                pltpu.VMEM((4 * SUBS, tok, model // 2 // SUBS), F32),
                pltpu.VMEM((4 * SUBS, tok, model // 2 // SUBS), F32),
                dma((12,)), dma((n_dev - 1,)), dma((n_dev - 1,)), dma((13,)), dma((13,)),
                dma((SUBS * n_chip,)), dma((SUBS * n_chip,)), dma((4 * SUBS,)), dma((4 * SUBS,)),
            ],
            compiler_params=pltpu.CompilerParams(collective_id=0, has_side_effects=True, vmem_limit_bytes=44 * 1024 * 1024),
            name="exchange",
        )(pair_counts, gate_vals.T, topk_idx.T, slot_ids.T, grad_y, y_routed, h_gate, h_up, w_gate, w_up, w_down, x_disp)
        js = 2
        ring_r = [(i, ((i // 2 + 1) % n_chip) * 2 + i % 2) for i in range(n_dev)]
        from_l = lax.ppermute(tail_r, "ep", ring_r)
        from_r = lax.ppermute(tail_l, "ep", [(b, a) for a, b in ring_r])
        gg, gwg, gwu, gwd = pl.pallas_call(
            functools.partial(weight_kernel, js),
            out_shape=(jax.ShapeDtypeStruct((top_k, tok), F32), jax.ShapeDtypeStruct((n_loc, model, ffn), F32),
                       jax.ShapeDtypeStruct((n_loc, model, ffn), F32), jax.ShapeDtypeStruct((n_loc, ffn, model), F32)),
            in_specs=[vm] * 5,
            out_specs=(vm, hbm, hbm, hbm),
            scratch_shapes=[pltpu.VMEM((2, model // js, 2 * ffn), F32), pltpu.VMEM((2, ffn // js, model), F32), dma((2, 3))],
            compiler_params=pltpu.CompilerParams(vmem_limit_bytes=20 * 1024 * 1024),
            cost_estimate=pl.CostEstimate(flops=6 * n_loc * rows * model * ffn, bytes_accessed=12 * n_loc * model * ffn, transcendentals=0),
            name="weights",
        )(x_rows, dh, act, d_rows, gg)
        gx = pl.pallas_call(
            finish_kernel,
            out_shape=jax.ShapeDtypeStruct((tok, model), BF16),
            in_specs=[vm] * 3,
            out_specs=vm,
            compiler_params=pltpu.CompilerParams(vmem_limit_bytes=4 * 1024 * 1024),
            name="finish",
        )(base, from_l, from_r)
        return gx, gg.T, gwg, gwu, gwd

    return jax.shard_map(local_step, mesh=mesh, in_specs=(rows_spec, rows_spec, rows_spec, rows_spec, rows_spec, cube_spec, cube_spec, cube_spec, cube_spec, weight_spec, weight_spec, weight_spec), out_specs=(rows_spec, rows_spec, cube_spec, cube_spec, cube_spec), check_vma=False)
```

```python
import functools

import jax
import jax.numpy as jnp
from jax import lax
from jax.experimental import pallas as pl
from jax.experimental.pallas import tpu as pltpu
from jax.sharding import PartitionSpec as P

MESH = pl.DeviceIdType.MESH
F32 = jnp.float32
BF16 = jnp.bfloat16
NT = (((1,), (1,)), ((), ()))
TN = (((0,), (0,)), ((), ()))
SUBS = 4
BUFS = 4


class Once:
    def __init__(self, cp, log, remote):
        self.cp, self.log, self.remote, self.got = cp, log, remote, False

    def start(self):
        self.cp.start()
        self.log.append(self)

    def wait(self):
        if not self.got:
            self.got = True
            self.cp.wait()

    def wait_recv(self):
        if not self.got:
            self.got = True
            self.cp.wait_recv()

    def finish(self):
        if self.remote:
            self.wait_recv()
            self.cp.wait_send()
        else:
            self.wait()


def exchange_kernel(n_dev, cap, counts_hbm, gates_hbm, idx_hbm, slot_hbm, gy_hbm, yr_hbm, h1_hbm, h3_hbm, wg_hbm, wu_hbm, wd_hbm, x_hbm,
                    base_out, tail_r, tail_l, gg_out, d_buf, dh_buf, a_buf, x_buf,
                    counts, idx, slot, gy_all, yr, h1, h3, wcat, wd, fs, gg_rows, meta, pt, rbuf, own, psend, pairin, rsend, rrecv,
                    loc_sem, meta_ssem, meta_rsem, ag_ssem, ag_rsem, pair_ssem, pair_rsem, ring_ssem, ring_rsem):
    n_loc, ffn, model = wd.shape
    top_k, tok = idx.shape
    n_chip = n_dev // 2
    half = model // 2
    hrow = tok // 2
    log = []
    me = lax.axis_index("ep")
    x = me // 2
    c = me % 2
    partner = x * 2 + (1 - c)

    def chip(d):
        return (x + d + n_chip) % n_chip

    def dev(i):
        return {"ep": i}

    def load(src, dst, s):
        cp = Once(pltpu.make_async_copy(src, dst, loc_sem.at[s]), log, False)
        cp.start()
        return cp

    ld_small = (load(counts_hbm, counts, 8), load(idx_hbm, idx, 9), load(slot_hbm, slot, 10), load(gates_hbm, meta.at[me, 0], 11))
    ld_gy = load(gy_hbm, gy_all.at[me], 0)
    ld_h1 = load(h1_hbm, h1, 2)
    ld_h3 = load(h3_hbm, h3, 3)
    ld_wd = load(wd_hbm, wd, 4)
    ld_wg = load(wg_hbm, wcat.at[:, :, pl.ds(0, ffn)], 5)
    ld_wu = load(wu_hbm, wcat.at[:, :, pl.ds(ffn, ffn)], 6)

    barrier = pltpu.get_barrier_semaphore()
    for r in range(1, n_dev):
        pl.semaphore_signal(barrier, inc=1, device_id=dev((me + r) % n_dev), device_id_type=MESH)

    def gy_copy(block, lo, n, s, to):
        ref = gy_all.at[block, pl.ds(lo, n), :]
        return Once(pltpu.make_async_remote_copy(src_ref=ref, dst_ref=ref, send_sem=ag_ssem.at[s], recv_sem=ag_rsem.at[s], device_id=dev(to), device_id_type=MESH), log, True)

    right = chip(1) * 2 + c
    left = chip(-1) * 2 + c
    far = chip(2) * 2 + c
    to_r0 = gy_copy(me, 0, hrow, 0, right)
    to_l1 = gy_copy(me, hrow, hrow, 1, left)
    to_r1 = gy_copy(me, hrow, hrow, 2, right)
    to_l0 = gy_copy(me, 0, hrow, 3, left)
    to_p = gy_copy(me, 0, tok, 4, partner)
    fw_r = gy_copy(left, 0, hrow, 5, right)
    fw_l = gy_copy(right, hrow, hrow, 6, left)
    p_l0 = gy_copy(left, 0, hrow, 7, partner)
    p_r1 = gy_copy(right, hrow, hrow, 8, partner)
    p_l1 = gy_copy(left, hrow, hrow, 9, partner)
    p_r0 = gy_copy(right, 0, hrow, 10, partner)
    p_f0 = gy_copy(far, 0, hrow, 11, partner)
    p_f1 = gy_copy(far, hrow, hrow, 12, partner)

    pl.semaphore_wait(barrier, n_dev - 1)
    ld_gy.wait()
    for cp in (to_r0, to_l1, to_p):
        cp.start()

    for cp in ld_small:
        cp.wait()
    cnt = jnp.zeros(idx.shape, jnp.int32)
    for e in range(n_loc * n_dev):
        cnt = jnp.where(idx[...] == e, counts[0, e], cnt)
    keep = (slot[...] >= 0) & (slot[...] < cnt)
    meta[me, 1] = jnp.where(keep, idx[...] * cap + slot[...], -1).astype(F32)

    meta_cp = {}
    for d in range(n_chip):
        for k in range(2):
            if d == 0 and k == 0:
                continue
            s = d * 2 + k - 1
            cp = Once(pltpu.make_async_remote_copy(src_ref=meta.at[me], dst_ref=meta.at[me], send_sem=meta_ssem.at[s], recv_sem=meta_rsem.at[s],
                                                   device_id=dev(chip(d) * 2 + (c if k == 0 else 1 - c)), device_id_type=MESH), log, True)
            cp.start()
            meta_cp[d, k] = cp
    to_r1.start()
    to_l0.start()

    def meta_wait(d):
        for k in range(2):
            if (d, k) != (0, 0):
                meta_cp[(n_chip - d) % n_chip, k].wait_recv()

    ld_h1.wait()
    ld_h3.wait()
    rstep = 32

    @pl.loop(0, n_loc * (h1.shape[1] // rstep))
    def _(i):
        e = i // (h1.shape[1] // rstep)
        r = pl.multiple_of((i % (h1.shape[1] // rstep)) * rstep, rstep)
        a = h1[e, pl.ds(r, rstep), :].astype(F32)
        b = h3[e, pl.ds(r, rstep), :].astype(F32)
        g = jax.nn.sigmoid(a)
        s = a * g
        a_buf[e, pl.ds(r, rstep), :] = (s * b).astype(BF16)
        fs[e, pl.ds(r, rstep), pl.ds(0, ffn)] = b * g * (1.0 + a * (1.0 - g))
        fs[e, pl.ds(r, rstep), pl.ds(ffn, ffn)] = s


    def build(h):
        rel = meta[h, 1] - (me * (n_loc * cap)).astype(F32)
        gate = meta[h, 0]
        rows = lax.broadcasted_iota(jnp.int32, (n_loc * cap, tok), 0).astype(F32)
        sel = jnp.zeros((n_loc * cap, tok), F32)
        gsel = jnp.zeros((n_loc * cap, tok), F32)
        for k in range(top_k):
            hit = rows == rel[k:k + 1, :]
            sel = jnp.where(hit, 1.0, sel)
            gsel = jnp.where(hit, gate[k:k + 1, :], gsel)
        grow = jnp.sum(gsel, axis=1, keepdims=True)
        pt[h] = sel.T.astype(BF16)
        picked = jnp.dot(sel.astype(BF16), gy_all[h], preferred_element_type=F32)
        rows_d = (grow * picked).astype(BF16)
        for e in range(n_loc):
            d_buf[e, pl.ds(pl.multiple_of(h * cap, cap), cap), :] = rows_d[e * cap:(e + 1) * cap]

    def pair_copy(q, s, lo):
        return Once(pltpu.make_async_remote_copy(src_ref=psend.at[q, lo], dst_ref=pairin.at[q, lo],
                                                 send_sem=pair_ssem.at[s], recv_sem=pair_rsem.at[s], device_id=dev(partner), device_id_type=MESH), log, True)

    def rows_of(ref, e, q):
        return ref[e, pl.ds(pl.multiple_of(q * (2 * cap), 2 * cap), 2 * cap), :]

    def hidden(qs):
        @pl.loop(0, n_loc)
        def _(e):
            d = jnp.concatenate([rows_of(d_buf, e, q) for q in qs], axis=0)
            da = lax.dot_general(d, wd[e], NT, preferred_element_type=F32).astype(BF16).astype(F32)
            da2 = jnp.concatenate([da, da], axis=1)
            for i, q in enumerate(qs):
                dh = (da2[i * 2 * cap:(i + 1) * 2 * cap] * rows_of(fs, e, q)).astype(BF16)
                dh_buf[e, pl.ds(pl.multiple_of(q * (2 * cap), 2 * cap), 2 * cap), :] = dh

    pair_cps = {}

    chunk = model // SUBS

    def back(dists, qs, hf):
        cols = pl.ds(hf * chunk, chunk)

        @pl.loop(0, n_loc)
        def _(e):
            dh = jnp.concatenate([rows_of(dh_buf, e, q) for q in qs], axis=0)
            r = lax.dot_general(dh, wcat[e, cols, :], NT, preferred_element_type=F32).astype(BF16)
            for i in range(len(qs)):
                for j in range(2):
                    rbuf[i, j, pl.ds(pl.multiple_of(e * cap, cap), cap), :] = r[(i * 2 + j) * cap:(i * 2 + j + 1) * cap]

        for i, q in enumerate(qs):
            psend[q, hf] = jnp.dot(pt[q * 2 + 1 - c], rbuf[i, 1 - c], preferred_element_type=F32)
        for i, d in enumerate(dists):
            cp = pair_copy(qs[i], ((d + n_chip) % n_chip) * SUBS + hf, hf)
            cp.start()
            pair_cps[d, hf] = cp
        for i, q in enumerate(qs):
            own[q, hf] = jnp.dot(pt[q * 2 + c], rbuf[i, c], preferred_element_type=F32)

    width = half // SUBS

    def ring_copy(dr, st, s):
        k = (dr * 2 + st) * SUBS + s
        return Once(pltpu.make_async_remote_copy(src_ref=rsend.at[k], dst_ref=rrecv.at[k], send_sem=ring_ssem.at[k], recv_sem=ring_rsem.at[k],
                                                 device_id=dev(right if dr == 0 else left), device_id_type=MESH), log, True)

    ring = {(dr, st, s): ring_copy(dr, st, s) for dr in range(2) for st in range(2) for s in range(SUBS)}
    dest = {0: (-1, 2, 1), 1: (1, 2, -1)}
    tails = (tail_r, tail_l)

    def pair_sum(d, s, dr):
        pair_cps[d, s].wait_recv()
        q = chip(d)
        cols = pl.ds(dr * width, width)
        return own[q, s, :, cols] + pairin[q, s, :, cols]

    def ring_step(st, s):
        for dr in range(2):
            v = pair_sum(dest[dr][st], s, dr)
            if st > 0:
                ring[dr, st - 1, s].wait_recv()
                v = v + rrecv[(dr * 2 + st - 1) * SUBS + s]
            if st < 2:
                rsend[(dr * 2 + st) * SUBS + s] = v
                ring[dr, st, s].start()
            else:
                tails[dr][s] = v

    def finish():
        for cp in log:
            cp.finish()

    meta_wait(0)
    to_p.wait_recv()
    build(x * 2)
    build(x * 2 + 1)
    to_r0.wait_recv()
    fw_r.start()
    p_l0.start()
    to_l1.wait_recv()
    fw_l.start()
    p_r1.start()
    ld_wd.wait()
    hidden([x])
    ld_wg.wait()
    ld_wu.wait()
    back((0,), [x], 0)
    to_r1.wait_recv()
    p_l1.start()
    to_l0.wait_recv()
    p_r0.start()
    ld_x = load(x_hbm, x_buf, 7)
    ld_yr = load(yr_hbm, yr, 1)
    meta_wait(-1)
    meta_wait(1)
    build(left)
    build(right)
    back((0,), [x], 1)
    p_l0.wait_recv()
    p_l1.wait_recv()
    build(chip(-1) * 2 + 1 - c)
    p_r0.wait_recv()
    p_r1.wait_recv()
    build(chip(1) * 2 + 1 - c)
    near = [chip(-1), chip(1)]
    hidden(near)
    back((-1, 1), near, 0)
    back((-1, 1), near, 1)
    fw_r.wait_recv()
    p_f0.start()
    fw_l.wait_recv()
    p_f1.start()
    ring_step(0, 0)
    for s in range(2, SUBS):
        back((-1, 1), near, s)
        ring_step(0, s - 1)
    meta_wait(2)
    build(far)
    ring_step(0, SUBS - 1)
    p_f0.wait_recv()
    p_f1.wait_recv()
    build(chip(2) * 2 + 1 - c)
    hidden([chip(2)])
    back((2,), [chip(2)], 0)
    for s in range(1, SUBS):
        back((2,), [chip(2)], s)
        ring_step(1, s - 1)
    ring_step(1, SUBS - 1)
    for s in range(2, SUBS):
        back((0,), [x], s)

    ld_yr.wait()
    step = 16

    @pl.loop(0, tok // step)
    def _(i):
        t = pl.multiple_of(i * step, step)
        g = gy_all[me, pl.ds(t, step), :].astype(F32)
        y = yr[pl.ds(t, step), :, :].astype(F32)
        gg_rows[pl.ds(t, step), :] = jnp.sum(y * g[:, None, :], axis=2)

    gg_out[...] = gg_rows[...].T

    for s in range(SUBS):
        for dr in range(2):
            base_out[s, :, pl.ds(dr * width, width)] = pair_sum(0, s, dr)
    for s in range(SUBS):
        ring_step(2, s)

    finish()


def weight_kernel(js, x_ref, dh_ref, a_ref, d_ref, gg_ref, gg_out, gwg, gwu, gwd, gbuf, dbuf, sem):
    n_loc, model, ffn = gwg.shape
    xc, ac = model // js, ffn // js
    gg_out[...] = gg_ref[...]

    def copies(i):
        e, j, b = i // js, i % js, i % BUFS
        rows, arows = pl.ds(pl.multiple_of(j * xc, xc), xc), pl.ds(pl.multiple_of(j * ac, ac), ac)
        return (pltpu.make_async_copy(gbuf.at[b, :, pl.ds(0, ffn)], gwg.at[e, rows, :], sem.at[b, 0]),
                pltpu.make_async_copy(gbuf.at[b, :, pl.ds(ffn, ffn)], gwu.at[e, rows, :], sem.at[b, 1]),
                pltpu.make_async_copy(dbuf.at[b], gwd.at[e, arows, :], sem.at[b, 2]))

    @pl.loop(0, n_loc * js)
    def _(i):
        e, j, b = i // js, i % js, i % BUFS

        @pl.when(i >= BUFS)
        def _():
            for cp in copies(i - BUFS):
                cp.wait()

        gbuf[b] = lax.dot_general(x_ref[e, :, pl.ds(pl.multiple_of(j * xc, xc), xc)], dh_ref[e], TN, preferred_element_type=F32)
        dbuf[b] = lax.dot_general(a_ref[e, :, pl.ds(pl.multiple_of(j * ac, ac), ac)], d_ref[e], TN, preferred_element_type=F32)
        for cp in copies(i):
            cp.start()

    for i in range(n_loc * js - BUFS, n_loc * js):
        for cp in copies(i):
            cp.wait()


def finish_kernel(base, from_l, from_r, gx_out):
    width = from_l.shape[2]
    for s in range(SUBS):
        for dr, ref in enumerate((from_l, from_r)):
            gx_out[:, pl.ds((2 * s + dr) * width, width)] = (base[s, :, pl.ds(dr * width, width)] + ref[s]).astype(BF16)


def solution(mesh):
    n_dev = mesh.shape["ep"]
    rows_spec = P(("dp", "ep"), None)
    cube_spec = P(("dp", "ep"), None, None)
    weight_spec = P("ep", None, None)

    def local_step(grad_y, gate_vals, topk_idx, slot_ids, pair_counts, y_routed, x_disp, h_gate, h_up, w_gate, w_up, w_down):
        n_loc, ffn, model = w_down.shape
        tok, top_k = topk_idx.shape
        rows = x_disp.shape[1]
        cap = rows // n_dev
        n_chip = n_dev // 2
        vm = pl.BlockSpec(memory_space=pltpu.VMEM)
        hbm = pl.BlockSpec(memory_space=pl.ANY)
        dma = pltpu.SemaphoreType.DMA
        vs = pltpu.VMEM
        tail = vs((SUBS, tok, model // 2 // SUBS), F32)
        base, tail_r, tail_l, gg, d_rows, dh, act, x_rows = pl.pallas_call(
            functools.partial(exchange_kernel, n_dev, cap),
            out_shape=(vs((SUBS, tok, model // SUBS), F32), tail, tail, pltpu.VMEM((top_k, tok), F32), pltpu.VMEM((n_loc, rows, model), BF16),
                       pltpu.VMEM((n_loc, rows, 2 * ffn), BF16), pltpu.VMEM((n_loc, rows, ffn), BF16), pltpu.VMEM((n_loc, rows, model), BF16)),
            in_specs=[hbm] * 12,
            out_specs=(vm,) * 8,
            scratch_shapes=[
                pltpu.SMEM(pair_counts.shape, jnp.int32),
                pltpu.VMEM((top_k, tok), jnp.int32),
                pltpu.VMEM((top_k, tok), jnp.int32),
                pltpu.VMEM((n_dev, tok, model), BF16),
                pltpu.VMEM((tok, top_k, model), BF16),
                pltpu.VMEM((n_loc, rows, ffn), BF16),
                pltpu.VMEM((n_loc, rows, ffn), BF16),
                pltpu.VMEM((n_loc, model, 2 * ffn), BF16),
                pltpu.VMEM((n_loc, ffn, model), BF16),
                pltpu.VMEM((n_loc, rows, 2 * ffn), F32),
                pltpu.VMEM((tok, top_k), F32),
                pltpu.VMEM((n_dev, 2, top_k, tok), F32),
                pltpu.VMEM((n_dev, tok, n_loc * cap), BF16),
                pltpu.VMEM((2, 2, n_loc * cap, model // SUBS), BF16),
                pltpu.VMEM((n_chip, SUBS, tok, model // SUBS), F32),
                pltpu.VMEM((n_chip, SUBS, tok, model // SUBS), F32),
                pltpu.VMEM((n_chip, SUBS, tok, model // SUBS), F32),
                pltpu.VMEM((4 * SUBS, tok, model // 2 // SUBS), F32),
                pltpu.VMEM((4 * SUBS, tok, model // 2 // SUBS), F32),
                dma((12,)), dma((n_dev - 1,)), dma((n_dev - 1,)), dma((13,)), dma((13,)),
                dma((SUBS * n_chip,)), dma((SUBS * n_chip,)), dma((4 * SUBS,)), dma((4 * SUBS,)),
            ],
            compiler_params=pltpu.CompilerParams(collective_id=0, has_side_effects=True, vmem_limit_bytes=44 * 1024 * 1024),
            name="exchange",
        )(pair_counts, gate_vals.T, topk_idx.T, slot_ids.T, grad_y, y_routed, h_gate, h_up, w_gate, w_up, w_down, x_disp)
        js = 4
        ring_r = [(i, ((i // 2 + 1) % n_chip) * 2 + i % 2) for i in range(n_dev)]
        from_l = lax.ppermute(tail_r, "ep", ring_r)
        from_r = lax.ppermute(tail_l, "ep", [(b, a) for a, b in ring_r])
        gg, gwg, gwu, gwd = pl.pallas_call(
            functools.partial(weight_kernel, js),
            out_shape=(jax.ShapeDtypeStruct((top_k, tok), F32), jax.ShapeDtypeStruct((n_loc, model, ffn), F32),
                       jax.ShapeDtypeStruct((n_loc, model, ffn), F32), jax.ShapeDtypeStruct((n_loc, ffn, model), F32)),
            in_specs=[vm] * 5,
            out_specs=(vm, hbm, hbm, hbm),
            scratch_shapes=[pltpu.VMEM((BUFS, model // js, 2 * ffn), F32), pltpu.VMEM((BUFS, ffn // js, model), F32), dma((BUFS, 3))],
            compiler_params=pltpu.CompilerParams(vmem_limit_bytes=20 * 1024 * 1024),
            cost_estimate=pl.CostEstimate(flops=6 * n_loc * rows * model * ffn, bytes_accessed=12 * n_loc * model * ffn, transcendentals=0),
            name="weights",
        )(x_rows, dh, act, d_rows, gg)
        gx = pl.pallas_call(
            finish_kernel,
            out_shape=jax.ShapeDtypeStruct((tok, model), BF16),
            in_specs=[vm] * 3,
            out_specs=vm,
            compiler_params=pltpu.CompilerParams(vmem_limit_bytes=4 * 1024 * 1024),
            name="finish",
        )(base, from_l, from_r)
        return gx, gg.T, gwg, gwu, gwd

    return jax.shard_map(local_step, mesh=mesh, in_specs=(rows_spec, rows_spec, rows_spec, rows_spec, rows_spec, cube_spec, cube_spec, cube_spec, cube_spec, weight_spec, weight_spec, weight_spec), out_specs=(rows_spec, rows_spec, cube_spec, cube_spec, cube_spec), check_vma=False)
```

```python
import functools

import jax
import jax.numpy as jnp
from jax import lax
from jax.experimental import pallas as pl
from jax.experimental.pallas import tpu as pltpu
from jax.sharding import PartitionSpec as P

MESH = pl.DeviceIdType.MESH
F32 = jnp.float32
BF16 = jnp.bfloat16
NT = (((1,), (1,)), ((), ()))
TN = (((0,), (0,)), ((), ()))
SUBS = 4
BUFS = 3


class Once:
    def __init__(self, cp, log, remote):
        self.cp, self.log, self.remote, self.got = cp, log, remote, False

    def start(self):
        self.cp.start()
        self.log.append(self)

    def wait(self):
        if not self.got:
            self.got = True
            self.cp.wait()

    def wait_recv(self):
        if not self.got:
            self.got = True
            self.cp.wait_recv()

    def finish(self):
        if self.remote:
            self.wait_recv()
            self.cp.wait_send()
        else:
            self.wait()


def exchange_kernel(n_dev, cap, counts_hbm, gates_hbm, idx_hbm, slot_hbm, gy_hbm, yr_hbm, h1_hbm, h3_hbm, wg_hbm, wu_hbm, wd_hbm, x_hbm,
                    base_out, tail_r, tail_l, gg_out, d_buf, dh_buf, a_buf, x_buf,
                    counts, idx, slot, gy_all, yr, h1, h3, wcat, wd, fs, gg_rows, meta, pt, rbuf, own, psend, pairin, rsend, rrecv,
                    loc_sem, meta_ssem, meta_rsem, ag_ssem, ag_rsem, pair_ssem, pair_rsem, ring_ssem, ring_rsem):
    n_loc, ffn, model = wd.shape
    top_k, tok = idx.shape
    n_chip = n_dev // 2
    half = model // 2
    hrow = tok // 2
    log = []
    me = lax.axis_index("ep")
    x = me // 2
    c = me % 2
    partner = x * 2 + (1 - c)

    def chip(d):
        return (x + d + n_chip) % n_chip

    def dev(i):
        return {"ep": i}

    def load(src, dst, s):
        cp = Once(pltpu.make_async_copy(src, dst, loc_sem.at[s]), log, False)
        cp.start()
        return cp

    ld_small = (load(counts_hbm, counts, 8), load(idx_hbm, idx, 9), load(slot_hbm, slot, 10), load(gates_hbm, meta.at[me, 0], 11))
    ld_gy = load(gy_hbm, gy_all.at[me], 0)
    ld_h1 = load(h1_hbm, h1, 2)
    ld_h3 = load(h3_hbm, h3, 3)
    ld_wd = load(wd_hbm, wd, 4)
    ld_wg = load(wg_hbm, wcat.at[:, :, pl.ds(0, ffn)], 5)
    ld_wu = load(wu_hbm, wcat.at[:, :, pl.ds(ffn, ffn)], 6)

    barrier = pltpu.get_barrier_semaphore()
    for r in range(1, n_dev):
        pl.semaphore_signal(barrier, inc=1, device_id=dev((me + r) % n_dev), device_id_type=MESH)

    def gy_copy(block, lo, n, s, to):
        ref = gy_all.at[block, pl.ds(lo, n), :]
        return Once(pltpu.make_async_remote_copy(src_ref=ref, dst_ref=ref, send_sem=ag_ssem.at[s], recv_sem=ag_rsem.at[s], device_id=dev(to), device_id_type=MESH), log, True)

    right = chip(1) * 2 + c
    left = chip(-1) * 2 + c
    far = chip(2) * 2 + c
    to_r0 = gy_copy(me, 0, hrow, 0, right)
    to_l1 = gy_copy(me, hrow, hrow, 1, left)
    to_r1 = gy_copy(me, hrow, hrow, 2, right)
    to_l0 = gy_copy(me, 0, hrow, 3, left)
    to_p = gy_copy(me, 0, tok, 4, partner)
    fw_r = gy_copy(left, 0, hrow, 5, right)
    fw_l = gy_copy(right, hrow, hrow, 6, left)
    p_l0 = gy_copy(left, 0, hrow, 7, partner)
    p_r1 = gy_copy(right, hrow, hrow, 8, partner)
    p_l1 = gy_copy(left, hrow, hrow, 9, partner)
    p_r0 = gy_copy(right, 0, hrow, 10, partner)
    p_f0 = gy_copy(far, 0, hrow, 11, partner)
    p_f1 = gy_copy(far, hrow, hrow, 12, partner)

    pl.semaphore_wait(barrier, n_dev - 1)
    ld_gy.wait()
    for cp in (to_r0, to_l1, to_p):
        cp.start()

    for cp in ld_small:
        cp.wait()
    cnt = jnp.zeros(idx.shape, jnp.int32)
    for e in range(n_loc * n_dev):
        cnt = jnp.where(idx[...] == e, counts[0, e], cnt)
    keep = (slot[...] >= 0) & (slot[...] < cnt)
    meta[me, 1] = jnp.where(keep, idx[...] * cap + slot[...], -1).astype(F32)

    meta_cp = {}
    for d in range(n_chip):
        for k in range(2):
            if d == 0 and k == 0:
                continue
            s = d * 2 + k - 1
            cp = Once(pltpu.make_async_remote_copy(src_ref=meta.at[me], dst_ref=meta.at[me], send_sem=meta_ssem.at[s], recv_sem=meta_rsem.at[s],
                                                   device_id=dev(chip(d) * 2 + (c if k == 0 else 1 - c)), device_id_type=MESH), log, True)
            cp.start()
            meta_cp[d, k] = cp
    to_r1.start()
    to_l0.start()

    def meta_wait(d):
        for k in range(2):
            if (d, k) != (0, 0):
                meta_cp[(n_chip - d) % n_chip, k].wait_recv()

    ld_h1.wait()
    ld_h3.wait()
    rstep = 32

    @pl.loop(0, n_loc * (h1.shape[1] // rstep))
    def _(i):
        e = i // (h1.shape[1] // rstep)
        r = pl.multiple_of((i % (h1.shape[1] // rstep)) * rstep, rstep)
        a = h1[e, pl.ds(r, rstep), :].astype(F32)
        b = h3[e, pl.ds(r, rstep), :].astype(F32)
        g = jax.nn.sigmoid(a)
        s = a * g
        a_buf[e, pl.ds(r, rstep), :] = (s * b).astype(BF16)
        fs[e, pl.ds(r, rstep), pl.ds(0, ffn)] = b * g * (1.0 + a * (1.0 - g))
        fs[e, pl.ds(r, rstep), pl.ds(ffn, ffn)] = s


    def build(h):
        rel = meta[h, 1] - (me * (n_loc * cap)).astype(F32)
        gate = meta[h, 0]
        rows = lax.broadcasted_iota(jnp.int32, (n_loc * cap, tok), 0).astype(F32)
        sel = jnp.zeros((n_loc * cap, tok), F32)
        gsel = jnp.zeros((n_loc * cap, tok), F32)
        for k in range(top_k):
            hit = rows == rel[k:k + 1, :]
            sel = jnp.where(hit, 1.0, sel)
            gsel = jnp.where(hit, gate[k:k + 1, :], gsel)
        grow = jnp.sum(gsel, axis=1, keepdims=True)
        pt[h] = sel.T.astype(BF16)
        picked = jnp.dot(sel.astype(BF16), gy_all[h], preferred_element_type=F32)
        rows_d = (grow * picked).astype(BF16)
        for e in range(n_loc):
            d_buf[e, pl.ds(pl.multiple_of(h * cap, cap), cap), :] = rows_d[e * cap:(e + 1) * cap]

    def pair_copy(q, s, lo):
        return Once(pltpu.make_async_remote_copy(src_ref=psend.at[q, lo], dst_ref=pairin.at[q, lo],
                                                 send_sem=pair_ssem.at[s], recv_sem=pair_rsem.at[s], device_id=dev(partner), device_id_type=MESH), log, True)

    def rows_of(ref, e, q):
        return ref[e, pl.ds(pl.multiple_of(q * (2 * cap), 2 * cap), 2 * cap), :]

    def hidden(qs):
        for e in range(n_loc):
            d = jnp.concatenate([rows_of(d_buf, e, q) for q in qs], axis=0)
            da = lax.dot_general(d, wd[e], NT, preferred_element_type=F32).astype(BF16).astype(F32)
            da2 = jnp.concatenate([da, da], axis=1)
            for i, q in enumerate(qs):
                dh = (da2[i * 2 * cap:(i + 1) * 2 * cap] * rows_of(fs, e, q)).astype(BF16)
                dh_buf[e, pl.ds(pl.multiple_of(q * (2 * cap), 2 * cap), 2 * cap), :] = dh

    pair_cps = {}

    chunk = model // SUBS

    def back(dists, qs, hf):
        cols = pl.ds(hf * chunk, chunk)

        for e in range(n_loc):
            dh = jnp.concatenate([rows_of(dh_buf, e, q) for q in qs], axis=0)
            r = lax.dot_general(dh, wcat[e, cols, :], NT, preferred_element_type=F32).astype(BF16)
            for i in range(len(qs)):
                for j in range(2):
                    rbuf[i, j, pl.ds(e * cap, cap), :] = r[(i * 2 + j) * cap:(i * 2 + j + 1) * cap]

        for i, q in enumerate(qs):
            psend[q, hf] = jnp.dot(pt[q * 2 + 1 - c], rbuf[i, 1 - c], preferred_element_type=F32)
        for i, d in enumerate(dists):
            cp = pair_copy(qs[i], ((d + n_chip) % n_chip) * SUBS + hf, hf)
            cp.start()
            pair_cps[d, hf] = cp
        for i, q in enumerate(qs):
            own[q, hf] = jnp.dot(pt[q * 2 + c], rbuf[i, c], preferred_element_type=F32)

    width = half // SUBS

    def ring_copy(dr, st, s):
        k = (dr * 2 + st) * SUBS + s
        return Once(pltpu.make_async_remote_copy(src_ref=rsend.at[k], dst_ref=rrecv.at[k], send_sem=ring_ssem.at[k], recv_sem=ring_rsem.at[k],
                                                 device_id=dev(right if dr == 0 else left), device_id_type=MESH), log, True)

    ring = {(dr, st, s): ring_copy(dr, st, s) for dr in range(2) for st in range(2) for s in range(SUBS)}
    dest = {0: (-1, 2, 1), 1: (1, 2, -1)}
    tails = (tail_r, tail_l)

    def pair_sum(d, s, dr):
        pair_cps[d, s].wait_recv()
        q = chip(d)
        cols = pl.ds(dr * width, width)
        return own[q, s, :, cols] + pairin[q, s, :, cols]

    def ring_step(st, s):
        for dr in range(2):
            v = pair_sum(dest[dr][st], s, dr)
            if st > 0:
                ring[dr, st - 1, s].wait_recv()
                v = v + rrecv[(dr * 2 + st - 1) * SUBS + s]
            if st < 2:
                rsend[(dr * 2 + st) * SUBS + s] = v
                ring[dr, st, s].start()
            else:
                tails[dr][s] = v

    def finish():
        for cp in log:
            cp.finish()

    meta_wait(0)
    to_p.wait_recv()
    build(x * 2)
    build(x * 2 + 1)
    to_r0.wait_recv()
    fw_r.start()
    p_l0.start()
    to_l1.wait_recv()
    fw_l.start()
    p_r1.start()
    ld_wd.wait()
    hidden([x])
    ld_wg.wait()
    ld_wu.wait()
    back((0,), [x], 0)
    to_r1.wait_recv()
    p_l1.start()
    to_l0.wait_recv()
    p_r0.start()
    ld_x = load(x_hbm, x_buf, 7)
    ld_yr = load(yr_hbm, yr, 1)
    meta_wait(-1)
    meta_wait(1)
    build(left)
    build(right)
    back((0,), [x], 1)
    p_l0.wait_recv()
    p_l1.wait_recv()
    build(chip(-1) * 2 + 1 - c)
    p_r0.wait_recv()
    p_r1.wait_recv()
    build(chip(1) * 2 + 1 - c)
    near = [chip(-1), chip(1)]
    hidden(near)
    back((-1, 1), near, 0)
    back((-1, 1), near, 1)
    fw_r.wait_recv()
    p_f0.start()
    fw_l.wait_recv()
    p_f1.start()
    ring_step(0, 0)
    for s in range(2, SUBS):
        back((-1, 1), near, s)
        ring_step(0, s - 1)
    meta_wait(2)
    build(far)
    ring_step(0, SUBS - 1)
    p_f0.wait_recv()
    p_f1.wait_recv()
    build(chip(2) * 2 + 1 - c)
    hidden([chip(2)])
    back((2,), [chip(2)], 0)
    for s in range(1, SUBS):
        back((2,), [chip(2)], s)
        ring_step(1, s - 1)
    ring_step(1, SUBS - 1)
    for s in range(2, SUBS):
        back((0,), [x], s)

    ld_yr.wait()
    step = 16

    @pl.loop(0, tok // step)
    def _(i):
        t = pl.multiple_of(i * step, step)
        g = gy_all[me, pl.ds(t, step), :].astype(F32)
        y = yr[pl.ds(t, step), :, :].astype(F32)
        gg_rows[pl.ds(t, step), :] = jnp.sum(y * g[:, None, :], axis=2)

    gg_out[...] = gg_rows[...].T

    for s in range(SUBS):
        for dr in range(2):
            base_out[s, :, pl.ds(dr * width, width)] = pair_sum(0, s, dr)
    for s in range(SUBS):
        ring_step(2, s)

    finish()


def weight_kernel(js, x_ref, dh_ref, a_ref, d_ref, gg_ref, gg_out, gwg, gwu, gwd, gbuf, dbuf, sem):
    n_loc, model, ffn = gwg.shape
    xc, ac = model // js, ffn // js
    gg_out[...] = gg_ref[...]

    def copies(i):
        e, j, b = i // js, i % js, i % BUFS
        rows, arows = pl.ds(j * xc, xc), pl.ds(j * ac, ac)
        return (pltpu.make_async_copy(gbuf.at[b, :, pl.ds(0, ffn)], gwg.at[e, rows, :], sem.at[b, 0]),
                pltpu.make_async_copy(gbuf.at[b, :, pl.ds(ffn, ffn)], gwu.at[e, rows, :], sem.at[b, 1]),
                pltpu.make_async_copy(dbuf.at[b], gwd.at[e, arows, :], sem.at[b, 2]))

    steps = n_loc * js
    for i in range(steps):
        e, j, b = i // js, i % js, i % BUFS
        if i >= BUFS:
            for cp in copies(i - BUFS):
                cp.wait()
        gbuf[b] = lax.dot_general(x_ref[e, :, pl.ds(j * xc, xc)], dh_ref[e], TN, preferred_element_type=F32)
        dbuf[b] = lax.dot_general(a_ref[e, :, pl.ds(j * ac, ac)], d_ref[e], TN, preferred_element_type=F32)
        for cp in copies(i):
            cp.start()
    for i in range(steps - BUFS, steps):
        for cp in copies(i):
            cp.wait()


def finish_kernel(base, from_l, from_r, gx_out):
    width = from_l.shape[2]
    for s in range(SUBS):
        for dr, ref in enumerate((from_l, from_r)):
            gx_out[:, pl.ds((2 * s + dr) * width, width)] = (base[s, :, pl.ds(dr * width, width)] + ref[s]).astype(BF16)


def solution(mesh):
    n_dev = mesh.shape["ep"]
    rows_spec = P(("dp", "ep"), None)
    cube_spec = P(("dp", "ep"), None, None)
    weight_spec = P("ep", None, None)

    def local_step(grad_y, gate_vals, topk_idx, slot_ids, pair_counts, y_routed, x_disp, h_gate, h_up, w_gate, w_up, w_down):
        n_loc, ffn, model = w_down.shape
        tok, top_k = topk_idx.shape
        rows = x_disp.shape[1]
        cap = rows // n_dev
        n_chip = n_dev // 2
        vm = pl.BlockSpec(memory_space=pltpu.VMEM)
        hbm = pl.BlockSpec(memory_space=pl.ANY)
        dma = pltpu.SemaphoreType.DMA
        vs = pltpu.VMEM
        tail = vs((SUBS, tok, model // 2 // SUBS), F32)
        base, tail_r, tail_l, gg, d_rows, dh, act, x_rows = pl.pallas_call(
            functools.partial(exchange_kernel, n_dev, cap),
            out_shape=(vs((SUBS, tok, model // SUBS), F32), tail, tail, pltpu.VMEM((top_k, tok), F32), pltpu.VMEM((n_loc, rows, model), BF16),
                       pltpu.VMEM((n_loc, rows, 2 * ffn), BF16), pltpu.VMEM((n_loc, rows, ffn), BF16), pltpu.VMEM((n_loc, rows, model), BF16)),
            in_specs=[hbm] * 12,
            out_specs=(vm,) * 8,
            scratch_shapes=[
                pltpu.SMEM(pair_counts.shape, jnp.int32),
                pltpu.VMEM((top_k, tok), jnp.int32),
                pltpu.VMEM((top_k, tok), jnp.int32),
                pltpu.VMEM((n_dev, tok, model), BF16),
                pltpu.VMEM((tok, top_k, model), BF16),
                pltpu.VMEM((n_loc, rows, ffn), BF16),
                pltpu.VMEM((n_loc, rows, ffn), BF16),
                pltpu.VMEM((n_loc, model, 2 * ffn), BF16),
                pltpu.VMEM((n_loc, ffn, model), BF16),
                pltpu.VMEM((n_loc, rows, 2 * ffn), F32),
                pltpu.VMEM((tok, top_k), F32),
                pltpu.VMEM((n_dev, 2, top_k, tok), F32),
                pltpu.VMEM((n_dev, tok, n_loc * cap), BF16),
                pltpu.VMEM((2, 2, n_loc * cap, model // SUBS), BF16),
                pltpu.VMEM((n_chip, SUBS, tok, model // SUBS), F32),
                pltpu.VMEM((n_chip, SUBS, tok, model // SUBS), F32),
                pltpu.VMEM((n_chip, SUBS, tok, model // SUBS), F32),
                pltpu.VMEM((4 * SUBS, tok, model // 2 // SUBS), F32),
                pltpu.VMEM((4 * SUBS, tok, model // 2 // SUBS), F32),
                dma((12,)), dma((n_dev - 1,)), dma((n_dev - 1,)), dma((13,)), dma((13,)),
                dma((SUBS * n_chip,)), dma((SUBS * n_chip,)), dma((4 * SUBS,)), dma((4 * SUBS,)),
            ],
            compiler_params=pltpu.CompilerParams(collective_id=0, has_side_effects=True, vmem_limit_bytes=44 * 1024 * 1024),
            name="exchange",
        )(pair_counts, gate_vals.T, topk_idx.T, slot_ids.T, grad_y, y_routed, h_gate, h_up, w_gate, w_up, w_down, x_disp)
        js = 2
        ring_r = [(i, ((i // 2 + 1) % n_chip) * 2 + i % 2) for i in range(n_dev)]
        from_l = lax.ppermute(tail_r, "ep", ring_r)
        from_r = lax.ppermute(tail_l, "ep", [(b, a) for a, b in ring_r])
        gg, gwg, gwu, gwd = pl.pallas_call(
            functools.partial(weight_kernel, js),
            out_shape=(jax.ShapeDtypeStruct((top_k, tok), F32), jax.ShapeDtypeStruct((n_loc, model, ffn), F32),
                       jax.ShapeDtypeStruct((n_loc, model, ffn), F32), jax.ShapeDtypeStruct((n_loc, ffn, model), F32)),
            in_specs=[vm] * 5,
            out_specs=(vm, hbm, hbm, hbm),
            scratch_shapes=[pltpu.VMEM((BUFS, model // js, 2 * ffn), F32), pltpu.VMEM((BUFS, ffn // js, model), F32), dma((BUFS, 3))],
            compiler_params=pltpu.CompilerParams(vmem_limit_bytes=24 * 1024 * 1024),
            cost_estimate=pl.CostEstimate(flops=6 * n_loc * rows * model * ffn, bytes_accessed=12 * n_loc * model * ffn, transcendentals=0),
            name="weights",
        )(x_rows, dh, act, d_rows, gg)
        gx = pl.pallas_call(
            finish_kernel,
            out_shape=jax.ShapeDtypeStruct((tok, model), BF16),
            in_specs=[vm] * 3,
            out_specs=vm,
            compiler_params=pltpu.CompilerParams(vmem_limit_bytes=4 * 1024 * 1024),
            name="finish",
        )(base, from_l, from_r)
        return gx, gg.T, gwg, gwu, gwd

    return jax.shard_map(local_step, mesh=mesh, in_specs=(rows_spec, rows_spec, rows_spec, rows_spec, rows_spec, cube_spec, cube_spec, cube_spec, cube_spec, weight_spec, weight_spec, weight_spec), out_specs=(rows_spec, rows_spec, cube_spec, cube_spec, cube_spec), check_vma=False)
```

```python
import functools

import jax
import jax.numpy as jnp
from jax import lax
from jax.experimental import pallas as pl
from jax.experimental.pallas import tpu as pltpu
from jax.sharding import PartitionSpec as P

MESH = pl.DeviceIdType.MESH
F32 = jnp.float32
BF16 = jnp.bfloat16
NT = (((1,), (1,)), ((), ()))
TN = (((0,), (0,)), ((), ()))
SUBS = 4
BUFS = 3


class Once:
    def __init__(self, cp, log, remote):
        self.cp, self.log, self.remote, self.got = cp, log, remote, False

    def start(self):
        self.cp.start()
        self.log.append(self)

    def wait(self):
        if not self.got:
            self.got = True
            self.cp.wait()

    def wait_recv(self):
        if not self.got:
            self.got = True
            self.cp.wait_recv()

    def finish(self):
        if self.remote:
            self.wait_recv()
            self.cp.wait_send()
        else:
            self.wait()


def exchange_kernel(n_dev, cap, counts_hbm, gates_hbm, idx_hbm, slot_hbm, gy_hbm, yr_hbm, h1_hbm, h3_hbm, wg_hbm, wu_hbm, wd_hbm, x_hbm,
                    base_out, tail_r, tail_l, gg_out, d_buf, dh_buf, a_buf, x_buf,
                    counts, idx, slot, gy_all, yr, h1, h3, wcat, wd, fs, gg_rows, meta, pt, rbuf, own, psend, pairin, rsend, rrecv,
                    loc_sem, meta_ssem, meta_rsem, ag_ssem, ag_rsem, pair_ssem, pair_rsem, ring_ssem, ring_rsem):
    n_loc, ffn, model = wd.shape
    top_k, tok = idx.shape
    n_chip = n_dev // 2
    half = model // 2
    hrow = tok // 2
    log = []
    me = lax.axis_index("ep")
    x = me // 2
    c = me % 2
    partner = x * 2 + (1 - c)

    def chip(d):
        return (x + d + n_chip) % n_chip

    def dev(i):
        return {"ep": i}

    def load(src, dst, s):
        cp = Once(pltpu.make_async_copy(src, dst, loc_sem.at[s]), log, False)
        cp.start()
        return cp

    ld_gy = load(gy_hbm, gy_all.at[me], 0)
    ld_small = (load(counts_hbm, counts, 8), load(idx_hbm, idx, 9), load(slot_hbm, slot, 10), load(gates_hbm, meta.at[me, 0], 11))
    barrier = pltpu.get_barrier_semaphore()
    for r in range(1, n_dev):
        pl.semaphore_signal(barrier, inc=1, device_id=dev((me + r) % n_dev), device_id_type=MESH)

    ld_h1 = load(h1_hbm, h1, 2)
    ld_h3 = load(h3_hbm, h3, 3)

    def gy_copy(block, lo, n, s, to):
        ref = gy_all.at[block, pl.ds(lo, n), :]
        return Once(pltpu.make_async_remote_copy(src_ref=ref, dst_ref=ref, send_sem=ag_ssem.at[s], recv_sem=ag_rsem.at[s], device_id=dev(to), device_id_type=MESH), log, True)

    right = chip(1) * 2 + c
    left = chip(-1) * 2 + c
    far = chip(2) * 2 + c
    to_r0 = gy_copy(me, 0, hrow, 0, right)
    to_l1 = gy_copy(me, hrow, hrow, 1, left)
    to_r1 = gy_copy(me, hrow, hrow, 2, right)
    to_l0 = gy_copy(me, 0, hrow, 3, left)
    to_p = gy_copy(me, 0, tok, 4, partner)
    fw_r = gy_copy(left, 0, hrow, 5, right)
    fw_l = gy_copy(right, hrow, hrow, 6, left)
    p_l0 = gy_copy(left, 0, hrow, 7, partner)
    p_r1 = gy_copy(right, hrow, hrow, 8, partner)
    p_l1 = gy_copy(left, hrow, hrow, 9, partner)
    p_r0 = gy_copy(right, 0, hrow, 10, partner)
    p_f0 = gy_copy(far, 0, hrow, 11, partner)
    p_f1 = gy_copy(far, hrow, hrow, 12, partner)

    pl.semaphore_wait(barrier, n_dev - 1)
    ld_gy.wait()
    for cp in (to_r0, to_l1, to_p):
        cp.start()
    ld_wd = load(wd_hbm, wd, 4)
    ld_wg = load(wg_hbm, wcat.at[:, :, pl.ds(0, ffn)], 5)
    ld_wu = load(wu_hbm, wcat.at[:, :, pl.ds(ffn, ffn)], 6)

    for cp in ld_small:
        cp.wait()
    cnt = jnp.zeros(idx.shape, jnp.int32)
    for e in range(n_loc * n_dev):
        cnt = jnp.where(idx[...] == e, counts[0, e], cnt)
    keep = (slot[...] >= 0) & (slot[...] < cnt)
    meta[me, 1] = jnp.where(keep, idx[...] * cap + slot[...], -1).astype(F32)

    meta_cp = {}
    for d in range(n_chip):
        for k in range(2):
            if d == 0 and k == 0:
                continue
            s = d * 2 + k - 1
            cp = Once(pltpu.make_async_remote_copy(src_ref=meta.at[me], dst_ref=meta.at[me], send_sem=meta_ssem.at[s], recv_sem=meta_rsem.at[s],
                                                   device_id=dev(chip(d) * 2 + (c if k == 0 else 1 - c)), device_id_type=MESH), log, True)
            cp.start()
            meta_cp[d, k] = cp
    to_r1.start()
    to_l0.start()

    def meta_wait(d):
        for k in range(2):
            if (d, k) != (0, 0):
                meta_cp[(n_chip - d) % n_chip, k].wait_recv()

    ld_h1.wait()
    ld_h3.wait()
    rstep = 32

    @pl.loop(0, n_loc * (h1.shape[1] // rstep))
    def _(i):
        e = i // (h1.shape[1] // rstep)
        r = pl.multiple_of((i % (h1.shape[1] // rstep)) * rstep, rstep)
        a = h1[e, pl.ds(r, rstep), :].astype(F32)
        b = h3[e, pl.ds(r, rstep), :].astype(F32)
        g = jax.nn.sigmoid(a)
        s = a * g
        a_buf[e, pl.ds(r, rstep), :] = (s * b).astype(BF16)
        fs[e, pl.ds(r, rstep), pl.ds(0, ffn)] = b * g * (1.0 + a * (1.0 - g))
        fs[e, pl.ds(r, rstep), pl.ds(ffn, ffn)] = s


    def build(h):
        rel = meta[h, 1] - (me * (n_loc * cap)).astype(F32)
        gate = meta[h, 0]
        rows = lax.broadcasted_iota(jnp.int32, (n_loc * cap, tok), 0).astype(F32)
        sel = jnp.zeros((n_loc * cap, tok), F32)
        gsel = jnp.zeros((n_loc * cap, tok), F32)
        for k in range(top_k):
            hit = rows == rel[k:k + 1, :]
            sel = jnp.where(hit, 1.0, sel)
            gsel = jnp.where(hit, gate[k:k + 1, :], gsel)
        grow = jnp.sum(gsel, axis=1, keepdims=True)
        pt[h] = sel.T.astype(BF16)
        picked = jnp.dot(sel.astype(BF16), gy_all[h], preferred_element_type=F32)
        rows_d = (grow * picked).astype(BF16)
        for e in range(n_loc):
            d_buf[e, pl.ds(pl.multiple_of(h * cap, cap), cap), :] = rows_d[e * cap:(e + 1) * cap]

    def pair_copy(q, s, lo):
        return Once(pltpu.make_async_remote_copy(src_ref=psend.at[q, lo], dst_ref=pairin.at[q, lo],
                                                 send_sem=pair_ssem.at[s], recv_sem=pair_rsem.at[s], device_id=dev(partner), device_id_type=MESH), log, True)

    def rows_of(ref, e, q):
        return ref[e, pl.ds(pl.multiple_of(q * (2 * cap), 2 * cap), 2 * cap), :]

    def hidden(qs):
        for e in range(n_loc):
            d = jnp.concatenate([rows_of(d_buf, e, q) for q in qs], axis=0)
            da = lax.dot_general(d, wd[e], NT, preferred_element_type=F32).astype(BF16).astype(F32)
            da2 = jnp.concatenate([da, da], axis=1)
            for i, q in enumerate(qs):
                dh = (da2[i * 2 * cap:(i + 1) * 2 * cap] * rows_of(fs, e, q)).astype(BF16)
                dh_buf[e, pl.ds(pl.multiple_of(q * (2 * cap), 2 * cap), 2 * cap), :] = dh

    pair_cps = {}

    chunk = model // SUBS

    def back(dists, qs, hf):
        cols = pl.ds(hf * chunk, chunk)

        for e in range(n_loc):
            dh = jnp.concatenate([rows_of(dh_buf, e, q) for q in qs], axis=0)
            r = lax.dot_general(dh, wcat[e, cols, :], NT, preferred_element_type=F32).astype(BF16)
            for i in range(len(qs)):
                for j in range(2):
                    rbuf[i, j, pl.ds(e * cap, cap), :] = r[(i * 2 + j) * cap:(i * 2 + j + 1) * cap]

        for i, q in enumerate(qs):
            psend[q, hf] = jnp.dot(pt[q * 2 + 1 - c], rbuf[i, 1 - c], preferred_element_type=F32)
        for i, d in enumerate(dists):
            cp = pair_copy(qs[i], ((d + n_chip) % n_chip) * SUBS + hf, hf)
            cp.start()
            pair_cps[d, hf] = cp
        for i, q in enumerate(qs):
            own[q, hf] = jnp.dot(pt[q * 2 + c], rbuf[i, c], preferred_element_type=F32)

    width = half // SUBS

    def ring_copy(dr, st, s):
        k = (dr * 2 + st) * SUBS + s
        return Once(pltpu.make_async_remote_copy(src_ref=rsend.at[k], dst_ref=rrecv.at[k], send_sem=ring_ssem.at[k], recv_sem=ring_rsem.at[k],
                                                 device_id=dev(right if dr == 0 else left), device_id_type=MESH), log, True)

    ring = {(dr, st, s): ring_copy(dr, st, s) for dr in range(2) for st in range(2) for s in range(SUBS)}
    dest = {0: (-1, 2, 1), 1: (1, 2, -1)}
    tails = (tail_r, tail_l)

    def pair_sum(d, s, dr):
        pair_cps[d, s].wait_recv()
        q = chip(d)
        cols = pl.ds(dr * width, width)
        return own[q, s, :, cols] + pairin[q, s, :, cols]

    def ring_step(st, s):
        for dr in range(2):
            v = pair_sum(dest[dr][st], s, dr)
            if st > 0:
                ring[dr, st - 1, s].wait_recv()
                v = v + rrecv[(dr * 2 + st - 1) * SUBS + s]
            if st < 2:
                rsend[(dr * 2 + st) * SUBS + s] = v
                ring[dr, st, s].start()
            else:
                tails[dr][s] = v

    def finish():
        for cp in log:
            cp.finish()

    meta_wait(0)
    to_p.wait_recv()
    build(x * 2)
    build(x * 2 + 1)
    to_r0.wait_recv()
    fw_r.start()
    p_l0.start()
    to_l1.wait_recv()
    fw_l.start()
    p_r1.start()
    ld_wd.wait()
    hidden([x])
    ld_wg.wait()
    ld_wu.wait()
    back((0,), [x], 0)
    to_r1.wait_recv()
    p_l1.start()
    to_l0.wait_recv()
    p_r0.start()
    meta_wait(-1)
    meta_wait(1)
    build(left)
    build(right)
    back((0,), [x], 1)
    p_l0.wait_recv()
    p_l1.wait_recv()
    build(chip(-1) * 2 + 1 - c)
    p_r0.wait_recv()
    p_r1.wait_recv()
    build(chip(1) * 2 + 1 - c)
    near = [chip(-1), chip(1)]
    hidden(near)
    back((-1, 1), near, 0)
    back((-1, 1), near, 1)
    ring_step(0, 0)
    fw_r.wait_recv()
    p_f0.start()
    fw_l.wait_recv()
    p_f1.start()
    for s in range(2, SUBS):
        back((-1, 1), near, s)
        ring_step(0, s - 1)
    meta_wait(2)
    build(far)
    ring_step(0, SUBS - 1)
    ld_x = load(x_hbm, x_buf, 7)
    ld_yr = load(yr_hbm, yr, 1)
    p_f0.wait_recv()
    p_f1.wait_recv()
    build(chip(2) * 2 + 1 - c)
    hidden([chip(2)])
    back((2,), [chip(2)], 0)
    for s in range(1, SUBS):
        back((2,), [chip(2)], s)
        ring_step(1, s - 1)
    ring_step(1, SUBS - 1)
    for s in range(2, SUBS):
        back((0,), [x], s)

    ld_yr.wait()
    step = 16

    @pl.loop(0, tok // step)
    def _(i):
        t = pl.multiple_of(i * step, step)
        g = gy_all[me, pl.ds(t, step), :].astype(F32)
        y = yr[pl.ds(t, step), :, :].astype(F32)
        gg_rows[pl.ds(t, step), :] = jnp.sum(y * g[:, None, :], axis=2)

    gg_out[...] = gg_rows[...].T

    for s in range(SUBS):
        for dr in range(2):
            base_out[s, :, pl.ds(dr * width, width)] = pair_sum(0, s, dr)
    for s in range(SUBS):
        ring_step(2, s)

    finish()


def weight_kernel(js, x_ref, dh_ref, a_ref, d_ref, gg_ref, gg_out, gwg, gwu, gwd, gbuf, dbuf, sem):
    n_loc, model, ffn = gwg.shape
    xc, ac = model // js, ffn // js
    gg_out[...] = gg_ref[...]

    def copies(i):
        e, j, b = i // js, i % js, i % BUFS
        rows, arows = pl.ds(j * xc, xc), pl.ds(j * ac, ac)
        return (pltpu.make_async_copy(gbuf.at[b, :, pl.ds(0, ffn)], gwg.at[e, rows, :], sem.at[b, 0]),
                pltpu.make_async_copy(gbuf.at[b, :, pl.ds(ffn, ffn)], gwu.at[e, rows, :], sem.at[b, 1]),
                pltpu.make_async_copy(dbuf.at[b], gwd.at[e, arows, :], sem.at[b, 2]))

    def gate_up(i):
        e, j, b = i // js, i % js, i % BUFS
        if i >= BUFS:
            for cp in copies(i - BUFS)[:2]:
                cp.wait()
        gbuf[b] = lax.dot_general(x_ref[e, :, pl.ds(j * xc, xc)], dh_ref[e], TN, preferred_element_type=F32)
        for cp in copies(i)[:2]:
            cp.start()

    def down(i):
        e, j, b = i // js, i % js, i % BUFS
        if i >= BUFS:
            copies(i - BUFS)[2].wait()
        dbuf[b] = lax.dot_general(a_ref[e, :, pl.ds(j * ac, ac)], d_ref[e], TN, preferred_element_type=F32)
        copies(i)[2].start()

    steps = n_loc * js
    for i in range(steps - 1):
        down(i)
        gate_up(i)
    gate_up(steps - 1)
    down(steps - 1)
    for i in range(steps - BUFS, steps):
        for cp in copies(i):
            cp.wait()


def finish_kernel(base, from_l, from_r, gx_out):
    width = from_l.shape[2]
    for s in range(SUBS):
        for dr, ref in enumerate((from_l, from_r)):
            gx_out[:, pl.ds((2 * s + dr) * width, width)] = (base[s, :, pl.ds(dr * width, width)] + ref[s]).astype(BF16)


def solution(mesh):
    n_dev = mesh.shape["ep"]
    rows_spec = P(("dp", "ep"), None)
    cube_spec = P(("dp", "ep"), None, None)
    weight_spec = P("ep", None, None)

    def local_step(grad_y, gate_vals, topk_idx, slot_ids, pair_counts, y_routed, x_disp, h_gate, h_up, w_gate, w_up, w_down):
        n_loc, ffn, model = w_down.shape
        tok, top_k = topk_idx.shape
        rows = x_disp.shape[1]
        cap = rows // n_dev
        n_chip = n_dev // 2
        vm = pl.BlockSpec(memory_space=pltpu.VMEM)
        hbm = pl.BlockSpec(memory_space=pl.ANY)
        dma = pltpu.SemaphoreType.DMA
        vs = pltpu.VMEM
        tail = vs((SUBS, tok, model // 2 // SUBS), F32)
        base, tail_r, tail_l, gg, d_rows, dh, act, x_rows = pl.pallas_call(
            functools.partial(exchange_kernel, n_dev, cap),
            out_shape=(vs((SUBS, tok, model // SUBS), F32), tail, tail, pltpu.VMEM((top_k, tok), F32), pltpu.VMEM((n_loc, rows, model), BF16),
                       pltpu.VMEM((n_loc, rows, 2 * ffn), BF16), pltpu.VMEM((n_loc, rows, ffn), BF16), pltpu.VMEM((n_loc, rows, model), BF16)),
            in_specs=[hbm] * 12,
            out_specs=(vm,) * 8,
            scratch_shapes=[
                pltpu.SMEM(pair_counts.shape, jnp.int32),
                pltpu.VMEM((top_k, tok), jnp.int32),
                pltpu.VMEM((top_k, tok), jnp.int32),
                pltpu.VMEM((n_dev, tok, model), BF16),
                pltpu.VMEM((tok, top_k, model), BF16),
                pltpu.VMEM((n_loc, rows, ffn), BF16),
                pltpu.VMEM((n_loc, rows, ffn), BF16),
                pltpu.VMEM((n_loc, model, 2 * ffn), BF16),
                pltpu.VMEM((n_loc, ffn, model), BF16),
                pltpu.VMEM((n_loc, rows, 2 * ffn), F32),
                pltpu.VMEM((tok, top_k), F32),
                pltpu.VMEM((n_dev, 2, top_k, tok), F32),
                pltpu.VMEM((n_dev, tok, n_loc * cap), BF16),
                pltpu.VMEM((2, 2, n_loc * cap, model // SUBS), BF16),
                pltpu.VMEM((n_chip, SUBS, tok, model // SUBS), F32),
                pltpu.VMEM((n_chip, SUBS, tok, model // SUBS), F32),
                pltpu.VMEM((n_chip, SUBS, tok, model // SUBS), F32),
                pltpu.VMEM((4 * SUBS, tok, model // 2 // SUBS), F32),
                pltpu.VMEM((4 * SUBS, tok, model // 2 // SUBS), F32),
                dma((12,)), dma((n_dev - 1,)), dma((n_dev - 1,)), dma((13,)), dma((13,)),
                dma((SUBS * n_chip,)), dma((SUBS * n_chip,)), dma((4 * SUBS,)), dma((4 * SUBS,)),
            ],
            compiler_params=pltpu.CompilerParams(collective_id=0, has_side_effects=True, vmem_limit_bytes=44 * 1024 * 1024),
            name="exchange",
        )(pair_counts, gate_vals.T, topk_idx.T, slot_ids.T, grad_y, y_routed, h_gate, h_up, w_gate, w_up, w_down, x_disp)
        js = 2
        ring_r = [(i, ((i // 2 + 1) % n_chip) * 2 + i % 2) for i in range(n_dev)]
        from_l = lax.ppermute(tail_r, "ep", ring_r)
        from_r = lax.ppermute(tail_l, "ep", [(b, a) for a, b in ring_r])
        gg, gwg, gwu, gwd = pl.pallas_call(
            functools.partial(weight_kernel, js),
            out_shape=(jax.ShapeDtypeStruct((top_k, tok), F32), jax.ShapeDtypeStruct((n_loc, model, ffn), F32),
                       jax.ShapeDtypeStruct((n_loc, model, ffn), F32), jax.ShapeDtypeStruct((n_loc, ffn, model), F32)),
            in_specs=[vm] * 5,
            out_specs=(vm, hbm, hbm, hbm),
            scratch_shapes=[pltpu.VMEM((BUFS, model // js, 2 * ffn), F32), pltpu.VMEM((BUFS, ffn // js, model), F32), dma((BUFS, 3))],
            compiler_params=pltpu.CompilerParams(vmem_limit_bytes=24 * 1024 * 1024),
            cost_estimate=pl.CostEstimate(flops=6 * n_loc * rows * model * ffn, bytes_accessed=12 * n_loc * model * ffn, transcendentals=0),
            name="weights",
        )(x_rows, dh, act, d_rows, gg)
        gx = pl.pallas_call(
            finish_kernel,
            out_shape=jax.ShapeDtypeStruct((tok, model), BF16),
            in_specs=[vm] * 3,
            out_specs=vm,
            compiler_params=pltpu.CompilerParams(vmem_limit_bytes=4 * 1024 * 1024),
            name="finish",
        )(base, from_l, from_r)
        return gx, gg.T, gwg, gwu, gwd

    return jax.shard_map(local_step, mesh=mesh, in_specs=(rows_spec, rows_spec, rows_spec, rows_spec, rows_spec, cube_spec, cube_spec, cube_spec, cube_spec, weight_spec, weight_spec, weight_spec), out_specs=(rows_spec, rows_spec, cube_spec, cube_spec, cube_spec), check_vma=False)
```

```python
import functools

import jax
import jax.numpy as jnp
from jax import lax
from jax.experimental import pallas as pl
from jax.experimental.pallas import tpu as pltpu
from jax.sharding import PartitionSpec as P

MESH = pl.DeviceIdType.MESH
F32 = jnp.float32
BF16 = jnp.bfloat16
NT = (((1,), (1,)), ((), ()))
TN = (((0,), (0,)), ((), ()))
SUBS = 4
BUFS = 3


class Once:
    def __init__(self, cp, log, remote):
        self.cp, self.log, self.remote, self.got = cp, log, remote, False

    def start(self):
        self.cp.start()
        self.log.append(self)

    def wait(self):
        if not self.got:
            self.got = True
            self.cp.wait()

    def wait_recv(self):
        if not self.got:
            self.got = True
            self.cp.wait_recv()

    def finish(self):
        if self.remote:
            self.wait_recv()
            self.cp.wait_send()
        else:
            self.wait()


def exchange_kernel(n_dev, cap, counts_hbm, gates_hbm, idx_hbm, slot_hbm, gy_hbm, yr_hbm, h1_hbm, h3_hbm, wg_hbm, wu_hbm, wd_hbm, x_hbm,
                    base_out, tail_r, tail_l, gg_out, d_buf, dh_buf, a_buf, x_buf, pre_g, pre_d,
                    counts, idx, slot, gy_all, yr, h1, h3, wcat, wd, fs, gg_rows, meta, pmat, grow, pt, rbuf, own, psend, pairin, rsend, rrecv,
                    loc_sem, meta_ssem, meta_rsem, ag_ssem, ag_rsem, pair_ssem, pair_rsem, ring_ssem, ring_rsem):
    n_loc, ffn, model = wd.shape
    top_k, tok = idx.shape
    n_chip = n_dev // 2
    half = model // 2
    hrow = tok // 2
    log = []
    me = lax.axis_index("ep")
    x = me // 2
    c = me % 2
    partner = x * 2 + (1 - c)

    def chip(d):
        return (x + d + n_chip) % n_chip

    def dev(i):
        return {"ep": i}

    def load(src, dst, s):
        cp = Once(pltpu.make_async_copy(src, dst, loc_sem.at[s]), log, False)
        cp.start()
        return cp

    ld_gy = load(gy_hbm, gy_all.at[me], 0)
    ld_small = (load(counts_hbm, counts, 8), load(idx_hbm, idx, 9), load(slot_hbm, slot, 10), load(gates_hbm, meta.at[me, 0], 11))
    ld_h1 = load(h1_hbm, h1, 2)
    ld_h3 = load(h3_hbm, h3, 3)
    ld_wd = load(wd_hbm, wd, 4)
    ld_wg = load(wg_hbm, wcat.at[:, :, pl.ds(0, ffn)], 5)
    ld_wu = load(wu_hbm, wcat.at[:, :, pl.ds(ffn, ffn)], 6)

    barrier = pltpu.get_barrier_semaphore()
    for r in range(1, n_dev):
        pl.semaphore_signal(barrier, inc=1, device_id=dev((me + r) % n_dev), device_id_type=MESH)

    def gy_copy(block, lo, n, s, to):
        ref = gy_all.at[block, pl.ds(lo, n), :]
        return Once(pltpu.make_async_remote_copy(src_ref=ref, dst_ref=ref, send_sem=ag_ssem.at[s], recv_sem=ag_rsem.at[s], device_id=dev(to), device_id_type=MESH), log, True)

    right = chip(1) * 2 + c
    left = chip(-1) * 2 + c
    far = chip(2) * 2 + c
    to_r0 = gy_copy(me, 0, hrow, 0, right)
    to_l1 = gy_copy(me, hrow, hrow, 1, left)
    to_r1 = gy_copy(me, hrow, hrow, 2, right)
    to_l0 = gy_copy(me, 0, hrow, 3, left)
    to_p = gy_copy(me, 0, tok, 4, partner)
    fw_r = gy_copy(left, 0, hrow, 5, right)
    fw_l = gy_copy(right, hrow, hrow, 6, left)
    p_l0 = gy_copy(left, 0, hrow, 7, partner)
    p_r1 = gy_copy(right, hrow, hrow, 8, partner)
    p_l1 = gy_copy(left, hrow, hrow, 9, partner)
    p_r0 = gy_copy(right, 0, hrow, 10, partner)
    p_f0 = gy_copy(far, 0, hrow, 11, partner)
    p_f1 = gy_copy(far, hrow, hrow, 12, partner)

    pl.semaphore_wait(barrier, n_dev - 1)
    ld_gy.wait()
    for cp in (to_r0, to_l1, to_p):
        cp.start()

    for cp in ld_small:
        cp.wait()
    cnt = jnp.zeros(idx.shape, jnp.int32)
    for e in range(n_loc * n_dev):
        cnt = jnp.where(idx[...] == e, counts[0, e], cnt)
    keep = (slot[...] >= 0) & (slot[...] < cnt)
    meta[me, 1] = jnp.where(keep, idx[...] * cap + slot[...], -1).astype(F32)

    meta_cp = {}
    for d in range(n_chip):
        for k in range(2):
            if d == 0 and k == 0:
                continue
            s = d * 2 + k - 1
            cp = Once(pltpu.make_async_remote_copy(src_ref=meta.at[me], dst_ref=meta.at[me], send_sem=meta_ssem.at[s], recv_sem=meta_rsem.at[s],
                                                   device_id=dev(chip(d) * 2 + (c if k == 0 else 1 - c)), device_id_type=MESH), log, True)
            cp.start()
            meta_cp[d, k] = cp
    to_r1.start()
    to_l0.start()

    def meta_wait(d):
        for k in range(2):
            if (d, k) != (0, 0):
                meta_cp[(n_chip - d) % n_chip, k].wait_recv()

    ld_h1.wait()
    ld_h3.wait()
    rstep = 32

    @pl.loop(0, n_loc * (h1.shape[1] // rstep))
    def _(i):
        e = i // (h1.shape[1] // rstep)
        r = pl.multiple_of((i % (h1.shape[1] // rstep)) * rstep, rstep)
        a = h1[e, pl.ds(r, rstep), :].astype(F32)
        b = h3[e, pl.ds(r, rstep), :].astype(F32)
        g = jax.nn.sigmoid(a)
        s = a * g
        a_buf[e, pl.ds(r, rstep), :] = (s * b).astype(BF16)
        fs[e, pl.ds(r, rstep), pl.ds(0, ffn)] = b * g * (1.0 + a * (1.0 - g))
        fs[e, pl.ds(r, rstep), pl.ds(ffn, ffn)] = s


    def prep(h):
        rel = meta[h, 1] - (me * (n_loc * cap)).astype(F32)
        gate = meta[h, 0]
        rows = lax.broadcasted_iota(jnp.int32, (n_loc * cap, tok), 0).astype(F32)
        sel = jnp.zeros((n_loc * cap, tok), F32)
        gsel = jnp.zeros((n_loc * cap, tok), F32)
        for k in range(top_k):
            hit = rows == rel[k:k + 1, :]
            sel = jnp.where(hit, 1.0, sel)
            gsel = jnp.where(hit, gate[k:k + 1, :], gsel)
        grow[h] = jnp.sum(gsel, axis=1, keepdims=True)
        pmat[h] = sel.astype(BF16)
        pt[h] = sel.T.astype(BF16)

    def build(h):
        picked = jnp.dot(pmat[h], gy_all[h], preferred_element_type=F32)
        rows_d = (grow[h] * picked).astype(BF16)
        for e in range(n_loc):
            d_buf[e, pl.ds(pl.multiple_of(h * cap, cap), cap), :] = rows_d[e * cap:(e + 1) * cap]

    def pair_copy(q, s, lo):
        return Once(pltpu.make_async_remote_copy(src_ref=psend.at[q, lo], dst_ref=pairin.at[q, lo],
                                                 send_sem=pair_ssem.at[s], recv_sem=pair_rsem.at[s], device_id=dev(partner), device_id_type=MESH), log, True)

    def rows_of(ref, e, q):
        return ref[e, pl.ds(pl.multiple_of(q * (2 * cap), 2 * cap), 2 * cap), :]

    def hidden(qs):
        for e in range(n_loc):
            d = jnp.concatenate([rows_of(d_buf, e, q) for q in qs], axis=0)
            da = lax.dot_general(d, wd[e], NT, preferred_element_type=F32).astype(BF16).astype(F32)
            da2 = jnp.concatenate([da, da], axis=1)
            for i, q in enumerate(qs):
                dh = (da2[i * 2 * cap:(i + 1) * 2 * cap] * rows_of(fs, e, q)).astype(BF16)
                dh_buf[e, pl.ds(pl.multiple_of(q * (2 * cap), 2 * cap), 2 * cap), :] = dh

    pair_cps = {}

    chunk = model // SUBS

    def back(dists, qs, hf):
        cols = pl.ds(hf * chunk, chunk)

        for e in range(n_loc):
            dh = jnp.concatenate([rows_of(dh_buf, e, q) for q in qs], axis=0)
            r = lax.dot_general(dh, wcat[e, cols, :], NT, preferred_element_type=F32).astype(BF16)
            for i in range(len(qs)):
                for j in range(2):
                    rbuf[i, j, pl.ds(e * cap, cap), :] = r[(i * 2 + j) * cap:(i * 2 + j + 1) * cap]

        for i, q in enumerate(qs):
            psend[q, hf] = jnp.dot(pt[q * 2 + 1 - c], rbuf[i, 1 - c], preferred_element_type=F32)
        for i, d in enumerate(dists):
            cp = pair_copy(qs[i], ((d + n_chip) % n_chip) * SUBS + hf, hf)
            cp.start()
            pair_cps[d, hf] = cp
        for i, q in enumerate(qs):
            own[q, hf] = jnp.dot(pt[q * 2 + c], rbuf[i, c], preferred_element_type=F32)

    width = half // SUBS

    def ring_copy(dr, st, s):
        k = (dr * 2 + st) * SUBS + s
        return Once(pltpu.make_async_remote_copy(src_ref=rsend.at[k], dst_ref=rrecv.at[k], send_sem=ring_ssem.at[k], recv_sem=ring_rsem.at[k],
                                                 device_id=dev(right if dr == 0 else left), device_id_type=MESH), log, True)

    ring = {(dr, st, s): ring_copy(dr, st, s) for dr in range(2) for st in range(2) for s in range(SUBS)}
    dest = {0: (-1, 2, 1), 1: (1, 2, -1)}
    tails = (tail_r, tail_l)

    def pair_sum(d, s, dr):
        pair_cps[d, s].wait_recv()
        q = chip(d)
        cols = pl.ds(dr * width, width)
        return own[q, s, :, cols] + pairin[q, s, :, cols]

    def ring_step(st, s):
        for dr in range(2):
            v = pair_sum(dest[dr][st], s, dr)
            if st > 0:
                ring[dr, st - 1, s].wait_recv()
                v = v + rrecv[(dr * 2 + st - 1) * SUBS + s]
            if st < 2:
                rsend[(dr * 2 + st) * SUBS + s] = v
                ring[dr, st, s].start()
            else:
                tails[dr][s] = v

    def finish():
        for cp in log:
            cp.finish()

    meta_wait(0)
    prep(x * 2)
    prep(x * 2 + 1)
    to_p.wait_recv()
    build(x * 2)
    build(x * 2 + 1)
    ld_wd.wait()
    hidden([x])
    to_r0.wait_recv()
    fw_r.start()
    p_l0.start()
    to_l1.wait_recv()
    fw_l.start()
    p_r1.start()
    for d in (-1, 1):
        meta_wait(d)
        for i in range(2):
            prep(chip(d) * 2 + i)
    ld_wg.wait()
    ld_wu.wait()
    back((0,), [x], 0)
    to_r1.wait_recv()
    p_l1.start()
    to_l0.wait_recv()
    p_r0.start()
    build(left)
    build(right)
    meta_wait(2)
    prep(chip(2) * 2)
    prep(chip(2) * 2 + 1)
    p_l0.wait_recv()
    p_l1.wait_recv()
    build(chip(-1) * 2 + 1 - c)
    p_r0.wait_recv()
    p_r1.wait_recv()
    build(chip(1) * 2 + 1 - c)
    near = [chip(-1), chip(1)]
    hidden(near)
    back((-1, 1), near, 0)
    back((-1, 1), near, 1)
    ring_step(0, 0)
    fw_r.wait_recv()
    p_f0.start()
    fw_l.wait_recv()
    p_f1.start()
    for s in range(2, SUBS):
        back((-1, 1), near, s)
        ring_step(0, s - 1)
    build(far)
    ring_step(0, SUBS - 1)
    ld_x = load(x_hbm, x_buf, 7)
    ld_yr = load(yr_hbm, yr, 1)
    p_f0.wait_recv()
    p_f1.wait_recv()
    build(chip(2) * 2 + 1 - c)
    hidden([chip(2)])
    back((2,), [chip(2)], 0)
    for s in range(1, SUBS):
        back((2,), [chip(2)], s)
        ring_step(1, s - 1)
    ring_step(1, SUBS - 1)
    for s in range(1, SUBS):
        back((0,), [x], s)

    ld_yr.wait()
    step = 16

    @pl.loop(0, tok // step)
    def _(i):
        t = pl.multiple_of(i * step, step)
        g = gy_all[me, pl.ds(t, step), :].astype(F32)
        y = yr[pl.ds(t, step), :, :].astype(F32)
        gg_rows[pl.ds(t, step), :] = jnp.sum(y * g[:, None, :], axis=2)

    gg_out[...] = gg_rows[...].T

    for s in range(SUBS):
        for dr in range(2):
            base_out[s, :, pl.ds(dr * width, width)] = pair_sum(0, s, dr)
    ld_x.wait()
    pre_g[...] = lax.dot_general(x_buf[0, :, pl.ds(0, pre_g.shape[0])], dh_buf[0], TN, preferred_element_type=F32)
    pre_d[...] = lax.dot_general(a_buf[0, :, pl.ds(0, pre_d.shape[0])], d_buf[0], TN, preferred_element_type=F32)
    for s in range(SUBS):
        ring_step(2, s)

    finish()


def weight_kernel(js, x_ref, dh_ref, a_ref, d_ref, gg_ref, pre_g, pre_d, gg_out, gwg, gwu, gwd, gbuf, dbuf, sem):
    n_loc, model, ffn = gwg.shape
    xc, ac = model // js, ffn // js
    gg_out[...] = gg_ref[...]

    def copies(i):
        e, j, b = i // js, i % js, i % BUFS
        rows, arows = pl.ds(j * xc, xc), pl.ds(j * ac, ac)
        g, d = (pre_g, pre_d) if i == 0 else (gbuf.at[b], dbuf.at[b])
        return (pltpu.make_async_copy(g.at[:, pl.ds(0, ffn)], gwg.at[e, rows, :], sem.at[b, 0]),
                pltpu.make_async_copy(g.at[:, pl.ds(ffn, ffn)], gwu.at[e, rows, :], sem.at[b, 1]),
                pltpu.make_async_copy(d, gwd.at[e, arows, :], sem.at[b, 2]))

    steps = n_loc * js
    for i in range(steps):
        e, j, b = i // js, i % js, i % BUFS
        if i >= BUFS:
            for cp in copies(i - BUFS):
                cp.wait()
        if i > 0:
            gbuf[b] = lax.dot_general(x_ref[e, :, pl.ds(j * xc, xc)], dh_ref[e], TN, preferred_element_type=F32)
            dbuf[b] = lax.dot_general(a_ref[e, :, pl.ds(j * ac, ac)], d_ref[e], TN, preferred_element_type=F32)
        for cp in copies(i):
            cp.start()
    for i in range(steps - BUFS, steps):
        for cp in copies(i):
            cp.wait()


def finish_kernel(base, from_l, from_r, gx_out):
    width = from_l.shape[2]
    for s in range(SUBS):
        for dr, ref in enumerate((from_l, from_r)):
            gx_out[:, pl.ds((2 * s + dr) * width, width)] = (base[s, :, pl.ds(dr * width, width)] + ref[s]).astype(BF16)


def solution(mesh):
    n_dev = mesh.shape["ep"]
    rows_spec = P(("dp", "ep"), None)
    cube_spec = P(("dp", "ep"), None, None)
    weight_spec = P("ep", None, None)

    def local_step(grad_y, gate_vals, topk_idx, slot_ids, pair_counts, y_routed, x_disp, h_gate, h_up, w_gate, w_up, w_down):
        n_loc, ffn, model = w_down.shape
        tok, top_k = topk_idx.shape
        rows = x_disp.shape[1]
        cap = rows // n_dev
        n_chip = n_dev // 2
        vm = pl.BlockSpec(memory_space=pltpu.VMEM)
        hbm = pl.BlockSpec(memory_space=pl.ANY)
        dma = pltpu.SemaphoreType.DMA
        vs = pltpu.VMEM
        tail = vs((SUBS, tok, model // 2 // SUBS), F32)
        js = 2
        base, tail_r, tail_l, gg, d_rows, dh, act, x_rows, pre_g, pre_d = pl.pallas_call(
            functools.partial(exchange_kernel, n_dev, cap),
            out_shape=(vs((SUBS, tok, model // SUBS), F32), tail, tail, pltpu.VMEM((top_k, tok), F32), pltpu.VMEM((n_loc, rows, model), BF16),
                       pltpu.VMEM((n_loc, rows, 2 * ffn), BF16), pltpu.VMEM((n_loc, rows, ffn), BF16), pltpu.VMEM((n_loc, rows, model), BF16),
                       vs((model // js, 2 * ffn), F32), vs((ffn // js, model), F32)),
            in_specs=[hbm] * 12,
            out_specs=(vm,) * 10,
            scratch_shapes=[
                pltpu.SMEM(pair_counts.shape, jnp.int32),
                pltpu.VMEM((top_k, tok), jnp.int32),
                pltpu.VMEM((top_k, tok), jnp.int32),
                pltpu.VMEM((n_dev, tok, model), BF16),
                pltpu.VMEM((tok, top_k, model), BF16),
                pltpu.VMEM((n_loc, rows, ffn), BF16),
                pltpu.VMEM((n_loc, rows, ffn), BF16),
                pltpu.VMEM((n_loc, model, 2 * ffn), BF16),
                pltpu.VMEM((n_loc, ffn, model), BF16),
                pltpu.VMEM((n_loc, rows, 2 * ffn), F32),
                pltpu.VMEM((tok, top_k), F32),
                pltpu.VMEM((n_dev, 2, top_k, tok), F32),
                pltpu.VMEM((n_dev, n_loc * cap, tok), BF16),
                pltpu.VMEM((n_dev, n_loc * cap, 1), F32),
                pltpu.VMEM((n_dev, tok, n_loc * cap), BF16),
                pltpu.VMEM((2, 2, n_loc * cap, model // SUBS), BF16),
                pltpu.VMEM((n_chip, SUBS, tok, model // SUBS), F32),
                pltpu.VMEM((n_chip, SUBS, tok, model // SUBS), F32),
                pltpu.VMEM((n_chip, SUBS, tok, model // SUBS), F32),
                pltpu.VMEM((4 * SUBS, tok, model // 2 // SUBS), F32),
                pltpu.VMEM((4 * SUBS, tok, model // 2 // SUBS), F32),
                dma((12,)), dma((n_dev - 1,)), dma((n_dev - 1,)), dma((13,)), dma((13,)),
                dma((SUBS * n_chip,)), dma((SUBS * n_chip,)), dma((4 * SUBS,)), dma((4 * SUBS,)),
            ],
            compiler_params=pltpu.CompilerParams(collective_id=0, has_side_effects=True, vmem_limit_bytes=43 * 1024 * 1024),
            name="exchange",
        )(pair_counts, gate_vals.T, topk_idx.T, slot_ids.T, grad_y, y_routed, h_gate, h_up, w_gate, w_up, w_down, x_disp)
        ring_r = [(i, ((i // 2 + 1) % n_chip) * 2 + i % 2) for i in range(n_dev)]
        from_l = lax.ppermute(tail_r, "ep", ring_r)
        from_r = lax.ppermute(tail_l, "ep", [(b, a) for a, b in ring_r])
        gg, gwg, gwu, gwd = pl.pallas_call(
            functools.partial(weight_kernel, js),
            out_shape=(jax.ShapeDtypeStruct((top_k, tok), F32), jax.ShapeDtypeStruct((n_loc, model, ffn), F32),
                       jax.ShapeDtypeStruct((n_loc, model, ffn), F32), jax.ShapeDtypeStruct((n_loc, ffn, model), F32)),
            in_specs=[vm] * 7,
            out_specs=(vm, hbm, hbm, hbm),
            scratch_shapes=[pltpu.VMEM((BUFS, model // js, 2 * ffn), F32), pltpu.VMEM((BUFS, ffn // js, model), F32), dma((BUFS, 3))],
            compiler_params=pltpu.CompilerParams(vmem_limit_bytes=20 * 1024 * 1024),
            cost_estimate=pl.CostEstimate(flops=6 * n_loc * rows * model * ffn, bytes_accessed=12 * n_loc * model * ffn, transcendentals=0),
            name="weights",
        )(x_rows, dh, act, d_rows, gg, pre_g, pre_d)
        gx = pl.pallas_call(
            finish_kernel,
            out_shape=jax.ShapeDtypeStruct((tok, model), BF16),
            in_specs=[vm] * 3,
            out_specs=vm,
            compiler_params=pltpu.CompilerParams(vmem_limit_bytes=4 * 1024 * 1024),
            name="finish",
        )(base, from_l, from_r)
        return gx, gg.T, gwg, gwu, gwd

    return jax.shard_map(local_step, mesh=mesh, in_specs=(rows_spec, rows_spec, rows_spec, rows_spec, rows_spec, cube_spec, cube_spec, cube_spec, cube_spec, weight_spec, weight_spec, weight_spec), out_specs=(rows_spec, rows_spec, cube_spec, cube_spec, cube_spec), check_vma=False)
```

```python
import functools

import jax
import jax.numpy as jnp
from jax import lax
from jax.experimental import pallas as pl
from jax.experimental.pallas import tpu as pltpu
from jax.sharding import PartitionSpec as P

MESH = pl.DeviceIdType.MESH
F32 = jnp.float32
BF16 = jnp.bfloat16
NT = (((1,), (1,)), ((), ()))
TN = (((0,), (0,)), ((), ()))
SUBS = 4
BUFS = 3


class Once:
    def __init__(self, cp, log, remote):
        self.cp, self.log, self.remote, self.got = cp, log, remote, False

    def start(self):
        self.cp.start()
        self.log.append(self)

    def wait(self):
        if not self.got:
            self.got = True
            self.cp.wait()

    def wait_recv(self):
        if not self.got:
            self.got = True
            self.cp.wait_recv()

    def finish(self):
        if self.remote:
            self.wait_recv()
            self.cp.wait_send()
        else:
            self.wait()


def exchange_kernel(n_dev, cap, counts_hbm, gates_hbm, idx_hbm, slot_hbm, gy_hbm, yr_hbm, h1_hbm, h3_hbm, wg_hbm, wu_hbm, wd_hbm, x_hbm,
                    base_out, tail_r, tail_l, gg_out, d_buf, dh_buf, a_buf, x_buf,
                    counts, idx, slot, gy_all, yr, h1, h3, wcat, wd, fs, gg_rows, meta, pmat, grow, pt, rbuf, own, psend, pairin, rsend, rrecv,
                    loc_sem, meta_ssem, meta_rsem, ag_ssem, ag_rsem, pair_ssem, pair_rsem, ring_ssem, ring_rsem):
    n_loc, ffn, model = wd.shape
    top_k, tok = idx.shape
    n_chip = n_dev // 2
    half = model // 2
    hrow = tok // 2
    log = []
    me = lax.axis_index("ep")
    x = me // 2
    c = me % 2
    partner = x * 2 + (1 - c)

    def chip(d):
        return (x + d + n_chip) % n_chip

    def dev(i):
        return {"ep": i}

    def load(src, dst, s):
        cp = Once(pltpu.make_async_copy(src, dst, loc_sem.at[s]), log, False)
        cp.start()
        return cp

    ld_gy = load(gy_hbm, gy_all.at[me], 0)
    ld_small = (load(counts_hbm, counts, 8), load(idx_hbm, idx, 9), load(slot_hbm, slot, 10), load(gates_hbm, meta.at[me, 0], 11))
    ld_h1 = load(h1_hbm, h1, 2)
    ld_h3 = load(h3_hbm, h3, 3)
    ld_wd = load(wd_hbm, wd, 4)
    ld_wg = load(wg_hbm, wcat.at[:, :, pl.ds(0, ffn)], 5)
    ld_wu = load(wu_hbm, wcat.at[:, :, pl.ds(ffn, ffn)], 6)

    barrier = pltpu.get_barrier_semaphore()
    for r in range(1, n_dev):
        pl.semaphore_signal(barrier, inc=1, device_id=dev((me + r) % n_dev), device_id_type=MESH)

    def gy_copy(block, lo, n, s, to):
        ref = gy_all.at[block, pl.ds(lo, n), :]
        return Once(pltpu.make_async_remote_copy(src_ref=ref, dst_ref=ref, send_sem=ag_ssem.at[s], recv_sem=ag_rsem.at[s], device_id=dev(to), device_id_type=MESH), log, True)

    right = chip(1) * 2 + c
    left = chip(-1) * 2 + c
    far = chip(2) * 2 + c
    to_r0 = gy_copy(me, 0, hrow, 0, right)
    to_l1 = gy_copy(me, hrow, hrow, 1, left)
    to_r1 = gy_copy(me, hrow, hrow, 2, right)
    to_l0 = gy_copy(me, 0, hrow, 3, left)
    to_p = gy_copy(me, 0, tok, 4, partner)
    fw_r = gy_copy(left, 0, hrow, 5, right)
    fw_l = gy_copy(right, hrow, hrow, 6, left)
    p_l0 = gy_copy(left, 0, hrow, 7, partner)
    p_r1 = gy_copy(right, hrow, hrow, 8, partner)
    p_l1 = gy_copy(left, hrow, hrow, 9, partner)
    p_r0 = gy_copy(right, 0, hrow, 10, partner)
    p_f0 = gy_copy(far, 0, hrow, 11, partner)
    p_f1 = gy_copy(far, hrow, hrow, 12, partner)

    pl.semaphore_wait(barrier, n_dev - 1)
    ld_gy.wait()
    for cp in (to_r0, to_l1, to_p):
        cp.start()

    for cp in ld_small:
        cp.wait()
    cnt = jnp.zeros(idx.shape, jnp.int32)
    for e in range(n_loc * n_dev):
        cnt = jnp.where(idx[...] == e, counts[0, e], cnt)
    keep = (slot[...] >= 0) & (slot[...] < cnt)
    meta[me, 1] = jnp.where(keep, idx[...] * cap + slot[...], -1).astype(F32)

    meta_cp = {}
    for d in range(n_chip):
        for k in range(2):
            if d == 0 and k == 0:
                continue
            s = d * 2 + k - 1
            cp = Once(pltpu.make_async_remote_copy(src_ref=meta.at[me], dst_ref=meta.at[me], send_sem=meta_ssem.at[s], recv_sem=meta_rsem.at[s],
                                                   device_id=dev(chip(d) * 2 + (c if k == 0 else 1 - c)), device_id_type=MESH), log, True)
            cp.start()
            meta_cp[d, k] = cp
    to_r1.start()
    to_l0.start()

    def meta_wait(d):
        for k in range(2):
            if (d, k) != (0, 0):
                meta_cp[(n_chip - d) % n_chip, k].wait_recv()

    ld_h1.wait()
    ld_h3.wait()
    rstep = 32

    @pl.loop(0, n_loc * (h1.shape[1] // rstep))
    def _(i):
        e = i // (h1.shape[1] // rstep)
        r = pl.multiple_of((i % (h1.shape[1] // rstep)) * rstep, rstep)
        a = h1[e, pl.ds(r, rstep), :].astype(F32)
        b = h3[e, pl.ds(r, rstep), :].astype(F32)
        g = jax.nn.sigmoid(a)
        s = a * g
        a_buf[e, pl.ds(r, rstep), :] = (s * b).astype(BF16)
        fs[e, pl.ds(r, rstep), pl.ds(0, ffn)] = b * g * (1.0 + a * (1.0 - g))
        fs[e, pl.ds(r, rstep), pl.ds(ffn, ffn)] = s


    def prep(h):
        rel = meta[h, 1] - (me * (n_loc * cap)).astype(F32)
        gate = meta[h, 0]
        rows = lax.broadcasted_iota(jnp.int32, (n_loc * cap, tok), 0).astype(F32)
        sel = jnp.zeros((n_loc * cap, tok), F32)
        gsel = jnp.zeros((n_loc * cap, tok), F32)
        for k in range(top_k):
            hit = rows == rel[k:k + 1, :]
            sel = jnp.where(hit, 1.0, sel)
            gsel = jnp.where(hit, gate[k:k + 1, :], gsel)
        grow[h] = jnp.sum(gsel, axis=1, keepdims=True)
        pmat[h] = sel.astype(BF16)
        pt[h] = sel.T.astype(BF16)

    def build(h):
        picked = jnp.dot(pmat[h], gy_all[h], preferred_element_type=F32)
        rows_d = (grow[h] * picked).astype(BF16)
        for e in range(n_loc):
            d_buf[e, pl.ds(pl.multiple_of(h * cap, cap), cap), :] = rows_d[e * cap:(e + 1) * cap]

    def pair_copy(q, s, lo):
        return Once(pltpu.make_async_remote_copy(src_ref=psend.at[q, lo], dst_ref=pairin.at[q, lo],
                                                 send_sem=pair_ssem.at[s], recv_sem=pair_rsem.at[s], device_id=dev(partner), device_id_type=MESH), log, True)

    def rows_of(ref, e, q):
        return ref[e, pl.ds(pl.multiple_of(q * (2 * cap), 2 * cap), 2 * cap), :]

    def hidden(qs):
        for e in range(n_loc):
            d = jnp.concatenate([rows_of(d_buf, e, q) for q in qs], axis=0)
            da = lax.dot_general(d, wd[e], NT, preferred_element_type=F32).astype(BF16).astype(F32)
            da2 = jnp.concatenate([da, da], axis=1)
            for i, q in enumerate(qs):
                dh = (da2[i * 2 * cap:(i + 1) * 2 * cap] * rows_of(fs, e, q)).astype(BF16)
                dh_buf[e, pl.ds(pl.multiple_of(q * (2 * cap), 2 * cap), 2 * cap), :] = dh

    pair_cps = {}

    chunk = model // SUBS

    def back(dists, qs, hf):
        cols = pl.ds(hf * chunk, chunk)

        for e in range(n_loc):
            dh = jnp.concatenate([rows_of(dh_buf, e, q) for q in qs], axis=0)
            r = lax.dot_general(dh, wcat[e, cols, :], NT, preferred_element_type=F32).astype(BF16)
            for i in range(len(qs)):
                for j in range(2):
                    rbuf[i, j, pl.ds(e * cap, cap), :] = r[(i * 2 + j) * cap:(i * 2 + j + 1) * cap]

        for i, q in enumerate(qs):
            psend[q, hf] = jnp.dot(pt[q * 2 + 1 - c], rbuf[i, 1 - c], preferred_element_type=F32)
        for i, d in enumerate(dists):
            cp = pair_copy(qs[i], ((d + n_chip) % n_chip) * SUBS + hf, hf)
            cp.start()
            pair_cps[d, hf] = cp
        for i, q in enumerate(qs):
            own[q, hf] = jnp.dot(pt[q * 2 + c], rbuf[i, c], preferred_element_type=F32)

    width = half // SUBS

    def ring_copy(dr, st, s):
        k = (dr * 2 + st) * SUBS + s
        return Once(pltpu.make_async_remote_copy(src_ref=rsend.at[k], dst_ref=rrecv.at[k], send_sem=ring_ssem.at[k], recv_sem=ring_rsem.at[k],
                                                 device_id=dev(right if dr == 0 else left), device_id_type=MESH), log, True)

    ring = {(dr, st, s): ring_copy(dr, st, s) for dr in range(2) for st in range(2) for s in range(SUBS)}
    dest = {0: (-1, 2, 1), 1: (1, 2, -1)}
    tails = (tail_r, tail_l)

    def pair_sum(d, s, dr):
        pair_cps[d, s].wait_recv()
        q = chip(d)
        cols = pl.ds(dr * width, width)
        return own[q, s, :, cols] + pairin[q, s, :, cols]

    def ring_step(st, s):
        for dr in range(2):
            v = pair_sum(dest[dr][st], s, dr)
            if st > 0:
                ring[dr, st - 1, s].wait_recv()
                v = v + rrecv[(dr * 2 + st - 1) * SUBS + s]
            if st < 2:
                rsend[(dr * 2 + st) * SUBS + s] = v
                ring[dr, st, s].start()
            else:
                tails[dr][s] = v

    def finish():
        for cp in log:
            cp.finish()

    meta_wait(0)
    prep(x * 2)
    prep(x * 2 + 1)
    to_p.wait_recv()
    build(x * 2)
    build(x * 2 + 1)
    ld_wd.wait()
    hidden([x])
    to_r0.wait_recv()
    fw_r.start()
    p_l0.start()
    to_l1.wait_recv()
    fw_l.start()
    p_r1.start()
    for d in (-1, 1):
        meta_wait(d)
        for i in range(2):
            prep(chip(d) * 2 + i)
    ld_wg.wait()
    ld_wu.wait()
    for s in range(3):
        back((0,), [x], s)
    to_r1.wait_recv()
    p_l1.start()
    to_l0.wait_recv()
    p_r0.start()
    build(left)
    build(right)
    meta_wait(2)
    prep(chip(2) * 2)
    prep(chip(2) * 2 + 1)
    p_l0.wait_recv()
    p_l1.wait_recv()
    build(chip(-1) * 2 + 1 - c)
    p_r0.wait_recv()
    p_r1.wait_recv()
    build(chip(1) * 2 + 1 - c)
    near = [chip(-1), chip(1)]
    hidden(near)
    back((-1, 1), near, 0)
    back((-1, 1), near, 1)
    ring_step(0, 0)
    fw_r.wait_recv()
    p_f0.start()
    fw_l.wait_recv()
    p_f1.start()
    for s in range(2, SUBS):
        back((-1, 1), near, s)
        ring_step(0, s - 1)
    build(far)
    ring_step(0, SUBS - 1)
    ld_x = load(x_hbm, x_buf, 7)
    ld_yr = load(yr_hbm, yr, 1)
    p_f0.wait_recv()
    p_f1.wait_recv()
    build(chip(2) * 2 + 1 - c)
    hidden([chip(2)])
    back((2,), [chip(2)], 0)
    for s in range(1, SUBS):
        back((2,), [chip(2)], s)
        ring_step(1, s - 1)
    ring_step(1, SUBS - 1)
    back((0,), [x], 3)

    ld_yr.wait()
    step = 16

    @pl.loop(0, tok // step)
    def _(i):
        t = pl.multiple_of(i * step, step)
        g = gy_all[me, pl.ds(t, step), :].astype(F32)
        y = yr[pl.ds(t, step), :, :].astype(F32)
        gg_rows[pl.ds(t, step), :] = jnp.sum(y * g[:, None, :], axis=2)

    gg_out[...] = gg_rows[...].T

    for s in range(SUBS):
        for dr in range(2):
            base_out[s, :, pl.ds(dr * width, width)] = pair_sum(0, s, dr)
    for s in range(SUBS):
        ring_step(2, s)

    finish()


def weight_kernel(js, x_ref, dh_ref, a_ref, d_ref, gg_ref, gg_out, gwg, gwu, gwd, gbuf, dbuf, sem):
    n_loc, model, ffn = gwg.shape
    xc, ac = model // js, ffn // js
    gg_out[...] = gg_ref[...]

    def copies(i):
        e, j, b = i // js, i % js, i % BUFS
        rows, arows = pl.ds(j * xc, xc), pl.ds(j * ac, ac)
        return (pltpu.make_async_copy(gbuf.at[b, :, pl.ds(0, ffn)], gwg.at[e, rows, :], sem.at[b, 0]),
                pltpu.make_async_copy(gbuf.at[b, :, pl.ds(ffn, ffn)], gwu.at[e, rows, :], sem.at[b, 1]),
                pltpu.make_async_copy(dbuf.at[b], gwd.at[e, arows, :], sem.at[b, 2]))

    steps = n_loc * js
    for i in range(steps):
        e, j, b = i // js, i % js, i % BUFS
        if i >= BUFS:
            for cp in copies(i - BUFS):
                cp.wait()
        gbuf[b] = lax.dot_general(x_ref[e, :, pl.ds(j * xc, xc)], dh_ref[e], TN, preferred_element_type=F32)
        dbuf[b] = lax.dot_general(a_ref[e, :, pl.ds(j * ac, ac)], d_ref[e], TN, preferred_element_type=F32)
        for cp in copies(i):
            cp.start()
    for i in range(steps - BUFS, steps):
        for cp in copies(i):
            cp.wait()


def finish_kernel(base, from_l, from_r, gx_out):
    width = from_l.shape[2]
    for s in range(SUBS):
        for dr, ref in enumerate((from_l, from_r)):
            gx_out[:, pl.ds((2 * s + dr) * width, width)] = (base[s, :, pl.ds(dr * width, width)] + ref[s]).astype(BF16)


def solution(mesh):
    n_dev = mesh.shape["ep"]
    rows_spec = P(("dp", "ep"), None)
    cube_spec = P(("dp", "ep"), None, None)
    weight_spec = P("ep", None, None)

    def local_step(grad_y, gate_vals, topk_idx, slot_ids, pair_counts, y_routed, x_disp, h_gate, h_up, w_gate, w_up, w_down):
        n_loc, ffn, model = w_down.shape
        tok, top_k = topk_idx.shape
        rows = x_disp.shape[1]
        cap = rows // n_dev
        n_chip = n_dev // 2
        vm = pl.BlockSpec(memory_space=pltpu.VMEM)
        hbm = pl.BlockSpec(memory_space=pl.ANY)
        dma = pltpu.SemaphoreType.DMA
        vs = pltpu.VMEM
        tail = vs((SUBS, tok, model // 2 // SUBS), F32)
        js = 2
        base, tail_r, tail_l, gg, d_rows, dh, act, x_rows = pl.pallas_call(
            functools.partial(exchange_kernel, n_dev, cap),
            out_shape=(vs((SUBS, tok, model // SUBS), F32), tail, tail, pltpu.VMEM((top_k, tok), F32), pltpu.VMEM((n_loc, rows, model), BF16),
                       pltpu.VMEM((n_loc, rows, 2 * ffn), BF16), pltpu.VMEM((n_loc, rows, ffn), BF16), pltpu.VMEM((n_loc, rows, model), BF16)),
            in_specs=[hbm] * 12,
            out_specs=(vm,) * 8,
            scratch_shapes=[
                pltpu.SMEM(pair_counts.shape, jnp.int32),
                pltpu.VMEM((top_k, tok), jnp.int32),
                pltpu.VMEM((top_k, tok), jnp.int32),
                pltpu.VMEM((n_dev, tok, model), BF16),
                pltpu.VMEM((tok, top_k, model), BF16),
                pltpu.VMEM((n_loc, rows, ffn), BF16),
                pltpu.VMEM((n_loc, rows, ffn), BF16),
                pltpu.VMEM((n_loc, model, 2 * ffn), BF16),
                pltpu.VMEM((n_loc, ffn, model), BF16),
                pltpu.VMEM((n_loc, rows, 2 * ffn), F32),
                pltpu.VMEM((tok, top_k), F32),
                pltpu.VMEM((n_dev, 2, top_k, tok), F32),
                pltpu.VMEM((n_dev, n_loc * cap, tok), BF16),
                pltpu.VMEM((n_dev, n_loc * cap, 1), F32),
                pltpu.VMEM((n_dev, tok, n_loc * cap), BF16),
                pltpu.VMEM((2, 2, n_loc * cap, model // SUBS), BF16),
                pltpu.VMEM((n_chip, SUBS, tok, model // SUBS), F32),
                pltpu.VMEM((n_chip, SUBS, tok, model // SUBS), F32),
                pltpu.VMEM((n_chip, SUBS, tok, model // SUBS), F32),
                pltpu.VMEM((4 * SUBS, tok, model // 2 // SUBS), F32),
                pltpu.VMEM((4 * SUBS, tok, model // 2 // SUBS), F32),
                dma((12,)), dma((n_dev - 1,)), dma((n_dev - 1,)), dma((13,)), dma((13,)),
                dma((SUBS * n_chip,)), dma((SUBS * n_chip,)), dma((4 * SUBS,)), dma((4 * SUBS,)),
            ],
            compiler_params=pltpu.CompilerParams(collective_id=0, has_side_effects=True, vmem_limit_bytes=44 * 1024 * 1024),
            name="exchange",
        )(pair_counts, gate_vals.T, topk_idx.T, slot_ids.T, grad_y, y_routed, h_gate, h_up, w_gate, w_up, w_down, x_disp)
        ring_r = [(i, ((i // 2 + 1) % n_chip) * 2 + i % 2) for i in range(n_dev)]
        from_l = lax.ppermute(tail_r, "ep", ring_r)
        from_r = lax.ppermute(tail_l, "ep", [(b, a) for a, b in ring_r])
        gg, gwg, gwu, gwd = pl.pallas_call(
            functools.partial(weight_kernel, js),
            out_shape=(jax.ShapeDtypeStruct((top_k, tok), F32), jax.ShapeDtypeStruct((n_loc, model, ffn), F32),
                       jax.ShapeDtypeStruct((n_loc, model, ffn), F32), jax.ShapeDtypeStruct((n_loc, ffn, model), F32)),
            in_specs=[vm] * 5,
            out_specs=(vm, hbm, hbm, hbm),
            scratch_shapes=[pltpu.VMEM((BUFS, model // js, 2 * ffn), F32), pltpu.VMEM((BUFS, ffn // js, model), F32), dma((BUFS, 3))],
            compiler_params=pltpu.CompilerParams(vmem_limit_bytes=24 * 1024 * 1024),
            cost_estimate=pl.CostEstimate(flops=6 * n_loc * rows * model * ffn, bytes_accessed=12 * n_loc * model * ffn, transcendentals=0),
            name="weights",
        )(x_rows, dh, act, d_rows, gg)
        gx = pl.pallas_call(
            finish_kernel,
            out_shape=jax.ShapeDtypeStruct((tok, model), BF16),
            in_specs=[vm] * 3,
            out_specs=vm,
            compiler_params=pltpu.CompilerParams(vmem_limit_bytes=4 * 1024 * 1024),
            name="finish",
        )(base, from_l, from_r)
        return gx, gg.T, gwg, gwu, gwd

    return jax.shard_map(local_step, mesh=mesh, in_specs=(rows_spec, rows_spec, rows_spec, rows_spec, rows_spec, cube_spec, cube_spec, cube_spec, cube_spec, weight_spec, weight_spec, weight_spec), out_specs=(rows_spec, rows_spec, cube_spec, cube_spec, cube_spec), check_vma=False)
```

```python
import functools

import jax
import jax.numpy as jnp
from jax import lax
from jax.experimental import pallas as pl
from jax.experimental.pallas import tpu as pltpu
from jax.sharding import PartitionSpec as P

MESH = pl.DeviceIdType.MESH
F32 = jnp.float32
BF16 = jnp.bfloat16
NT = (((1,), (1,)), ((), ()))
TN = (((0,), (0,)), ((), ()))
SUBS = 4
BUFS = 3


class Once:
    def __init__(self, cp, log, remote):
        self.cp, self.log, self.remote, self.got = cp, log, remote, False

    def start(self):
        self.cp.start()
        self.log.append(self)

    def wait(self):
        if not self.got:
            self.got = True
            self.cp.wait()

    def wait_recv(self):
        if not self.got:
            self.got = True
            self.cp.wait_recv()

    def finish(self):
        if self.remote:
            self.wait_recv()
            self.cp.wait_send()
        else:
            self.wait()


def exchange_kernel(n_dev, cap, counts_hbm, gates_hbm, idx_hbm, slot_hbm, gy_hbm, yr_hbm, h1_hbm, h3_hbm, wg_hbm, wu_hbm, wd_hbm, x_hbm,
                    base_out, tail, gg_out, d_buf, dh_buf, a_buf, x_buf,
                    counts, idx, slot, gy_all, yr, h1, h3, wcat, wd, fs, gg_rows, meta, pmat, grow, pt, rbuf, own, psend, pairin, rsend, rrecv,
                    loc_sem, meta_ssem, meta_rsem, ag_ssem, ag_rsem, pair_ssem, pair_rsem, ring_ssem, ring_rsem):
    n_loc, ffn, model = wd.shape
    top_k, tok = idx.shape
    n_chip = n_dev // 2
    half = model // 2
    hrow = tok // 2
    log = []
    me = lax.axis_index("ep")
    x = me // 2
    c = me % 2
    partner = x * 2 + (1 - c)

    def chip(d):
        return (x + d + n_chip) % n_chip

    def dev(i):
        return {"ep": i}

    def load(src, dst, s):
        cp = Once(pltpu.make_async_copy(src, dst, loc_sem.at[s]), log, False)
        cp.start()
        return cp

    ld_gy = load(gy_hbm, gy_all.at[me], 0)
    ld_small = (load(counts_hbm, counts, 8), load(idx_hbm, idx, 9), load(slot_hbm, slot, 10), load(gates_hbm, meta.at[me, 0], 11))
    ld_h1 = load(h1_hbm, h1, 2)
    ld_h3 = load(h3_hbm, h3, 3)
    ld_wd = load(wd_hbm, wd, 4)
    ld_wg = load(wg_hbm, wcat.at[:, :, pl.ds(0, ffn)], 5)
    ld_wu = load(wu_hbm, wcat.at[:, :, pl.ds(ffn, ffn)], 6)

    barrier = pltpu.get_barrier_semaphore()
    for r in range(1, n_dev):
        pl.semaphore_signal(barrier, inc=1, device_id=dev((me + r) % n_dev), device_id_type=MESH)

    def gy_copy(block, lo, n, s, to):
        ref = gy_all.at[block, pl.ds(lo, n), :]
        return Once(pltpu.make_async_remote_copy(src_ref=ref, dst_ref=ref, send_sem=ag_ssem.at[s], recv_sem=ag_rsem.at[s], device_id=dev(to), device_id_type=MESH), log, True)

    right = chip(1) * 2 + c
    left = chip(-1) * 2 + c
    far = chip(2) * 2 + c
    to_r0 = gy_copy(me, 0, hrow, 0, right)
    to_l1 = gy_copy(me, hrow, hrow, 1, left)
    to_r1 = gy_copy(me, hrow, hrow, 2, right)
    to_l0 = gy_copy(me, 0, hrow, 3, left)
    to_p = gy_copy(me, 0, tok, 4, partner)
    fw_r = gy_copy(left, 0, hrow, 5, right)
    fw_l = gy_copy(right, hrow, hrow, 6, left)
    p_l0 = gy_copy(left, 0, hrow, 7, partner)
    p_r1 = gy_copy(right, hrow, hrow, 8, partner)
    p_l1 = gy_copy(left, hrow, hrow, 9, partner)
    p_r0 = gy_copy(right, 0, hrow, 10, partner)
    p_f0 = gy_copy(far, 0, hrow, 11, partner)
    p_f1 = gy_copy(far, hrow, hrow, 12, partner)

    pl.semaphore_wait(barrier, n_dev - 1)
    ld_gy.wait()
    for cp in (to_r0, to_l1, to_p):
        cp.start()

    for cp in ld_small:
        cp.wait()
    cnt = jnp.zeros(idx.shape, jnp.int32)
    for e in range(n_loc * n_dev):
        cnt = jnp.where(idx[...] == e, counts[0, e], cnt)
    keep = (slot[...] >= 0) & (slot[...] < cnt)
    meta[me, 1] = jnp.where(keep, idx[...] * cap + slot[...], -1).astype(F32)

    meta_cp = {}
    for d in range(n_chip):
        for k in range(2):
            if d == 0 and k == 0:
                continue
            s = d * 2 + k - 1
            cp = Once(pltpu.make_async_remote_copy(src_ref=meta.at[me], dst_ref=meta.at[me], send_sem=meta_ssem.at[s], recv_sem=meta_rsem.at[s],
                                                   device_id=dev(chip(d) * 2 + (c if k == 0 else 1 - c)), device_id_type=MESH), log, True)
            cp.start()
            meta_cp[d, k] = cp
    to_r1.start()
    to_l0.start()

    def meta_wait(d):
        for k in range(2):
            if (d, k) != (0, 0):
                meta_cp[(n_chip - d) % n_chip, k].wait_recv()

    ld_h1.wait()
    ld_h3.wait()
    rstep = 32

    @pl.loop(0, n_loc * (h1.shape[1] // rstep))
    def _(i):
        e = i // (h1.shape[1] // rstep)
        r = pl.multiple_of((i % (h1.shape[1] // rstep)) * rstep, rstep)
        a = h1[e, pl.ds(r, rstep), :].astype(F32)
        b = h3[e, pl.ds(r, rstep), :].astype(F32)
        g = jax.nn.sigmoid(a)
        s = a * g
        a_buf[e, pl.ds(r, rstep), :] = (s * b).astype(BF16)
        fs[e, pl.ds(r, rstep), pl.ds(0, ffn)] = b * g * (1.0 + a * (1.0 - g))
        fs[e, pl.ds(r, rstep), pl.ds(ffn, ffn)] = s


    def prep(h):
        rel = meta[h, 1] - (me * (n_loc * cap)).astype(F32)
        gate = meta[h, 0]
        rows = lax.broadcasted_iota(jnp.int32, (n_loc * cap, tok), 0).astype(F32)
        sel = jnp.zeros((n_loc * cap, tok), F32)
        gsel = jnp.zeros((n_loc * cap, tok), F32)
        for k in range(top_k):
            hit = rows == rel[k:k + 1, :]
            sel = jnp.where(hit, 1.0, sel)
            gsel = jnp.where(hit, gate[k:k + 1, :], gsel)
        grow[h] = jnp.sum(gsel, axis=1, keepdims=True)
        pmat[h] = sel.astype(BF16)
        pt[h] = sel.T.astype(BF16)

    def build(h):
        picked = jnp.dot(pmat[h], gy_all[h], preferred_element_type=F32)
        rows_d = (grow[h] * picked).astype(BF16)
        for e in range(n_loc):
            d_buf[e, pl.ds(pl.multiple_of(h * cap, cap), cap), :] = rows_d[e * cap:(e + 1) * cap]

    def pair_copy(q, s, lo):
        return Once(pltpu.make_async_remote_copy(src_ref=psend.at[q, lo], dst_ref=pairin.at[q, lo],
                                                 send_sem=pair_ssem.at[s], recv_sem=pair_rsem.at[s], device_id=dev(partner), device_id_type=MESH), log, True)

    def rows_of(ref, e, q):
        return ref[e, pl.ds(pl.multiple_of(q * (2 * cap), 2 * cap), 2 * cap), :]

    def hidden(qs):
        for e in range(n_loc):
            d = jnp.concatenate([rows_of(d_buf, e, q) for q in qs], axis=0)
            da = lax.dot_general(d, wd[e], NT, preferred_element_type=F32).astype(BF16).astype(F32)
            da2 = jnp.concatenate([da, da], axis=1)
            for i, q in enumerate(qs):
                dh = (da2[i * 2 * cap:(i + 1) * 2 * cap] * rows_of(fs, e, q)).astype(BF16)
                dh_buf[e, pl.ds(pl.multiple_of(q * (2 * cap), 2 * cap), 2 * cap), :] = dh

    sgn = 1 - 2 * c
    pair_cps = {}

    chunk = model // SUBS

    def back(roles, qs, hf):
        cols = pl.ds(hf * chunk, chunk)

        for e in range(n_loc):
            dh = jnp.concatenate([rows_of(dh_buf, e, q) for q in qs], axis=0)
            r = lax.dot_general(dh, wcat[e, cols, :], NT, preferred_element_type=F32).astype(BF16)
            for i in range(len(qs)):
                for j in range(2):
                    rbuf[i, j, pl.ds(e * cap, cap), :] = r[(i * 2 + j) * cap:(i * 2 + j + 1) * cap]

        for i, q in enumerate(qs):
            psend[q, hf] = jnp.dot(pt[q * 2 + 1 - c], rbuf[i, 1 - c], preferred_element_type=F32)
        for i, role in enumerate(roles):
            cp = pair_copy(qs[i], role * SUBS + hf, hf)
            cp.start()
            pair_cps[role, hf] = cp
        for i, q in enumerate(qs):
            own[q, hf] = jnp.dot(pt[q * 2 + c], rbuf[i, c], preferred_element_type=F32)

    def ring_copy(st, s):
        k = st * SUBS + s
        return Once(pltpu.make_async_remote_copy(src_ref=rsend.at[k], dst_ref=rrecv.at[k], send_sem=ring_ssem.at[k], recv_sem=ring_rsem.at[k],
                                                 device_id=dev(chip(sgn) * 2 + c), device_id_type=MESH), log, True)

    ring = {(st, s): ring_copy(st, s) for st in range(2) for s in range(SUBS)}
    stops = ((0, chip(-sgn)), (2, chip(2)), (1, chip(sgn)))

    def pair_sum(role, s, q):
        pair_cps[role, s].wait_recv()
        return own[q, s] + pairin[q, s]

    def ring_step(st, s):
        role, q = stops[st]
        v = pair_sum(role, s, q)
        if st > 0:
            ring[st - 1, s].wait_recv()
            v = v + rrecv[(st - 1) * SUBS + s]
        if st < 2:
            rsend[st * SUBS + s] = v
            ring[st, s].start()
        else:
            tail[s] = v

    def finish():
        for cp in log:
            cp.finish()

    meta_wait(0)
    prep(x * 2)
    prep(x * 2 + 1)
    to_p.wait_recv()
    build(x * 2)
    build(x * 2 + 1)
    ld_wd.wait()
    hidden([x])
    to_r0.wait_recv()
    fw_r.start()
    p_l0.start()
    to_l1.wait_recv()
    fw_l.start()
    p_r1.start()
    for d in (-1, 1):
        meta_wait(d)
        for i in range(2):
            prep(chip(d) * 2 + i)
    ld_wg.wait()
    ld_wu.wait()
    for s in range(3):
        back((3,), [x], s)
    to_r1.wait_recv()
    p_l1.start()
    to_l0.wait_recv()
    p_r0.start()
    build(left)
    build(right)
    meta_wait(2)
    prep(chip(2) * 2)
    prep(chip(2) * 2 + 1)
    p_l0.wait_recv()
    p_l1.wait_recv()
    build(chip(-1) * 2 + 1 - c)
    p_r0.wait_recv()
    p_r1.wait_recv()
    build(chip(1) * 2 + 1 - c)
    near = [chip(sgn), chip(-sgn)]
    hidden(near)
    back((0, 1), near, 0)
    back((0, 1), near, 1)
    ring_step(0, 0)
    fw_r.wait_recv()
    p_f0.start()
    fw_l.wait_recv()
    p_f1.start()
    for s in range(2, SUBS):
        back((0, 1), near, s)
        ring_step(0, s - 1)
    build(far)
    ring_step(0, SUBS - 1)
    ld_x = load(x_hbm, x_buf, 7)
    ld_yr = load(yr_hbm, yr, 1)
    p_f0.wait_recv()
    p_f1.wait_recv()
    build(chip(2) * 2 + 1 - c)
    hidden([chip(2)])
    back((2,), [chip(2)], 0)
    for s in range(1, SUBS):
        back((2,), [chip(2)], s)
        ring_step(1, s - 1)
    ring_step(1, SUBS - 1)
    back((3,), [x], 3)

    ld_yr.wait()
    step = 16

    @pl.loop(0, tok // step)
    def _(i):
        t = pl.multiple_of(i * step, step)
        g = gy_all[me, pl.ds(t, step), :].astype(F32)
        y = yr[pl.ds(t, step), :, :].astype(F32)
        gg_rows[pl.ds(t, step), :] = jnp.sum(y * g[:, None, :], axis=2)

    gg_out[...] = gg_rows[...].T

    for s in range(SUBS):
        base_out[s] = pair_sum(3, s, x)
    for s in range(SUBS):
        ring_step(2, s)

    finish()


def weight_kernel(js, x_ref, dh_ref, a_ref, d_ref, gg_ref, gg_out, gwg, gwu, gwd, gbuf, dbuf, sem):
    n_loc, model, ffn = gwg.shape
    xc, ac = model // js, ffn // js
    gg_out[...] = gg_ref[...]

    def copies(i):
        e, j, b = i // js, i % js, i % BUFS
        rows, arows = pl.ds(j * xc, xc), pl.ds(j * ac, ac)
        return (pltpu.make_async_copy(gbuf.at[b, 0], gwg.at[e, rows, :], sem.at[b, 0]),
                pltpu.make_async_copy(gbuf.at[b, 1], gwu.at[e, rows, :], sem.at[b, 1]),
                pltpu.make_async_copy(dbuf.at[b], gwd.at[e, arows, :], sem.at[b, 2]))

    steps = n_loc * js
    for i in range(steps):
        e, j, b = i // js, i % js, i % BUFS
        if i >= BUFS:
            for cp in copies(i - BUFS):
                cp.wait()
        r = lax.dot_general(x_ref[e, :, pl.ds(j * xc, xc)], dh_ref[e], TN, preferred_element_type=F32)
        gbuf[b, 0] = r[:, :ffn]
        gbuf[b, 1] = r[:, ffn:]
        dbuf[b] = lax.dot_general(a_ref[e, :, pl.ds(j * ac, ac)], d_ref[e], TN, preferred_element_type=F32)
        for cp in copies(i):
            cp.start()
    for i in range(steps - BUFS, steps):
        for cp in copies(i):
            cp.wait()


def finish_kernel(base, got, gx_out):
    chunk = got.shape[2]
    for s in range(SUBS):
        gx_out[:, pl.ds(s * chunk, chunk)] = (base[s] + got[s]).astype(BF16)


def solution(mesh):
    n_dev = mesh.shape["ep"]
    rows_spec = P(("dp", "ep"), None)
    cube_spec = P(("dp", "ep"), None, None)
    weight_spec = P("ep", None, None)

    def local_step(grad_y, gate_vals, topk_idx, slot_ids, pair_counts, y_routed, x_disp, h_gate, h_up, w_gate, w_up, w_down):
        n_loc, ffn, model = w_down.shape
        tok, top_k = topk_idx.shape
        rows = x_disp.shape[1]
        cap = rows // n_dev
        n_chip = n_dev // 2
        vm = pl.BlockSpec(memory_space=pltpu.VMEM)
        hbm = pl.BlockSpec(memory_space=pl.ANY)
        dma = pltpu.SemaphoreType.DMA
        vs = pltpu.VMEM
        tail = vs((SUBS, tok, model // SUBS), F32)
        js = 2
        base, last, gg, d_rows, dh, act, x_rows = pl.pallas_call(
            functools.partial(exchange_kernel, n_dev, cap),
            out_shape=(tail, tail, pltpu.VMEM((top_k, tok), F32), pltpu.VMEM((n_loc, rows, model), BF16),
                       pltpu.VMEM((n_loc, rows, 2 * ffn), BF16), pltpu.VMEM((n_loc, rows, ffn), BF16), pltpu.VMEM((n_loc, rows, model), BF16)),
            in_specs=[hbm] * 12,
            out_specs=(vm,) * 7,
            scratch_shapes=[
                pltpu.SMEM(pair_counts.shape, jnp.int32),
                pltpu.VMEM((top_k, tok), jnp.int32),
                pltpu.VMEM((top_k, tok), jnp.int32),
                pltpu.VMEM((n_dev, tok, model), BF16),
                pltpu.VMEM((tok, top_k, model), BF16),
                pltpu.VMEM((n_loc, rows, ffn), BF16),
                pltpu.VMEM((n_loc, rows, ffn), BF16),
                pltpu.VMEM((n_loc, model, 2 * ffn), BF16),
                pltpu.VMEM((n_loc, ffn, model), BF16),
                pltpu.VMEM((n_loc, rows, 2 * ffn), F32),
                pltpu.VMEM((tok, top_k), F32),
                pltpu.VMEM((n_dev, 2, top_k, tok), F32),
                pltpu.VMEM((n_dev, n_loc * cap, tok), BF16),
                pltpu.VMEM((n_dev, n_loc * cap, 1), F32),
                pltpu.VMEM((n_dev, tok, n_loc * cap), BF16),
                pltpu.VMEM((2, 2, n_loc * cap, model // SUBS), BF16),
                pltpu.VMEM((n_chip, SUBS, tok, model // SUBS), F32),
                pltpu.VMEM((n_chip, SUBS, tok, model // SUBS), F32),
                pltpu.VMEM((n_chip, SUBS, tok, model // SUBS), F32),
                pltpu.VMEM((2 * SUBS, tok, model // SUBS), F32),
                pltpu.VMEM((2 * SUBS, tok, model // SUBS), F32),
                dma((12,)), dma((n_dev - 1,)), dma((n_dev - 1,)), dma((13,)), dma((13,)),
                dma((SUBS * n_chip,)), dma((SUBS * n_chip,)), dma((2 * SUBS,)), dma((2 * SUBS,)),
            ],
            compiler_params=pltpu.CompilerParams(collective_id=0, has_side_effects=True, vmem_limit_bytes=44 * 1024 * 1024),
            name="exchange",
        )(pair_counts, gate_vals.T, topk_idx.T, slot_ids.T, grad_y, y_routed, h_gate, h_up, w_gate, w_up, w_down, x_disp)
        hops = [(i, ((i // 2 + 1 - 2 * (i % 2)) % n_chip) * 2 + i % 2) for i in range(n_dev)]
        got = lax.ppermute(last, "ep", hops)
        gg, gwg, gwu, gwd = pl.pallas_call(
            functools.partial(weight_kernel, js),
            out_shape=(jax.ShapeDtypeStruct((top_k, tok), F32), jax.ShapeDtypeStruct((n_loc, model, ffn), F32),
                       jax.ShapeDtypeStruct((n_loc, model, ffn), F32), jax.ShapeDtypeStruct((n_loc, ffn, model), F32)),
            in_specs=[vm] * 5,
            out_specs=(vm, hbm, hbm, hbm),
            scratch_shapes=[pltpu.VMEM((BUFS, 2, model // js, ffn), F32), pltpu.VMEM((BUFS, ffn // js, model), F32), dma((BUFS, 3))],
            compiler_params=pltpu.CompilerParams(vmem_limit_bytes=24 * 1024 * 1024),
            cost_estimate=pl.CostEstimate(flops=6 * n_loc * rows * model * ffn, bytes_accessed=12 * n_loc * model * ffn, transcendentals=0),
            name="weights",
        )(x_rows, dh, act, d_rows, gg)
        gx = pl.pallas_call(
            finish_kernel,
            out_shape=jax.ShapeDtypeStruct((tok, model), BF16),
            in_specs=[vm] * 2,
            out_specs=vm,
            compiler_params=pltpu.CompilerParams(vmem_limit_bytes=4 * 1024 * 1024),
            name="finish",
        )(base, got)
        return gx, gg.T, gwg, gwu, gwd

    return jax.shard_map(local_step, mesh=mesh, in_specs=(rows_spec, rows_spec, rows_spec, rows_spec, rows_spec, cube_spec, cube_spec, cube_spec, cube_spec, weight_spec, weight_spec, weight_spec), out_specs=(rows_spec, rows_spec, cube_spec, cube_spec, cube_spec), check_vma=False)
```

```python
import functools

import jax
import jax.numpy as jnp
from jax import lax
from jax.experimental import pallas as pl
from jax.experimental.pallas import tpu as pltpu
from jax.sharding import PartitionSpec as P

MESH = pl.DeviceIdType.MESH
F32 = jnp.float32
BF16 = jnp.bfloat16
NT = (((1,), (1,)), ((), ()))
TN = (((0,), (0,)), ((), ()))
SUBS = 4
BUFS = 6


class Once:
    def __init__(self, cp, log, remote):
        self.cp, self.log, self.remote, self.got = cp, log, remote, False

    def start(self):
        self.cp.start()
        self.log.append(self)

    def wait(self):
        if not self.got:
            self.got = True
            self.cp.wait()

    def wait_recv(self):
        if not self.got:
            self.got = True
            self.cp.wait_recv()

    def finish(self):
        if self.remote:
            self.wait_recv()
            self.cp.wait_send()
        else:
            self.wait()


def exchange_kernel(n_dev, cap, counts_hbm, gates_hbm, idx_hbm, slot_hbm, gy_hbm, yr_hbm, h1_hbm, h3_hbm, wg_hbm, wu_hbm, wd_hbm, x_hbm,
                    base_out, tail, gg_out, d_buf, dh_buf, a_buf, x_buf,
                    counts, idx, slot, gy_all, yr, h1, h3, wcat, wd, fs, gg_rows, meta, pmat, grow, pt, rbuf, own, psend, pairin, rsend, rrecv,
                    loc_sem, meta_ssem, meta_rsem, ag_ssem, ag_rsem, pair_ssem, pair_rsem, ring_ssem, ring_rsem):
    n_loc, ffn, model = wd.shape
    top_k, tok = idx.shape
    n_chip = n_dev // 2
    half = model // 2
    hrow = tok // 2
    log = []
    me = lax.axis_index("ep")
    x = me // 2
    c = me % 2
    partner = x * 2 + (1 - c)

    def chip(d):
        return (x + d + n_chip) % n_chip

    def dev(i):
        return {"ep": i}

    def load(src, dst, s):
        cp = Once(pltpu.make_async_copy(src, dst, loc_sem.at[s]), log, False)
        cp.start()
        return cp

    ld_gy = load(gy_hbm, gy_all.at[me], 0)
    ld_small = (load(counts_hbm, counts, 8), load(idx_hbm, idx, 9), load(slot_hbm, slot, 10), load(gates_hbm, meta.at[me, 0], 11))
    ld_h1 = load(h1_hbm, h1, 2)
    ld_h3 = load(h3_hbm, h3, 3)
    ld_wd = load(wd_hbm, wd, 4)
    ld_wg = load(wg_hbm, wcat.at[:, :, pl.ds(0, ffn)], 5)
    ld_wu = load(wu_hbm, wcat.at[:, :, pl.ds(ffn, ffn)], 6)

    barrier = pltpu.get_barrier_semaphore()
    for r in range(1, n_dev):
        pl.semaphore_signal(barrier, inc=1, device_id=dev((me + r) % n_dev), device_id_type=MESH)

    def gy_copy(block, lo, n, s, to):
        ref = gy_all.at[block, pl.ds(lo, n), :]
        return Once(pltpu.make_async_remote_copy(src_ref=ref, dst_ref=ref, send_sem=ag_ssem.at[s], recv_sem=ag_rsem.at[s], device_id=dev(to), device_id_type=MESH), log, True)

    right = chip(1) * 2 + c
    left = chip(-1) * 2 + c
    far = chip(2) * 2 + c
    to_r0 = gy_copy(me, 0, hrow, 0, right)
    to_l1 = gy_copy(me, hrow, hrow, 1, left)
    to_r1 = gy_copy(me, hrow, hrow, 2, right)
    to_l0 = gy_copy(me, 0, hrow, 3, left)
    to_p = gy_copy(me, 0, tok, 4, partner)
    fw_r = gy_copy(left, 0, hrow, 5, right)
    fw_l = gy_copy(right, hrow, hrow, 6, left)
    p_l0 = gy_copy(left, 0, hrow, 7, partner)
    p_r1 = gy_copy(right, hrow, hrow, 8, partner)
    p_l1 = gy_copy(left, hrow, hrow, 9, partner)
    p_r0 = gy_copy(right, 0, hrow, 10, partner)
    p_f0 = gy_copy(far, 0, hrow, 11, partner)
    p_f1 = gy_copy(far, hrow, hrow, 12, partner)

    pl.semaphore_wait(barrier, n_dev - 1)
    ld_gy.wait()
    for cp in (to_r0, to_l1, to_p):
        cp.start()

    for cp in ld_small:
        cp.wait()
    cnt = jnp.zeros(idx.shape, jnp.int32)
    for e in range(n_loc * n_dev):
        cnt = jnp.where(idx[...] == e, counts[0, e], cnt)
    keep = (slot[...] >= 0) & (slot[...] < cnt)
    meta[me, 1] = jnp.where(keep, idx[...] * cap + slot[...], -1).astype(F32)

    meta_cp = {}
    for d in range(n_chip):
        for k in range(2):
            if d == 0 and k == 0:
                continue
            s = d * 2 + k - 1
            cp = Once(pltpu.make_async_remote_copy(src_ref=meta.at[me], dst_ref=meta.at[me], send_sem=meta_ssem.at[s], recv_sem=meta_rsem.at[s],
                                                   device_id=dev(chip(d) * 2 + (c if k == 0 else 1 - c)), device_id_type=MESH), log, True)
            cp.start()
            meta_cp[d, k] = cp
    to_r1.start()
    to_l0.start()

    def meta_wait(d):
        for k in range(2):
            if (d, k) != (0, 0):
                meta_cp[(n_chip - d) % n_chip, k].wait_recv()

    ld_h1.wait()
    ld_h3.wait()
    rstep = 32

    @pl.loop(0, n_loc * (h1.shape[1] // rstep))
    def _(i):
        e = i // (h1.shape[1] // rstep)
        r = pl.multiple_of((i % (h1.shape[1] // rstep)) * rstep, rstep)
        a = h1[e, pl.ds(r, rstep), :].astype(F32)
        b = h3[e, pl.ds(r, rstep), :].astype(F32)
        g = jax.nn.sigmoid(a)
        s = a * g
        a_buf[e, pl.ds(r, rstep), :] = (s * b).astype(BF16)
        fs[e, pl.ds(r, rstep), pl.ds(0, ffn)] = b * g * (1.0 + a * (1.0 - g))
        fs[e, pl.ds(r, rstep), pl.ds(ffn, ffn)] = s


    def prep(h):
        rel = meta[h, 1] - (me * (n_loc * cap)).astype(F32)
        gate = meta[h, 0]
        rows = lax.broadcasted_iota(jnp.int32, (n_loc * cap, tok), 0).astype(F32)
        sel = jnp.zeros((n_loc * cap, tok), F32)
        gsel = jnp.zeros((n_loc * cap, tok), F32)
        for k in range(top_k):
            hit = rows == rel[k:k + 1, :]
            sel = jnp.where(hit, 1.0, sel)
            gsel = jnp.where(hit, gate[k:k + 1, :], gsel)
        grow[h] = jnp.sum(gsel, axis=1, keepdims=True)
        pmat[h] = sel.astype(BF16)
        pt[h] = sel.T.astype(BF16)

    def build(h):
        picked = jnp.dot(pmat[h], gy_all[h], preferred_element_type=F32)
        rows_d = (grow[h] * picked).astype(BF16)
        for e in range(n_loc):
            d_buf[e, pl.ds(pl.multiple_of(h * cap, cap), cap), :] = rows_d[e * cap:(e + 1) * cap]

    def pair_copy(q, s, lo):
        return Once(pltpu.make_async_remote_copy(src_ref=psend.at[q, lo], dst_ref=pairin.at[q, lo],
                                                 send_sem=pair_ssem.at[s], recv_sem=pair_rsem.at[s], device_id=dev(partner), device_id_type=MESH), log, True)

    def rows_of(ref, e, q):
        return ref[e, pl.ds(pl.multiple_of(q * (2 * cap), 2 * cap), 2 * cap), :]

    def hidden(qs):
        for e in range(n_loc):
            d = jnp.concatenate([rows_of(d_buf, e, q) for q in qs], axis=0)
            da = lax.dot_general(d, wd[e], NT, preferred_element_type=F32).astype(BF16).astype(F32)
            da2 = jnp.concatenate([da, da], axis=1)
            for i, q in enumerate(qs):
                dh = (da2[i * 2 * cap:(i + 1) * 2 * cap] * rows_of(fs, e, q)).astype(BF16)
                dh_buf[e, pl.ds(pl.multiple_of(q * (2 * cap), 2 * cap), 2 * cap), :] = dh

    sgn = 1 - 2 * c
    pair_cps = {}

    chunk = model // SUBS

    def back(roles, qs, hf):
        cols = pl.ds(hf * chunk, chunk)

        for e in range(n_loc):
            dh = jnp.concatenate([rows_of(dh_buf, e, q) for q in qs], axis=0)
            r = lax.dot_general(dh, wcat[e, cols, :], NT, preferred_element_type=F32).astype(BF16)
            for i in range(len(qs)):
                for j in range(2):
                    rbuf[i, j, pl.ds(e * cap, cap), :] = r[(i * 2 + j) * cap:(i * 2 + j + 1) * cap]

        for i, (role, q) in enumerate(zip(roles, qs)):
            psend[q, hf] = jnp.dot(pt[q * 2 + 1 - c], rbuf[i, 1 - c], preferred_element_type=F32)
            cp = pair_copy(q, role * SUBS + hf, hf)
            cp.start()
            pair_cps[role, hf] = cp
        for i, q in enumerate(qs):
            own[q, hf] = jnp.dot(pt[q * 2 + c], rbuf[i, c], preferred_element_type=F32)

    def ring_copy(st, s):
        k = st * SUBS + s
        return Once(pltpu.make_async_remote_copy(src_ref=rsend.at[k], dst_ref=rrecv.at[k], send_sem=ring_ssem.at[k], recv_sem=ring_rsem.at[k],
                                                 device_id=dev(chip(sgn) * 2 + c), device_id_type=MESH), log, True)

    ring = {(st, s): ring_copy(st, s) for st in range(2) for s in range(SUBS)}
    stops = ((0, chip(-sgn)), (2, chip(2)), (1, chip(sgn)))

    def pair_sum(role, s, q):
        pair_cps[role, s].wait_recv()
        return own[q, s] + pairin[q, s]

    def ring_step(st, s):
        role, q = stops[st]
        v = pair_sum(role, s, q)
        if st > 0:
            ring[st - 1, s].wait_recv()
            v = v + rrecv[(st - 1) * SUBS + s]
        if st < 2:
            rsend[st * SUBS + s] = v
            ring[st, s].start()
        else:
            tail[s] = v

    def finish():
        for cp in log:
            cp.finish()

    meta_wait(0)
    prep(x * 2)
    prep(x * 2 + 1)
    to_p.wait_recv()
    build(x * 2)
    build(x * 2 + 1)
    ld_wd.wait()
    hidden([x])
    to_r0.wait_recv()
    fw_r.start()
    p_l0.start()
    to_l1.wait_recv()
    fw_l.start()
    p_r1.start()
    for d in (-1, 1):
        meta_wait(d)
        for i in range(2):
            prep(chip(d) * 2 + i)
    ld_wg.wait()
    ld_wu.wait()
    for s in range(3):
        back((3,), [x], s)
    to_r1.wait_recv()
    p_l1.start()
    to_l0.wait_recv()
    p_r0.start()
    build(left)
    build(right)
    meta_wait(2)
    prep(chip(2) * 2)
    prep(chip(2) * 2 + 1)
    p_l0.wait_recv()
    p_l1.wait_recv()
    build(chip(-1) * 2 + 1 - c)
    p_r0.wait_recv()
    p_r1.wait_recv()
    build(chip(1) * 2 + 1 - c)
    near = [chip(sgn), chip(-sgn)]
    hidden(near)
    back((0, 1), near, 0)
    back((0, 1), near, 1)
    ring_step(0, 0)
    fw_r.wait_recv()
    p_f0.start()
    fw_l.wait_recv()
    p_f1.start()
    for s in range(2, SUBS):
        back((0, 1), near, s)
        ring_step(0, s - 1)
    build(far)
    ring_step(0, SUBS - 1)
    ld_x = load(x_hbm, x_buf, 7)
    ld_yr = load(yr_hbm, yr, 1)
    p_f0.wait_recv()
    p_f1.wait_recv()
    build(chip(2) * 2 + 1 - c)
    hidden([chip(2)])
    back((2,), [chip(2)], 0)
    for s in range(1, SUBS):
        back((2,), [chip(2)], s)
        ring_step(1, s - 1)
    ring_step(1, SUBS - 1)
    back((3,), [x], 3)

    ld_yr.wait()
    step = 16

    @pl.loop(0, tok // step)
    def _(i):
        t = pl.multiple_of(i * step, step)
        g = gy_all[me, pl.ds(t, step), :].astype(F32)
        y = yr[pl.ds(t, step), :, :].astype(F32)
        gg_rows[pl.ds(t, step), :] = jnp.sum(y * g[:, None, :], axis=2)

    gg_out[...] = gg_rows[...].T

    for s in range(SUBS):
        base_out[s] = pair_sum(3, s, x)
    for s in range(SUBS):
        ring_step(2, s)

    finish()


def weight_kernel(js, x_ref, dh_ref, a_ref, d_ref, gg_ref, gg_out, gwg, gwu, gwd, gbuf, dbuf, sem):
    n_loc, model, ffn = gwg.shape
    xc, ac = model // js, ffn // js
    gg_out[...] = gg_ref[...]

    def copies(i):
        e, j, b = i // js, i % js, i % BUFS
        rows, arows = pl.ds(j * xc, xc), pl.ds(j * ac, ac)
        return (pltpu.make_async_copy(gbuf.at[b, 0], gwg.at[e, rows, :], sem.at[b, 0]),
                pltpu.make_async_copy(gbuf.at[b, 1], gwu.at[e, rows, :], sem.at[b, 1]),
                pltpu.make_async_copy(dbuf.at[b], gwd.at[e, arows, :], sem.at[b, 2]))

    steps = n_loc * js
    for i in range(steps):
        e, j, b = i // js, i % js, i % BUFS
        if i >= BUFS:
            for cp in copies(i - BUFS):
                cp.wait()
        r = lax.dot_general(x_ref[e, :, pl.ds(j * xc, xc)], dh_ref[e], TN, preferred_element_type=F32)
        gbuf[b, 0] = r[:, :ffn]
        gbuf[b, 1] = r[:, ffn:]
        dbuf[b] = lax.dot_general(a_ref[e, :, pl.ds(j * ac, ac)], d_ref[e], TN, preferred_element_type=F32)
        for cp in copies(i):
            cp.start()
    for i in range(steps - BUFS, steps):
        for cp in copies(i):
            cp.wait()


def finish_kernel(base, got, gx_out):
    chunk = got.shape[2]
    for s in range(SUBS):
        gx_out[:, pl.ds(s * chunk, chunk)] = (base[s] + got[s]).astype(BF16)


def solution(mesh):
    n_dev = mesh.shape["ep"]
    rows_spec = P(("dp", "ep"), None)
    cube_spec = P(("dp", "ep"), None, None)
    weight_spec = P("ep", None, None)

    def local_step(grad_y, gate_vals, topk_idx, slot_ids, pair_counts, y_routed, x_disp, h_gate, h_up, w_gate, w_up, w_down):
        n_loc, ffn, model = w_down.shape
        tok, top_k = topk_idx.shape
        rows = x_disp.shape[1]
        cap = rows // n_dev
        n_chip = n_dev // 2
        vm = pl.BlockSpec(memory_space=pltpu.VMEM)
        hbm = pl.BlockSpec(memory_space=pl.ANY)
        dma = pltpu.SemaphoreType.DMA
        vs = pltpu.VMEM
        tail = vs((SUBS, tok, model // SUBS), F32)
        js = 4
        base, last, gg, d_rows, dh, act, x_rows = pl.pallas_call(
            functools.partial(exchange_kernel, n_dev, cap),
            out_shape=(tail, tail, pltpu.VMEM((top_k, tok), F32), pltpu.VMEM((n_loc, rows, model), BF16),
                       pltpu.VMEM((n_loc, rows, 2 * ffn), BF16), pltpu.VMEM((n_loc, rows, ffn), BF16), pltpu.VMEM((n_loc, rows, model), BF16)),
            in_specs=[hbm] * 12,
            out_specs=(vm,) * 7,
            scratch_shapes=[
                pltpu.SMEM(pair_counts.shape, jnp.int32),
                pltpu.VMEM((top_k, tok), jnp.int32),
                pltpu.VMEM((top_k, tok), jnp.int32),
                pltpu.VMEM((n_dev, tok, model), BF16),
                pltpu.VMEM((tok, top_k, model), BF16),
                pltpu.VMEM((n_loc, rows, ffn), BF16),
                pltpu.VMEM((n_loc, rows, ffn), BF16),
                pltpu.VMEM((n_loc, model, 2 * ffn), BF16),
                pltpu.VMEM((n_loc, ffn, model), BF16),
                pltpu.VMEM((n_loc, rows, 2 * ffn), F32),
                pltpu.VMEM((tok, top_k), F32),
                pltpu.VMEM((n_dev, 2, top_k, tok), F32),
                pltpu.VMEM((n_dev, n_loc * cap, tok), BF16),
                pltpu.VMEM((n_dev, n_loc * cap, 1), F32),
                pltpu.VMEM((n_dev, tok, n_loc * cap), BF16),
                pltpu.VMEM((2, 2, n_loc * cap, model // SUBS), BF16),
                pltpu.VMEM((n_chip, SUBS, tok, model // SUBS), F32),
                pltpu.VMEM((n_chip, SUBS, tok, model // SUBS), F32),
                pltpu.VMEM((n_chip, SUBS, tok, model // SUBS), F32),
                pltpu.VMEM((2 * SUBS, tok, model // SUBS), F32),
                pltpu.VMEM((2 * SUBS, tok, model // SUBS), F32),
                dma((12,)), dma((n_dev - 1,)), dma((n_dev - 1,)), dma((13,)), dma((13,)),
                dma((SUBS * n_chip,)), dma((SUBS * n_chip,)), dma((2 * SUBS,)), dma((2 * SUBS,)),
            ],
            compiler_params=pltpu.CompilerParams(collective_id=0, has_side_effects=True, vmem_limit_bytes=44 * 1024 * 1024),
            name="exchange",
        )(pair_counts, gate_vals.T, topk_idx.T, slot_ids.T, grad_y, y_routed, h_gate, h_up, w_gate, w_up, w_down, x_disp)
        hops = [(i, ((i // 2 + 1 - 2 * (i % 2)) % n_chip) * 2 + i % 2) for i in range(n_dev)]
        got = lax.ppermute(last, "ep", hops)
        gg, gwg, gwu, gwd = pl.pallas_call(
            functools.partial(weight_kernel, js),
            out_shape=(jax.ShapeDtypeStruct((top_k, tok), F32), jax.ShapeDtypeStruct((n_loc, model, ffn), F32),
                       jax.ShapeDtypeStruct((n_loc, model, ffn), F32), jax.ShapeDtypeStruct((n_loc, ffn, model), F32)),
            in_specs=[vm] * 5,
            out_specs=(vm, hbm, hbm, hbm),
            scratch_shapes=[pltpu.VMEM((BUFS, 2, model // js, ffn), F32), pltpu.VMEM((BUFS, ffn // js, model), F32), dma((BUFS, 3))],
            compiler_params=pltpu.CompilerParams(vmem_limit_bytes=24 * 1024 * 1024),
            cost_estimate=pl.CostEstimate(flops=6 * n_loc * rows * model * ffn, bytes_accessed=12 * n_loc * model * ffn, transcendentals=0),
            name="weights",
        )(x_rows, dh, act, d_rows, gg)
        gx = pl.pallas_call(
            finish_kernel,
            out_shape=jax.ShapeDtypeStruct((tok, model), BF16),
            in_specs=[vm] * 2,
            out_specs=vm,
            compiler_params=pltpu.CompilerParams(vmem_limit_bytes=4 * 1024 * 1024),
            name="finish",
        )(base, got)
        return gx, gg.T, gwg, gwu, gwd

    return jax.shard_map(local_step, mesh=mesh, in_specs=(rows_spec, rows_spec, rows_spec, rows_spec, rows_spec, cube_spec, cube_spec, cube_spec, cube_spec, weight_spec, weight_spec, weight_spec), out_specs=(rows_spec, rows_spec, cube_spec, cube_spec, cube_spec), check_vma=False)
```

```python
import functools

import jax
import jax.numpy as jnp
from jax import lax
from jax.experimental import pallas as pl
from jax.experimental.pallas import tpu as pltpu
from jax.sharding import PartitionSpec as P

MESH = pl.DeviceIdType.MESH
F32 = jnp.float32
BF16 = jnp.bfloat16
NT = (((1,), (1,)), ((), ()))
TN = (((0,), (0,)), ((), ()))
SUBS = 4
BUFS = 3


class Once:
    def __init__(self, cp, log, remote):
        self.cp, self.log, self.remote, self.got = cp, log, remote, False

    def start(self):
        self.cp.start()
        self.log.append(self)

    def wait(self):
        if not self.got:
            self.got = True
            self.cp.wait()

    def wait_recv(self):
        if not self.got:
            self.got = True
            self.cp.wait_recv()

    def finish(self):
        if self.remote:
            self.wait_recv()
            self.cp.wait_send()
        else:
            self.wait()


def exchange_kernel(n_dev, cap, counts_hbm, gates_hbm, idx_hbm, slot_hbm, gy_hbm, yr_hbm, h1_hbm, h3_hbm, wg_hbm, wu_hbm, wd_hbm, x_hbm,
                    base_out, tail, gg_out, d_buf, dh_buf, a_buf, x_buf,
                    counts, idx, slot, gy_all, yr, h1, h3, wcat, wd, fs, gg_rows, meta, pmat, grow, pt, rbuf, own, psend, pairin, rsend, rrecv,
                    loc_sem, meta_ssem, meta_rsem, ag_ssem, ag_rsem, pair_ssem, pair_rsem, ring_ssem, ring_rsem):
    n_loc, ffn, model = wd.shape
    top_k, tok = idx.shape
    n_chip = n_dev // 2
    half = model // 2
    hrow = tok // 2
    log = []
    me = lax.axis_index("ep")
    x = me // 2
    c = me % 2
    partner = x * 2 + (1 - c)

    def chip(d):
        return (x + d + n_chip) % n_chip

    def dev(i):
        return {"ep": i}

    def load(src, dst, s):
        cp = Once(pltpu.make_async_copy(src, dst, loc_sem.at[s]), log, False)
        cp.start()
        return cp

    ld_gy = load(gy_hbm, gy_all.at[me], 0)
    ld_small = (load(counts_hbm, counts, 8), load(idx_hbm, idx, 9), load(slot_hbm, slot, 10), load(gates_hbm, meta.at[me, 0], 11))
    ld_h1 = load(h1_hbm, h1, 2)
    ld_h3 = load(h3_hbm, h3, 3)
    ld_wd = load(wd_hbm, wd, 4)
    ld_wg = load(wg_hbm, wcat.at[:, :, pl.ds(0, ffn)], 5)
    ld_wu = load(wu_hbm, wcat.at[:, :, pl.ds(ffn, ffn)], 6)

    barrier = pltpu.get_barrier_semaphore()
    for r in range(1, n_dev):
        pl.semaphore_signal(barrier, inc=1, device_id=dev((me + r) % n_dev), device_id_type=MESH)

    def gy_copy(block, lo, n, s, to):
        ref = gy_all.at[block, pl.ds(lo, n), :]
        return Once(pltpu.make_async_remote_copy(src_ref=ref, dst_ref=ref, send_sem=ag_ssem.at[s], recv_sem=ag_rsem.at[s], device_id=dev(to), device_id_type=MESH), log, True)

    right = chip(1) * 2 + c
    left = chip(-1) * 2 + c
    far = chip(2) * 2 + c
    to_r0 = gy_copy(me, 0, hrow, 0, right)
    to_l1 = gy_copy(me, hrow, hrow, 1, left)
    to_r1 = gy_copy(me, hrow, hrow, 2, right)
    to_l0 = gy_copy(me, 0, hrow, 3, left)
    to_p = gy_copy(me, 0, tok, 4, partner)
    fw_r = gy_copy(left, 0, hrow, 5, right)
    fw_l = gy_copy(right, hrow, hrow, 6, left)
    p_l0 = gy_copy(left, 0, hrow, 7, partner)
    p_r1 = gy_copy(right, hrow, hrow, 8, partner)
    p_l1 = gy_copy(left, hrow, hrow, 9, partner)
    p_r0 = gy_copy(right, 0, hrow, 10, partner)
    p_f0 = gy_copy(far, 0, hrow, 11, partner)
    p_f1 = gy_copy(far, hrow, hrow, 12, partner)

    pl.semaphore_wait(barrier, n_dev - 1)
    ld_gy.wait()
    for cp in (to_r0, to_l1, to_p):
        cp.start()

    for cp in ld_small:
        cp.wait()
    cnt = jnp.zeros(idx.shape, jnp.int32)
    for e in range(n_loc * n_dev):
        cnt = jnp.where(idx[...] == e, counts[0, e], cnt)
    keep = (slot[...] >= 0) & (slot[...] < cnt)
    meta[me, 1] = jnp.where(keep, idx[...] * cap + slot[...], -1).astype(F32)

    meta_cp = {}
    for d in range(n_chip):
        for k in range(2):
            if d == 0 and k == 0:
                continue
            s = d * 2 + k - 1
            cp = Once(pltpu.make_async_remote_copy(src_ref=meta.at[me], dst_ref=meta.at[me], send_sem=meta_ssem.at[s], recv_sem=meta_rsem.at[s],
                                                   device_id=dev(chip(d) * 2 + (c if k == 0 else 1 - c)), device_id_type=MESH), log, True)
            cp.start()
            meta_cp[d, k] = cp
    to_r1.start()
    to_l0.start()

    def meta_wait(d):
        for k in range(2):
            if (d, k) != (0, 0):
                meta_cp[(n_chip - d) % n_chip, k].wait_recv()

    ld_h1.wait()
    ld_h3.wait()
    rstep = 32

    @pl.loop(0, n_loc * (h1.shape[1] // rstep))
    def _(i):
        e = i // (h1.shape[1] // rstep)
        r = pl.multiple_of((i % (h1.shape[1] // rstep)) * rstep, rstep)
        a = h1[e, pl.ds(r, rstep), :].astype(F32)
        b = h3[e, pl.ds(r, rstep), :].astype(F32)
        g = jax.nn.sigmoid(a)
        s = a * g
        a_buf[e, pl.ds(r, rstep), :] = (s * b).astype(BF16)
        fs[e, pl.ds(r, rstep), pl.ds(0, ffn)] = b * g * (1.0 + a * (1.0 - g))
        fs[e, pl.ds(r, rstep), pl.ds(ffn, ffn)] = s


    def prep(h):
        rel = meta[h, 1] - (me * (n_loc * cap)).astype(F32)
        gate = meta[h, 0]
        rows = lax.broadcasted_iota(jnp.int32, (n_loc * cap, tok), 0).astype(F32)
        sel = jnp.zeros((n_loc * cap, tok), F32)
        gsel = jnp.zeros((n_loc * cap, tok), F32)
        for k in range(top_k):
            hit = rows == rel[k:k + 1, :]
            sel = jnp.where(hit, 1.0, sel)
            gsel = jnp.where(hit, gate[k:k + 1, :], gsel)
        grow[h] = jnp.sum(gsel, axis=1, keepdims=True)
        pmat[h] = sel.astype(BF16)
        pt[h] = sel.T.astype(BF16)

    def build(h):
        picked = jnp.dot(pmat[h], gy_all[h], preferred_element_type=F32)
        rows_d = (grow[h] * picked).astype(BF16)
        for e in range(n_loc):
            d_buf[e, pl.ds(pl.multiple_of(h * cap, cap), cap), :] = rows_d[e * cap:(e + 1) * cap]

    def pair_copy(q, s, lo):
        return Once(pltpu.make_async_remote_copy(src_ref=psend.at[q, lo], dst_ref=pairin.at[q, lo],
                                                 send_sem=pair_ssem.at[s], recv_sem=pair_rsem.at[s], device_id=dev(partner), device_id_type=MESH), log, True)

    def rows_of(ref, e, q):
        return ref[e, pl.ds(pl.multiple_of(q * (2 * cap), 2 * cap), 2 * cap), :]

    def hidden(qs):
        for e in range(n_loc):
            d = jnp.concatenate([rows_of(d_buf, e, q) for q in qs], axis=0)
            da = lax.dot_general(d, wd[e], NT, preferred_element_type=F32).astype(BF16).astype(F32)
            da2 = jnp.concatenate([da, da], axis=1)
            for i, q in enumerate(qs):
                dh = (da2[i * 2 * cap:(i + 1) * 2 * cap] * rows_of(fs, e, q)).astype(BF16)
                dh_buf[e, pl.ds(pl.multiple_of(q * (2 * cap), 2 * cap), 2 * cap), :] = dh

    sgn = 1 - 2 * c
    pair_cps = {}

    chunk = model // SUBS

    def back(roles, qs, hf):
        cols = pl.ds(hf * chunk, chunk)

        for e in range(n_loc):
            dh = jnp.concatenate([rows_of(dh_buf, e, q) for q in qs], axis=0)
            r = lax.dot_general(dh, wcat[e, cols, :], NT, preferred_element_type=F32).astype(BF16)
            for i in range(len(qs)):
                for j in range(2):
                    rbuf[i, j, pl.ds(e * cap, cap), :] = r[(i * 2 + j) * cap:(i * 2 + j + 1) * cap]

        for i, q in enumerate(qs):
            psend[q, hf] = jnp.dot(pt[q * 2 + 1 - c], rbuf[i, 1 - c], preferred_element_type=F32)
        for i, role in enumerate(roles):
            cp = pair_copy(qs[i], role * SUBS + hf, hf)
            cp.start()
            pair_cps[role, hf] = cp
        for i, q in enumerate(qs):
            own[q, hf] = jnp.dot(pt[q * 2 + c], rbuf[i, c], preferred_element_type=F32)

    def ring_copy(st, s):
        k = st * SUBS + s
        return Once(pltpu.make_async_remote_copy(src_ref=rsend.at[k], dst_ref=rrecv.at[k], send_sem=ring_ssem.at[k], recv_sem=ring_rsem.at[k],
                                                 device_id=dev(chip(sgn) * 2 + c), device_id_type=MESH), log, True)

    ring = {(st, s): ring_copy(st, s) for st in range(2) for s in range(SUBS)}
    stops = ((0, chip(-sgn)), (2, chip(2)), (1, chip(sgn)))

    def pair_sum(role, s, q):
        pair_cps[role, s].wait_recv()
        return own[q, s] + pairin[q, s]

    def ring_step(st, s):
        role, q = stops[st]
        v = pair_sum(role, s, q)
        if st > 0:
            ring[st - 1, s].wait_recv()
            v = v + rrecv[(st - 1) * SUBS + s]
        if st < 2:
            rsend[st * SUBS + s] = v
            ring[st, s].start()
        else:
            tail[s] = v

    def finish():
        for cp in log:
            cp.finish()

    meta_wait(0)
    prep(x * 2)
    prep(x * 2 + 1)
    to_p.wait_recv()
    build(x * 2)
    build(x * 2 + 1)
    ld_wd.wait()
    hidden([x])
    to_r0.wait_recv()
    fw_r.start()
    p_l0.start()
    to_l1.wait_recv()
    fw_l.start()
    p_r1.start()
    for d in (-1, 1):
        meta_wait(d)
        for i in range(2):
            prep(chip(d) * 2 + i)
    ld_wg.wait()
    ld_wu.wait()
    back((3,), [x], 0)
    to_r1.wait_recv()
    p_l1.start()
    to_l0.wait_recv()
    p_r0.start()
    build(left)
    build(right)
    meta_wait(2)
    prep(chip(2) * 2)
    prep(chip(2) * 2 + 1)
    p_l0.wait_recv()
    p_l1.wait_recv()
    build(chip(-1) * 2 + 1 - c)
    p_r0.wait_recv()
    p_r1.wait_recv()
    build(chip(1) * 2 + 1 - c)
    near = [chip(sgn), chip(-sgn)]
    hidden(near)
    back((0, 1), near, 0)
    back((0, 1), near, 1)
    ring_step(0, 0)
    fw_r.wait_recv()
    p_f0.start()
    fw_l.wait_recv()
    p_f1.start()
    for s in range(2, SUBS):
        back((0, 1), near, s)
        ring_step(0, s - 1)
    build(far)
    ring_step(0, SUBS - 1)
    ld_x = load(x_hbm, x_buf, 7)
    ld_yr = load(yr_hbm, yr, 1)
    p_f0.wait_recv()
    p_f1.wait_recv()
    build(chip(2) * 2 + 1 - c)
    hidden([chip(2)])
    back((2,), [chip(2)], 0)
    for s in range(1, SUBS):
        back((2,), [chip(2)], s)
        ring_step(1, s - 1)
    ring_step(1, SUBS - 1)
    for s in range(1, SUBS):
        back((3,), [x], s)

    ld_yr.wait()
    step = 16

    @pl.loop(0, tok // step)
    def _(i):
        t = pl.multiple_of(i * step, step)
        g = gy_all[me, pl.ds(t, step), :].astype(F32)
        y = yr[pl.ds(t, step), :, :].astype(F32)
        gg_rows[pl.ds(t, step), :] = jnp.sum(y * g[:, None, :], axis=2)

    gg_out[...] = gg_rows[...].T

    for s in range(SUBS):
        base_out[s] = pair_sum(3, s, x)
    for s in range(SUBS):
        ring_step(2, s)

    finish()


def weight_kernel(js, x_ref, dh_ref, a_ref, d_ref, gg_ref, gg_out, gwg, gwu, gwd, gbuf, dbuf, sem):
    n_loc, model, ffn = gwg.shape
    xc, ac = model // js, ffn // js
    gg_out[...] = gg_ref[...]

    def copies(i):
        e, j, b = i // js, i % js, i % BUFS
        rows, arows = pl.ds(j * xc, xc), pl.ds(j * ac, ac)
        return (pltpu.make_async_copy(gbuf.at[b, 0], gwg.at[e, rows, :], sem.at[b, 0]),
                pltpu.make_async_copy(gbuf.at[b, 1], gwu.at[e, rows, :], sem.at[b, 1]),
                pltpu.make_async_copy(dbuf.at[b], gwd.at[e, arows, :], sem.at[b, 2]))

    steps = n_loc * js
    for i in range(steps):
        e, j, b = i // js, i % js, i % BUFS
        if i >= BUFS:
            for cp in copies(i - BUFS):
                cp.wait()
        r = lax.dot_general(x_ref[e, :, pl.ds(j * xc, xc)], dh_ref[e], TN, preferred_element_type=F32)
        gbuf[b, 0] = r[:, :ffn]
        gbuf[b, 1] = r[:, ffn:]
        dbuf[b] = lax.dot_general(a_ref[e, :, pl.ds(j * ac, ac)], d_ref[e], TN, preferred_element_type=F32)
        for cp in copies(i):
            cp.start()
    for i in range(steps - BUFS, steps):
        for cp in copies(i):
            cp.wait()


def finish_kernel(base, got, gx_out):
    chunk = got.shape[2]
    for s in range(SUBS):
        gx_out[:, pl.ds(s * chunk, chunk)] = (base[s] + got[s]).astype(BF16)


def solution(mesh):
    n_dev = mesh.shape["ep"]
    rows_spec = P(("dp", "ep"), None)
    cube_spec = P(("dp", "ep"), None, None)
    weight_spec = P("ep", None, None)

    def local_step(grad_y, gate_vals, topk_idx, slot_ids, pair_counts, y_routed, x_disp, h_gate, h_up, w_gate, w_up, w_down):
        n_loc, ffn, model = w_down.shape
        tok, top_k = topk_idx.shape
        rows = x_disp.shape[1]
        cap = rows // n_dev
        n_chip = n_dev // 2
        vm = pl.BlockSpec(memory_space=pltpu.VMEM)
        hbm = pl.BlockSpec(memory_space=pl.ANY)
        dma = pltpu.SemaphoreType.DMA
        vs = pltpu.VMEM
        tail = vs((SUBS, tok, model // SUBS), F32)
        js = 2
        base, last, gg, d_rows, dh, act, x_rows = pl.pallas_call(
            functools.partial(exchange_kernel, n_dev, cap),
            out_shape=(tail, tail, pltpu.VMEM((top_k, tok), F32), pltpu.VMEM((n_loc, rows, model), BF16),
                       pltpu.VMEM((n_loc, rows, 2 * ffn), BF16), pltpu.VMEM((n_loc, rows, ffn), BF16), pltpu.VMEM((n_loc, rows, model), BF16)),
            in_specs=[hbm] * 12,
            out_specs=(vm,) * 7,
            scratch_shapes=[
                pltpu.SMEM(pair_counts.shape, jnp.int32),
                pltpu.VMEM((top_k, tok), jnp.int32),
                pltpu.VMEM((top_k, tok), jnp.int32),
                pltpu.VMEM((n_dev, tok, model), BF16),
                pltpu.VMEM((tok, top_k, model), BF16),
                pltpu.VMEM((n_loc, rows, ffn), BF16),
                pltpu.VMEM((n_loc, rows, ffn), BF16),
                pltpu.VMEM((n_loc, model, 2 * ffn), BF16),
                pltpu.VMEM((n_loc, ffn, model), BF16),
                pltpu.VMEM((n_loc, rows, 2 * ffn), F32),
                pltpu.VMEM((tok, top_k), F32),
                pltpu.VMEM((n_dev, 2, top_k, tok), F32),
                pltpu.VMEM((n_dev, n_loc * cap, tok), BF16),
                pltpu.VMEM((n_dev, n_loc * cap, 1), F32),
                pltpu.VMEM((n_dev, tok, n_loc * cap), BF16),
                pltpu.VMEM((2, 2, n_loc * cap, model // SUBS), BF16),
                pltpu.VMEM((n_chip, SUBS, tok, model // SUBS), F32),
                pltpu.VMEM((n_chip, SUBS, tok, model // SUBS), F32),
                pltpu.VMEM((n_chip, SUBS, tok, model // SUBS), F32),
                pltpu.VMEM((2 * SUBS, tok, model // SUBS), F32),
                pltpu.VMEM((2 * SUBS, tok, model // SUBS), F32),
                dma((12,)), dma((n_dev - 1,)), dma((n_dev - 1,)), dma((13,)), dma((13,)),
                dma((SUBS * n_chip,)), dma((SUBS * n_chip,)), dma((2 * SUBS,)), dma((2 * SUBS,)),
            ],
            compiler_params=pltpu.CompilerParams(collective_id=0, has_side_effects=True, vmem_limit_bytes=44 * 1024 * 1024),
            name="exchange",
        )(pair_counts, gate_vals.T, topk_idx.T, slot_ids.T, grad_y, y_routed, h_gate, h_up, w_gate, w_up, w_down, x_disp)
        hops = [(i, ((i // 2 + 1 - 2 * (i % 2)) % n_chip) * 2 + i % 2) for i in range(n_dev)]
        got = lax.ppermute(last, "ep", hops)
        gg, gwg, gwu, gwd = pl.pallas_call(
            functools.partial(weight_kernel, js),
            out_shape=(jax.ShapeDtypeStruct((top_k, tok), F32), jax.ShapeDtypeStruct((n_loc, model, ffn), F32),
                       jax.ShapeDtypeStruct((n_loc, model, ffn), F32), jax.ShapeDtypeStruct((n_loc, ffn, model), F32)),
            in_specs=[vm] * 5,
            out_specs=(vm, hbm, hbm, hbm),
            scratch_shapes=[pltpu.VMEM((BUFS, 2, model // js, ffn), F32), pltpu.VMEM((BUFS, ffn // js, model), F32), dma((BUFS, 3))],
            compiler_params=pltpu.CompilerParams(vmem_limit_bytes=24 * 1024 * 1024),
            cost_estimate=pl.CostEstimate(flops=6 * n_loc * rows * model * ffn, bytes_accessed=12 * n_loc * model * ffn, transcendentals=0),
            name="weights",
        )(x_rows, dh, act, d_rows, gg)
        gx = pl.pallas_call(
            finish_kernel,
            out_shape=jax.ShapeDtypeStruct((tok, model), BF16),
            in_specs=[vm] * 2,
            out_specs=vm,
            compiler_params=pltpu.CompilerParams(vmem_limit_bytes=4 * 1024 * 1024),
            name="finish",
        )(base, got)
        return gx, gg.T, gwg, gwu, gwd

    return jax.shard_map(local_step, mesh=mesh, in_specs=(rows_spec, rows_spec, rows_spec, rows_spec, rows_spec, cube_spec, cube_spec, cube_spec, cube_spec, weight_spec, weight_spec, weight_spec), out_specs=(rows_spec, rows_spec, cube_spec, cube_spec, cube_spec), check_vma=False)
```
